32 devices in a mesh: gx: 4 (over y, x), gy: 2 (over core), gz: 4 (over z).
Axes of the slice: x: 2, y: 2, z: 4, core: 2. Of those that a mesh axis runs over, the one named last changes fastest.
Arguments:
- labels: int32 [128, 128, 512], P('gx', 'gy', 'gz'), may hold values from 0 to 7
- conductivity: float32 [7, 8], replicated, may hold values from -0.08 to 2, as said below
- right_side: float32 [128, 128, 512], P('gx', 'gy', 'gz'), may hold values from -18 to 18
Outputs:
- solution: float32 [128, 128, 512], P('gx', 'gy', 'gz')
The draws below stay inside these ranges and needn't reach their ends.
Inputs may be any that keep to these rules, and one draw needn't show every extreme that they name: `conductivity`: rows 0 to 2 are positive, rows 3 to 5 have magnitude at most 0.08, row 6 is at least 0.5.
All inputs are finite; a program needn't handle non-finite values.
Results may differ from the reference program's by a relative error of at most 0.0001.
Values sent between devices are 32-bit elements; how exact they have to be, the bound alone decides.
A program may use at most 128 MiB of HBM per device.

```python
import math
import jax
import jax.numpy as jnp
from jax import lax

ITERS = 3
LABELS = 8
NX = 128
NY = 128
NZ = 512


def draw_conductivity(key, part):
    key_diag = jax.random.fold_in(key, 11)
    key_off = jax.random.fold_in(key, 12)
    key_mass = jax.random.fold_in(key, 13)
    diagonal = jnp.exp(jax.random.uniform(key_diag, (3, LABELS), jnp.float32, math.log(0.5), math.log(2.0)))
    offdiag = jax.random.uniform(key_off, (3, LABELS), jnp.float32, -0.08, 0.08)
    mass = jnp.exp(jax.random.uniform(key_mass, (1, LABELS), jnp.float32, math.log(0.5), math.log(1.0)))
    return jnp.concatenate([diagonal, offdiag, mass], axis=0).astype(jnp.float32)


def draw_right_side(key, part):
    key_base = jax.random.fold_in(key, 21)
    key_scale = jax.random.fold_in(key, 22)
    column = jnp.exp(jax.random.uniform(key_scale, (NX, NY, 1), jnp.float32, math.log(0.3), math.log(3.0)))
    ramp = 0.5 + jnp.arange(NY, dtype=jnp.float32)[None, :, None] / NY
    base = jnp.clip(jax.random.normal(key_base, (NX, NY, NZ), jnp.float32), -3.6, 3.6)
    return (base * column * ramp + 1.0).astype(jnp.float32)


def place_ends(array, stream_key, low, top_value):
    index_at = [jax.random.randint(jax.random.fold_in(stream_key, axis), (), 0, length) for axis, length in enumerate(array.shape)]
    widest = array.shape.index(max(array.shape))
    neighbour = index_at[:widest] + [(index_at[widest] + 1) % array.shape[widest]] + index_at[widest + 1:]
    return array.at[tuple(index_at)].set(low).at[tuple(neighbour)].set(top_value)


def setup_inputs(seed: int = 0) -> dict:
    arg_keys = jax.random.split(jax.random.key(seed), 4)
    labels = place_ends(jax.random.randint(arg_keys[0], (NX, NY, NZ), 0, LABELS), jax.random.fold_in(arg_keys[0], 1), 0, LABELS - 1).astype(jnp.int32)
    conductivity = draw_conductivity(jax.random.fold_in(arg_keys[3], 71), 0)
    right_side = draw_right_side(jax.random.fold_in(arg_keys[3], 71), 0)
    return {"labels": labels, "conductivity": conductivity, "right_side": right_side}


def neighbour_value(arr, shift_x, shift_y, shift_z, cell_grid):
    size_x, size_y, size_z = cell_grid
    return arr[..., 1 + shift_x:1 + shift_x + size_x, 1 + shift_y:1 + shift_y + size_y, 1 + shift_z:1 + shift_z + size_z]


def stencil_apply(padded_value, padded_sigma, self_coefficient):
    cell_grid = self_coefficient.shape
    value_entry = neighbour_value(padded_value, 0, 0, 0, cell_grid)
    total_flux = self_coefficient * value_entry
    for axis in range(3):
        for sign in (-1, 1):
            stencil_offset = [0, 0, 0]
            stencil_offset[axis] = sign
            face_flux = 0.5 * (neighbour_value(padded_sigma[axis], 0, 0, 0, cell_grid) + neighbour_value(padded_sigma[axis], stencil_offset[0], stencil_offset[1], stencil_offset[2], cell_grid))
            total_flux = total_flux + face_flux * (value_entry - neighbour_value(padded_value, stencil_offset[0], stencil_offset[1], stencil_offset[2], cell_grid))
    for first, second, comp in ((0, 1, 3), (0, 2, 4), (1, 2, 5)):
        for sign_a in (-1, 1):
            for sign_b in (-1, 1):
                stencil_offset = [0, 0, 0]
                stencil_offset[first] = sign_a
                stencil_offset[second] = sign_b
                cross_term = (0.25 * sign_a * sign_b) * (neighbour_value(padded_sigma[comp], 0, 0, 0, cell_grid) + neighbour_value(padded_sigma[comp], stencil_offset[0], stencil_offset[1], stencil_offset[2], cell_grid))
                total_flux = total_flux - cross_term * neighbour_value(padded_value, stencil_offset[0], stencil_offset[1], stencil_offset[2], cell_grid)
    return total_flux


def diagonal_of(padded_sigma, self_coefficient):
    cell_grid = self_coefficient.shape
    total_flux = self_coefficient
    for axis in range(3):
        for sign in (-1, 1):
            stencil_offset = [0, 0, 0]
            stencil_offset[axis] = sign
            total_flux = total_flux + 0.5 * (neighbour_value(padded_sigma[axis], 0, 0, 0, cell_grid) + neighbour_value(padded_sigma[axis], stencil_offset[0], stencil_offset[1], stencil_offset[2], cell_grid))
    return total_flux


def reference(labels, conductivity, right_side):
    extended = jnp.concatenate([jnp.zeros((7, 1), conductivity.dtype), conductivity], axis=1)
    label_pad = jnp.pad(labels.astype(jnp.int32) + 1, 1)
    planes = jnp.arange(labels.shape[0], dtype=jnp.int32)

    def slab_table(index):
        part = lax.dynamic_slice_in_dim(label_pad, index, 3, 0)
        table = jnp.take(extended, part, axis=1)
        return table[:6], table[6, 1:2, 1:-1, 1:-1]

    def diag_plane(index):
        padded_sigma, self_coefficient = slab_table(index)
        return diagonal_of(padded_sigma, self_coefficient)[0]

    diag = lax.map(diag_plane, planes)

    def operate(field):
        field_pad = jnp.pad(field, 1)

        def one_plane(index):
            padded_sigma, self_coefficient = slab_table(index)
            part = lax.dynamic_slice_in_dim(field_pad, index, 3, 0)
            return stencil_apply(part, padded_sigma, self_coefficient)[0]

        return lax.map(one_plane, planes)

    solution = jnp.zeros_like(right_side)
    residual = right_side
    precond = residual / diag
    direction = precond
    gamma = jnp.sum(residual * precond)
    for step in range(ITERS):
        image = operate(direction)
        alpha = gamma / jnp.sum(direction * image)
        solution = solution + alpha * direction
        residual = residual - alpha * image
        precond = residual / diag
        fresh = jnp.sum(residual * precond)
        direction = precond + (fresh / gamma) * direction
        gamma = fresh
    return solution
```

```python
import functools
import itertools
import math
import jax
import jax.numpy as jnp
from jax import lax
from jax.experimental import pallas as pl
from jax.experimental.pallas import tpu as pltpu
from jax.sharding import PartitionSpec as P

ITERS = 3
AXES = ("gx", "gy", "gz")
ROUNDS = ITERS + 1
MOMENTS = 2 * ITERS
LANES = 128
PAD = 8
T8 = 8


def group_size(n, most):
    return max(u for u in range(1, most + 1) if n % u == 0)


def kernel(
    sizes, lab_hbm, cond, rhs_hbm, out, lab, rhs, V0, V1, V2, V3, S, F, DI, PS, PR, ES, ER, HB, HS, PG, CP, MA, RS,
    RR, send_sem, recv_sem, ar_send, ar_recv, in_sem,
):
    V = (V0, V1, V2, V3)
    X, Y, Z = rhs.shape
    lab_copy = pltpu.make_async_copy(lab_hbm, lab, in_sem.at[0])
    lab_copy.start()
    rhs_copy = pltpu.make_async_copy(rhs_hbm, rhs, in_sem.at[1])
    rhs_copy.start()
    YE = Y + 2 * PAD
    TOP = PAD + Y
    KT = Y // T8
    me = [lax.axis_index(a) for a in AXES]
    f32 = jnp.float32
    scope = jax.named_scope

    directions = []
    for dx in (-1, 0, 1):
        for dy in (-1, 0, 1):
            for dz in (-1, 0, 1):
                d = (dx, dy, dz)
                live = sum(1 for t in d if t)
                if live in (1, 2) and all(n > 1 for t, n in zip(d, sizes) if t):
                    directions.append(d)

    def needed(d, r):
        if r < ROUNDS - 1:
            return True
        if d[2]:
            return d[2] < 0
        return d[0] <= 0 and d[1] <= 0

    def present(d):
        ok = None
        for t, m, n in zip(d, me, sizes):
            if t == 0:
                continue
            here = (m < n - 1) if t > 0 else (m > 0)
            ok = here if ok is None else jnp.logical_and(ok, here)
        return ok

    def places(d, r):
        dx, dy, dz = d
        rows_from = pl.ds(PAD, Y) if dy == 0 else (pl.ds(TOP - 8, 8) if dy > 0 else pl.ds(PAD, 8))
        rows_to = pl.ds(PAD, Y) if dy == 0 else (pl.ds(0, 8) if dy > 0 else pl.ds(TOP, 8))
        if dz == 0:
            if dx == 0:
                return V[r].at[pl.ds(1, X), rows_from], V[r].at[pl.ds(1, X), rows_to]
            fx, tx = (X, 0) if dx > 0 else (1, X + 1)
            return V[r].at[fx, rows_from], V[r].at[tx, rows_to]
        side = 0 if dz > 0 else 1
        if dx == 0:
            return PS.at[r, rows_from], PR.at[r, side, rows_to]
        slot = (0 if dx > 0 else 2) + side
        return ES.at[r], ER.at[r, slot]

    def copy(d, r):
        src, dst = places(d, r)
        m = directions.index(d)
        return pltpu.make_async_remote_copy(
            src_ref=src,
            dst_ref=dst,
            send_sem=send_sem.at[r, m],
            recv_sem=recv_sem.at[r, m],
            device_id=tuple(a + t for a, t in zip(me, d)),
            device_id_type=pl.DeviceIdType.MESH,
        )

    groups = [(0, 1, 2)] if math.prod(sizes) <= 32 else [(0, 1), (2,)]
    near = len(groups) == 1 and max(sizes) <= ROUNDS and sum(n - 1 for n in sizes) <= 2 * ROUNDS - 1

    def offsets(group):
        ranges = [range(n) if i in group else (0,) for i, n in enumerate(sizes)]
        return [t for t in itertools.product(*ranges) if any(t)]

    def partner(t):
        return tuple(lax.rem(m + k, n) for m, k, n in zip(me, t, sizes))

    barrier = pltpu.get_barrier_semaphore()
    greeted = 0
    if not near:
        for group in groups:
            for t in offsets(group):
                pl.semaphore_signal(
                    barrier, inc=1, device_id=partner(t), device_id_type=pl.DeviceIdType.MESH
                )
                greeted += 1
    if near or len(groups) > 1:
        for d in directions:
            pl.when(present(d))(
                lambda d=d: pl.semaphore_signal(
                    barrier,
                    inc=1,
                    device_id=tuple(a + t for a, t in zip(me, d)),
                    device_id_type=pl.DeviceIdType.MESH,
                )
            )
            greeted = greeted + jnp.where(present(d), 1, 0)

    for d in [
        (dx, dy, dz)
        for dx in (-1, 0, 1)
        for dy in (-1, 0, 1)
        for dz in (-1, 0, 1)
        if sum(1 for t in (dx, dy, dz) if t) in (1, 2)
    ]:
        def clear(d=d):
            for r in range(ROUNDS):
                if needed(d, r):
                    _, dst = places(d, r)
                    dst[...] = jnp.zeros(dst.shape, f32)

        if d in directions:
            back = tuple(-t for t in d)
            pl.when(jnp.logical_not(present(back)))(clear)
        else:
            clear()

    for r in range(ROUNDS):
        for a in (0, TOP):
            PS[r, pl.ds(a, PAD), :] = jnp.zeros((PAD, LANES), f32)
    MA[...] = jnp.zeros(MA.shape, f32)

    lane_e = lax.broadcasted_iota(jnp.int32, (YE, LANES), 1)
    lane_8 = lax.broadcasted_iota(jnp.int32, (T8, LANES), 1)
    row_8 = lax.broadcasted_iota(jnp.int32, (T8, LANES), 0)
    even = lane_e % 2 == 0
    ends = jnp.logical_or(lane_8 == 0, lane_8 == LANES - 1)
    inner = lane_8 < LANES - 1
    tiles = [PAD + T8 * k for k in range(KT)]

    scale = (0.5, 0.5, 0.5, 0.25, 0.25, 0.25, 1.0)
    count = cond.shape[1]
    tables = []
    for c in range(7):
        table = jnp.zeros((T8, LANES), f32)
        for k in range(count):
            table = jnp.where(row_8 == k, cond[c, k] * scale[c], table)
        tables.append(table)

    def look(c, index):
        return jnp.take_along_axis(tables[c], index, axis=0, mode="promise_in_bounds")

    def look_known(values, components):
        index = jnp.maximum(values.astype(jnp.int32) - 1, 0)
        hit = values > 0.0
        return [jnp.where(hit, look(c, index), 0.0) for c in components]

    def send(d, r):
        if d in directions and needed(d, r):
            pl.when(present(d))(lambda: copy(d, r).start())

    def start_x(r, plane):
        tile = jnp.zeros((T8, LANES), f32)
        for col, (x, at) in enumerate(((0, 0), (0, LANES - 1), (X - 1, 0), (X - 1, LANES - 1))):
            for k in range(KT):
                to = col * KT + k
                part = plane(x, k)
                tile = jnp.where(lane_8 == to, pltpu.roll(part, (to - at) % LANES, 1), tile)
        ES[r] = tile
        for d in directions:
            if d[0]:
                send(d, r)

    def start_rest(r):
        for d in directions:
            if not d[0]:
                send(d, r)

    def wait(r):
        for d in directions:
            if needed(d, r):
                back = tuple(-t for t in d)
                pl.when(present(back))(lambda d=d: copy(d, r).wait_recv())

    def build_halo(r):
        low = pltpu.roll(PR[r, 0], 1, 1)
        high = pltpu.roll(PR[r, 1], LANES - 1, 1)
        valid = jnp.logical_or(lane_e <= 2 * (X - 1), lane_e == LANES - 1)
        last = r == ROUNDS - 1
        HB[...] = jnp.where(valid, jnp.where(even, 0.0 if last else low, high), 0.0)
        targets = (((LANES - 2), 3), ((LANES - 3), 2), (2 * X, 1), (2 * X - 1, 0))
        slots = (1, 3) if last else (0, 1, 2, 3)
        got = {slot: ER[r, slot] for slot in slots}
        for k in range(KT):
            rows = pl.ds(PAD + T8 * k, T8)
            part = HB[rows, :]
            for slot in slots:
                target, col = targets[slot]
                at = col * KT + k
                part = jnp.where(
                    lane_8 == target, pltpu.roll(got[slot], (target - at) % LANES, 1), part
                )
            HB[rows, :] = part

    def zm(a):
        return pltpu.roll(a, 1, 1)

    def zp(a):
        return pltpu.roll(a, LANES - 1, 1)

    def unpack(part, x):
        return jnp.where(ends, pltpu.roll(part, lax.rem(LANES - 2 * x, LANES), 1), 0.0)

    def pack(r, plane):
        for k in range(KT):
            tile = plane(0, k)
            for x in range(1, X):
                here = jnp.logical_and(lane_8 >= 2 * x - 1, inner)
                tile = jnp.where(here, pltpu.roll(plane(x, k), 2 * x, 1), tile)
            PS[r, pl.ds(PAD + T8 * k, T8), :] = tile

    def label_tile(x, k):
        return (lab[x, pl.ds(T8 * k, T8), :] + 1).astype(f32)

    def field_tile(r):
        return lambda x, k: V[r][x + 1, pl.ds(PAD + T8 * k, T8), :]

    with scope("labwait"):
        lab_copy.wait()

    with scope("conv"):
        for x in (0, X - 1):
            for k in range(KT):
                V[0][x + 1, pl.ds(PAD + T8 * k, T8), :] = label_tile(x, k)

        for x in range(1, X - 1):
            for k in (0, KT - 1):
                V[0][x + 1, pl.ds(PAD + T8 * k, T8), :] = label_tile(x, k)

    with scope("pack0"):
        pack(0, label_tile)
    with scope("barrier"):
        pl.semaphore_wait(barrier, greeted)
    with scope("start0"):
        start_x(0, label_tile)
        start_rest(0)

    with scope("sigma_own"):
        @pl.loop(0, X, unroll=4)
        def _(x):
            for a in tiles:
                index = lab[x, pl.ds(a - PAD, T8), :]
                for c in range(6):
                    S[c, x + 1, pl.ds(a, T8), :] = look(c, index)

    with scope("wait0"):
        wait(0)

    with scope("sigma_halo"):
        for x in (0, X + 1):
            for a in range(0, YE, T8):
                rows = pl.ds(a, T8)
                for c, s in enumerate(look_known(V[0][x, rows, :], range(6))):
                    S[c, x, rows, :] = s

        @pl.loop(1, X + 1, unroll=4)
        def _(x):
            for a in (0, TOP):
                rows = pl.ds(a, T8)
                for c, s in enumerate(look_known(V[0][x, rows, :], range(6))):
                    S[c, x, rows, :] = s

        build_halo(0)
        for a in range(0, YE, T8):
            rows = pl.ds(a, T8)
            for i, s in enumerate(look_known(HB[rows, :], (2, 4, 5))):
                HS[i, rows, :] = s
            for i, s in enumerate(look_known(PS[0, rows, :], (2, 4, 5))):
                PG[i, rows, :] = s
        CP[...] = PG[0] + HS[0]
        rhs_copy.wait()

    def coefficients(p):
        for a in [0] + tiles:
            rows, up = pl.ds(a, T8), pl.ds(a + 1, T8)
            s1, s1u = S[1, p, rows, :], S[1, p, up, :]
            s3, s3u = S[3, p, rows, :], S[3, p, up, :]
            t3, t3u = S[3, p + 1, rows, :], S[3, p + 1, up, :]
            s5, s5u = S[5, p, rows, :], S[5, p, up, :]
            F[1, p, rows, :] = s1 + s1u
            F[3, p, rows, :] = s3 + t3u
            F[4, p, rows, :] = t3 + s3u
            F[7, p, rows, :] = jnp.where(inner, s5 + zp(s5u), 0.0)
            F[8, p, rows, :] = jnp.where(inner, s5u + zp(s5), 0.0)
            if a:
                s2 = S[2, p, rows, :]
                s4, t4 = S[4, p, rows, :], S[4, p + 1, rows, :]
                F[0, p, rows, :] = S[0, p, rows, :] + S[0, p + 1, rows, :]
                F[2, p, rows, :] = jnp.where(inner, s2 + zp(s2), 0.0)
                F[5, p, rows, :] = jnp.where(inner, s4 + zp(t4), 0.0)
                F[6, p, rows, :] = jnp.where(inner, t4 + zp(s4), 0.0)

    def diagonal(x, total):
        p = x + 1
        for a in tiles:
            rows, down = pl.ds(a, T8), pl.ds(a - 1, T8)
            own = pl.ds(a - PAD, T8)
            f2 = F[2, p, rows, :]
            diag = look(6, lab[x, own, :]) + F[0, p, rows, :] + F[0, p - 1, rows, :]
            diag = diag + F[1, p, rows, :] + F[1, p, down, :]
            diag = diag + (f2 + zm(f2)) + unpack(CP[rows, :], x)
            inverse = 1.0 / diag
            DI[x, own, :] = inverse
            r0 = rhs[x, own, :]
            w = r0 * inverse
            V[1][p, rows, :] = w
            total = total + r0 * w
        return total

    def zero():
        return jnp.zeros((T8, LANES), f32)

    with scope("coef_x"):
        for p in (0, 1, X - 1, X):
            coefficients(p)
        MA[0] = diagonal(X - 1, diagonal(0, zero()))
    with scope("startx_1"):
        start_x(1, field_tile(1))

    with scope("coef"):
        @pl.loop(2, X - 1)
        def _(p):
            coefficients(p)

    with scope("diag"):
        width = group_size(X - 2, 6)

        @pl.loop(0, (X - 2) // width)
        def _(g):
            total = zero()
            for i in range(width):
                total = diagonal(1 + g * width + i, total)
            MA[0] = MA[0] + total

    def planes(r, x0, width):
        odd, evn = zero(), zero()
        field, nxt = V[r], V[r + 1]
        for a in tiles:
            rows, up, down = pl.ds(a, T8), pl.ds(a + 1, T8), pl.ds(a - 1, T8)
            own = pl.ds(a - PAD, T8)
            halo = CP[rows, :]
            m, mu, md = field[x0, rows, :], field[x0, up, :], field[x0, down, :]
            v, vu, vd = field[x0 + 1, rows, :], field[x0 + 1, up, :], field[x0 + 1, down, :]
            tv = zp(v)
            acc = F[0, x0, rows, :] * m + F[3, x0, down, :] * md
            acc = acc - F[4, x0, rows, :] * mu - F[6, x0, rows, :] * zp(m)
            accs = F[5, x0, rows, :] * m
            for i in range(width):
                x = x0 + i
                p = x + 1
                n, nu, nd = field[p + 1, rows, :], field[p + 1, up, :], field[p + 1, down, :]
                tn = zp(n)
                f0 = F[0, p, rows, :]
                f2 = F[2, p, rows, :]
                f3, f3d = F[3, p, rows, :], F[3, p, down, :]
                f4, f4d = F[4, p, rows, :], F[4, p, down, :]
                f5, f6 = F[5, p, rows, :], F[6, p, rows, :]
                f7, f7d = F[7, p, rows, :], F[7, p, down, :]
                f8, f8d = F[8, p, rows, :], F[8, p, down, :]
                s = (accs + f2 * v) + (f7d * vd - f8 * vu) - f6 * n
                q = (acc + f0 * n) + (F[1, p, rows, :] * vu + F[1, p, down, :] * vd)
                q = q + (f3 * nu - f4d * nd) + (f2 * tv + f5 * tn)
                q = q + (f7 * zp(vu) - f8d * zp(vd))
                q = q + zm(s) + unpack(halo, x)
                acc = (f0 * v + f3d * vd) - (f4 * vu + f6 * tv)
                accs = f5 * v
                odd = odd + v * q
                w = q * DI[x, own, :]
                evn = evn + w * q
                nxt[p, rows, :] = w
                v, vu, vd, tv = n, nu, nd, tn
        return odd, evn

    def pairs(r, x0, width):
        total = zero()
        field = V[r]
        for a in tiles:
            rows, up = pl.ds(a, T8), pl.ds(a + 1, T8)
            v, vu = field[x0 + 1, rows, :], field[x0 + 1, up, :]
            tv, tvu = zp(v), zp(vu)
            for i in range(width):
                p = x0 + i + 1
                n, nu = field[p + 1, rows, :], field[p + 1, up, :]
                tn, tnu = zp(n), zp(nu)
                a0 = (F[0, p, rows, :] * n + F[1, p, rows, :] * vu) + (F[3, p, rows, :] * nu + F[5, p, rows, :] * tn)
                a0 = a0 + F[7, p, rows, :] * tvu
                a1 = F[2, p, rows, :] * v - F[6, p, rows, :] * n - F[8, p, rows, :] * vu
                total = total + v * a0 + (tv * a1 - (F[4, p, rows, :] * n) * vu)
                v, vu, tv, tvu = n, nu, tn, tnu
        return total

    def along_x(a):
        return pltpu.roll(a, LANES - 2, 1) - pltpu.roll(a, 2, 1)

    def along_y(a):
        return pltpu.roll(a, YE - 1, 0) - pltpu.roll(a, 1, 0)

    sign = jnp.where(even, f32(-1.0), f32(1.0))
    for step in range(ITERS):
        r = step + 1
        last = step + 1 == ITERS
        with scope(f"pack_{r}"):
            pack(r, field_tile(r))
        with scope(f"start_{r}"):
            start_rest(r)
        with scope(f"wait_{r}"):
            wait(r)
        with scope(f"halo_{r}"):
            build_halo(r)
            h = HB[...]
            CP[...] = (PG[0] + HS[0]) * h + sign * (
                PG[1] * along_x(h) + along_x(HS[1] * h) + PG[2] * along_y(h) + along_y(HS[2] * h)
            )
        if last:
            break
        with scope(f"edge_{r}"):
            o0, e0 = planes(r, 0, 1)
            o1, e1 = planes(r, X - 1, 1)
            MA[2 * step + 1] = o0 + o1
            MA[2 * step + 2] = e0 + e1
        with scope(f"startx_{r + 1}"):
            start_x(r + 1, field_tile(r + 1))
        with scope(f"matvec_{r}"):
            width = group_size(X - 2, 6)

            @pl.loop(0, (X - 2) // width)
            def _(g):
                odd, evn = planes(r, 1 + g * width, width)
                MA[2 * step + 1] = MA[2 * step + 1] + odd
                MA[2 * step + 2] = MA[2 * step + 2] + evn

    with scope("pairs"):
        width = group_size(X, 8)
        mine = jnp.logical_and(lane_8 % 2 == 1, jnp.logical_or(lane_8 < 2 * (X - 1), lane_8 == LANES - 1))
        total = zero()
        for a in tiles:
            rows = pl.ds(a, T8)
            total = total + jnp.where(mine, PS[ROUNDS - 1, rows, :] * CP[rows, :], 0.0)
        MA[MOMENTS - 1] = total

        @pl.loop(0, X // width)
        def _(g):
            MA[MOMENTS - 1] = MA[MOMENTS - 1] + pairs(ROUNDS - 1, g * width, width)

    with scope("allreduce"):
        tile = zero()
        for k in range(MOMENTS):
            value = jnp.sum(jnp.sum(MA[k], axis=0, keepdims=True), axis=1, keepdims=True)
            tile = jnp.where(lane_8 == k, value * (2.0 if k == MOMENTS - 1 else 1.0), tile)
        for order, group in enumerate(groups):
            slot = 0
            members = 1
            for i in group:
                slot = slot * sizes[i] + me[i]
                members *= sizes[i]
            RS[order] = tile[0:1]
            copies = []
            for index, t in enumerate(offsets(group)):
                c = pltpu.make_async_remote_copy(
                    src_ref=RS.at[order],
                    dst_ref=RR.at[order, slot],
                    send_sem=ar_send.at[order, index],
                    recv_sem=ar_recv.at[order, index],
                    device_id=partner(t),
                    device_id_type=pl.DeviceIdType.MESH,
                )
                c.start()
                copies.append(c)
            RR[order, slot] = tile[0:1]
            for c in copies:
                c.wait()
            parts = [RR[order, t] for t in range(members)]
            while len(parts) > 1:
                parts = [sum(parts[i + 1 : i + 2], parts[i]) for i in range(0, len(parts), 2)]
            tile = jnp.broadcast_to(parts[0], (T8, LANES))

    n0, n1, n2, n3, n4, n5 = (
        jnp.sum(jnp.where(lane_8 == k, tile, 0.0)[0:1], axis=1, keepdims=True) for k in range(MOMENTS)
    )

    def inverse_of(d):
        return jnp.where(d > 0.0, 1.0 / d, 0.0)

    g00, g01, g02, g12, g22 = n0 - n1, n1 - n2, n2 - n3, n3 - n4, n4 - n5
    i0 = 1.0 / g00
    l1, l2 = g01 * i0, g02 * i0
    i1 = inverse_of(g02 - l1 * g01)
    e = g12 - l2 * g01
    l21 = e * i1
    i2 = inverse_of(g22 - l2 * g02 - l21 * e)
    y1 = n1 - l1 * n0
    y2 = n2 - l2 * n0 - l21 * y1
    c2 = y2 * i2
    c1 = y1 * i1 - l21 * c2
    c0 = n0 * i0 - l1 * c1 - l2 * c2

    with scope("output"):
        @pl.loop(0, X, unroll=4)
        def _(x):
            for a in tiles:
                rows = pl.ds(a, T8)
                out[x, pl.ds(a - PAD, T8), :] = (
                    c0 * V[1][x + 1, rows, :] + c1 * V[2][x + 1, rows, :] + c2 * V[3][x + 1, rows, :]
                )

    for r in range(ROUNDS):
        for d in directions:
            if needed(d, r):
                pl.when(present(d))(lambda d=d, r=r: copy(d, r).wait_send())


def solution(mesh):
    sizes = tuple(mesh.shape[a] for a in AXES)

    def local(labels, conductivity, right_side):
        X, Y, Z = right_side.shape
        YE = Y + 2 * PAD
        f32 = jnp.float32
        vmem = pltpu.VMEM
        return pl.pallas_call(
            functools.partial(kernel, sizes),
            out_shape=jax.ShapeDtypeStruct((X, Y, Z), f32),
            in_specs=[
                pl.BlockSpec(memory_space=pl.ANY),
                pl.BlockSpec(memory_space=pltpu.SMEM),
                pl.BlockSpec(memory_space=pl.ANY),
            ],
            out_specs=pl.BlockSpec(memory_space=pltpu.VMEM),
            scratch_shapes=[
                vmem((X, Y, Z), jnp.int32),
                vmem((X, Y, Z), f32),
                vmem((X + 2, YE, Z), f32),
                vmem((X + 2, YE, Z), f32),
                vmem((X + 2, YE, Z), f32),
                vmem((X + 2, YE, Z), f32),
                vmem((6, X + 2, YE, Z), f32),
                vmem((9, X + 1, YE, Z), f32),
                vmem((X, Y, Z), f32),
                vmem((ROUNDS, YE, Z), f32),
                vmem((ROUNDS, 2, YE, Z), f32),
                vmem((ROUNDS, 8, Z), f32),
                vmem((ROUNDS, 4, 8, Z), f32),
                vmem((YE, Z), f32),
                vmem((3, YE, Z), f32),
                vmem((3, YE, Z), f32),
                vmem((YE, Z), f32),
                vmem((MOMENTS, 8, Z), f32),
                vmem((2, 1, Z), f32),
                vmem((2, 32, 1, Z), f32),
                pltpu.SemaphoreType.DMA((ROUNDS, 18)),
                pltpu.SemaphoreType.DMA((ROUNDS, 18)),
                pltpu.SemaphoreType.DMA((2, 32)),
                pltpu.SemaphoreType.DMA((2, 32)),
                pltpu.SemaphoreType.DMA((2,)),
            ],
            compiler_params=pltpu.CompilerParams(
                collective_id=0, has_side_effects=True, vmem_limit_bytes=60 * 1024 * 1024
            ),
        )(labels, conductivity, right_side)

    return jax.shard_map(
        local,
        mesh=mesh,
        in_specs=(P("gx", "gy", "gz"), P(), P("gx", "gy", "gz")),
        out_specs=P("gx", "gy", "gz"),
        check_vma=False,
    )
```

```python
import functools
import itertools
import math
import jax
import jax.numpy as jnp
from jax import lax
from jax.experimental import pallas as pl
from jax.experimental.pallas import tpu as pltpu
from jax.sharding import PartitionSpec as P

ITERS = 3
AXES = ("gx", "gy", "gz")
ROUNDS = ITERS + 1
MOMENTS = 2 * ITERS
LANES = 128
PAD = 8
T8 = 8


def group_size(n, most):
    return max(u for u in range(1, most + 1) if n % u == 0)


def groups_of(sizes):
    return [(0, 1, 2)] if math.prod(sizes) <= 32 else [(0, 1), (2,)]


def kernel(
    sizes, lab_hbm, cond_hbm, rhs_hbm, W, C, lab, cond, rhs, V0, V1, V2, V3, S, F, DI, PS, PZ, PR, ZR, ES, ER, HB, HS, PG, CP,
    MA, RS, RR, send_sem, recv_sem, ar_send, ar_recv, in_sem,
):
    V = (V0, V1, V2, V3)
    X, Y, Z = rhs.shape
    lab_copy = pltpu.make_async_copy(lab_hbm, lab, in_sem.at[0])
    lab_copy.start()
    cond_copy = pltpu.make_async_copy(cond_hbm, cond, in_sem.at[2])
    cond_copy.start()
    rhs_copy = pltpu.make_async_copy(rhs_hbm, rhs, in_sem.at[1])
    YE = Y + 2 * PAD
    TOP = PAD + Y
    KT = Y // T8
    me = [lax.axis_index(a) for a in AXES]
    f32 = jnp.float32
    scope = jax.named_scope

    directions = []
    for dx in (-1, 0, 1):
        for dy in (-1, 0, 1):
            for dz in (-1, 0, 1):
                d = (dx, dy, dz)
                live = sum(1 for t in d if t)
                if live in (1, 2) and all(n > 1 for t, n in zip(d, sizes) if t):
                    directions.append(d)

    def needed(d, r):
        if r < ROUNDS - 1:
            return True
        if d[2]:
            return d[2] < 0
        return d[0] <= 0 and d[1] <= 0

    def present(d):
        ok = None
        for t, m, n in zip(d, me, sizes):
            if t == 0:
                continue
            here = (m < n - 1) if t > 0 else (m > 0)
            ok = here if ok is None else jnp.logical_and(ok, here)
        return ok

    def places(d, r):
        dx, dy, dz = d
        rows_from = pl.ds(PAD, Y) if dy == 0 else (pl.ds(TOP - 8, 8) if dy > 0 else pl.ds(PAD, 8))
        rows_to = pl.ds(PAD, Y) if dy == 0 else (pl.ds(0, 8) if dy > 0 else pl.ds(TOP, 8))
        if dz == 0:
            if dx == 0:
                return V[r].at[pl.ds(1, X), rows_from], V[r].at[pl.ds(1, X), rows_to]
            fx, tx = (X, 0) if dx > 0 else (1, X + 1)
            return V[r].at[fx, rows_from], V[r].at[tx, rows_to]
        side = 0 if dz > 0 else 1
        if dx == 0 and dy == 0:
            return PZ.at[r, side], ZR.at[r, side]
        if dx == 0:
            return PS.at[r, rows_from], PR.at[r, side, 0 if dy > 0 else 1]
        slot = (0 if dx > 0 else 2) + side
        return ES.at[r], ER.at[r, slot]

    def copy(d, r):
        src, dst = places(d, r)
        m = directions.index(d)
        return pltpu.make_async_remote_copy(
            src_ref=src,
            dst_ref=dst,
            send_sem=send_sem.at[r % 2, m],
            recv_sem=recv_sem.at[r % 2, m],
            device_id=tuple(a + t for a, t in zip(me, d)),
            device_id_type=pl.DeviceIdType.MESH,
        )

    groups = groups_of(sizes)
    near = len(groups) == 1 and max(sizes) <= ROUNDS and sum(n - 1 for n in sizes) <= 2 * ROUNDS - 1

    def offsets(group):
        ranges = [range(n) if i in group else (0,) for i, n in enumerate(sizes)]
        return [t for t in itertools.product(*ranges) if any(t)]

    def partner(t):
        return tuple(lax.rem(m + k, n) for m, k, n in zip(me, t, sizes))

    barrier = pltpu.get_barrier_semaphore()
    greeted = 0
    if not near:
        for group in groups:
            for t in offsets(group):
                pl.semaphore_signal(
                    barrier, inc=1, device_id=partner(t), device_id_type=pl.DeviceIdType.MESH
                )
                greeted += 1
    if near or len(groups) > 1:
        for d in directions:
            pl.when(present(d))(
                lambda d=d: pl.semaphore_signal(
                    barrier,
                    inc=1,
                    device_id=tuple(a + t for a, t in zip(me, d)),
                    device_id_type=pl.DeviceIdType.MESH,
                )
            )
            greeted = greeted + jnp.where(present(d), 1, 0)

    for d in [
        (dx, dy, dz)
        for dx in (-1, 0, 1)
        for dy in (-1, 0, 1)
        for dz in (-1, 0, 1)
        if sum(1 for t in (dx, dy, dz) if t) in (1, 2)
    ]:
        def clear(d=d):
            for r in range(ROUNDS):
                if needed(d, r):
                    _, dst = places(d, r)
                    dst[...] = jnp.zeros(dst.shape, f32)

        if d in directions:
            back = tuple(-t for t in d)
            pl.when(jnp.logical_not(present(back)))(clear)
        else:
            clear()

    for r in range(ROUNDS):
        for a in (0, TOP):
            PS[r, pl.ds(a, PAD), :] = jnp.zeros((PAD, LANES), f32)
    MA[...] = jnp.zeros(MA.shape, f32)

    lane_e = lax.broadcasted_iota(jnp.int32, (YE, LANES), 1)
    lane_8 = lax.broadcasted_iota(jnp.int32, (T8, LANES), 1)
    row_8 = lax.broadcasted_iota(jnp.int32, (T8, LANES), 0)
    even = lane_e % 2 == 0
    ends = jnp.logical_or(lane_8 == 0, lane_8 == LANES - 1)
    inner = lane_8 < LANES - 1
    tiles = [PAD + T8 * k for k in range(KT)]

    def look(c, index):
        return jnp.take_along_axis(tables[c], index, axis=0, mode="promise_in_bounds")

    def look_known(values, components):
        index = jnp.maximum(values.astype(jnp.int32) - 1, 0)
        hit = values > 0.0
        return [jnp.where(hit, look(c, index), 0.0) for c in components]

    half = LANES // 2
    offs = (0, 1, half, half + 1)
    slots_of = [jnp.logical_and(lane_8 % 2 == off % 2, (lane_8 < half) == (off < half)) for off in offs]

    def send(d, r):
        if d in directions and needed(d, r):
            pl.when(present(d))(lambda: copy(d, r).start())

    def start_x(r, plane):
        tile = jnp.zeros((T8, LANES), f32)
        for col, (x, at) in enumerate(((0, 0), (0, LANES - 1), (X - 1, 0), (X - 1, LANES - 1))):
            for k in range(KT):
                to = col * KT + k
                part = plane(x, k)
                tile = jnp.where(lane_8 == to, pltpu.roll(part, (to - at) % LANES, 1), tile)
        ES[r] = tile
        for d in directions:
            if d[0]:
                send(d, r)

    def start_rest(r):
        for d in sorted(directions, key=lambda d: (-abs(d[2]), abs(d[1]))):
            if not d[0]:
                send(d, r)

    def wait_sent(r):
        for d in directions:
            if needed(d, r):
                pl.when(present(d))(lambda d=d: copy(d, r).wait_send())

    def wait(r):
        if r:
            wait_sent(r - 1)
        for d in directions:
            if needed(d, r):
                back = tuple(-t for t in d)
                pl.when(present(back))(lambda d=d: copy(d, r).wait_recv())

    def spread(r):
        for side in range(2):
            if side == 0 and r == ROUNDS - 1:
                continue
            for t in range(KT // 4):
                tile = None
                for j, off in enumerate(offs):
                    part = PS[r, pl.ds(PAD + T8 * (4 * t + j), T8), :]
                    part = pltpu.roll(part, (off + 1 - side) % LANES, 1) if off + 1 - side else part
                    tile = part if tile is None else jnp.where(slots_of[j], part, tile)
                PZ[r, side, pl.ds(T8 * t, T8), :] = tile

    def build_halo(r):
        valid = jnp.logical_or(lane_8 <= 2 * (X - 1), lane_8 == LANES - 1)
        even = lane_8 % 2 == 0
        last = r == ROUNDS - 1

        def join(low, high):
            return jnp.where(valid, jnp.where(even, 0.0 if last else low, high), 0.0)

        for i, a in enumerate((0, TOP)):
            low = None if last else pltpu.roll(PR[r, 0, i], 1, 1)
            HB[pl.ds(a, T8), :] = join(low, pltpu.roll(PR[r, 1, i], LANES - 1, 1))
        for k in range(KT):
            t, off = pl.ds(T8 * (k // 4), T8), offs[k % 4]
            low = None if last else pltpu.roll(ZR[r, 0, t, :], (LANES - off) % LANES, 1)
            high = pltpu.roll(ZR[r, 1, t, :], LANES - 1 - off, 1)
            HB[pl.ds(PAD + T8 * k, T8), :] = join(low, high)
        targets = (((LANES - 2), 3), ((LANES - 3), 2), (2 * X, 1), (2 * X - 1, 0))
        slots = (1, 3) if last else (0, 1, 2, 3)
        got = {slot: ER[r, slot] for slot in slots}
        for k in range(KT):
            rows = pl.ds(PAD + T8 * k, T8)
            part = HB[rows, :]
            for slot in slots:
                target, col = targets[slot]
                at = col * KT + k
                part = jnp.where(
                    lane_8 == target, pltpu.roll(got[slot], (target - at) % LANES, 1), part
                )
            HB[rows, :] = part

    def zm(a):
        return pltpu.roll(a, 1, 1)

    def zp(a):
        return pltpu.roll(a, LANES - 1, 1)

    def unpack(part, x):
        return jnp.where(ends, pltpu.roll(part, lax.rem(LANES - 2 * x, LANES), 1), 0.0)

    def pack(r, plane):
        for k in range(KT):
            tile = plane(0, k)
            for x in range(1, X):
                here = jnp.logical_and(lane_8 >= 2 * x - 1, inner)
                tile = jnp.where(here, pltpu.roll(plane(x, k), 2 * x, 1), tile)
            PS[r, pl.ds(PAD + T8 * k, T8), :] = tile
        spread(r)

    def label_tile(x, k):
        return (lab[x, pl.ds(T8 * k, T8), :] + 1).astype(f32)

    def field_tile(r):
        return lambda x, k: V[r][x + 1, pl.ds(PAD + T8 * k, T8), :]

    with scope("labwait"):
        lab_copy.wait()
        rhs_copy.start()

    with scope("conv"):
        for x in (0, X - 1):
            for k in range(KT):
                V[0][x + 1, pl.ds(PAD + T8 * k, T8), :] = label_tile(x, k)

        for x in range(1, X - 1):
            for k in (0, KT - 1):
                V[0][x + 1, pl.ds(PAD + T8 * k, T8), :] = label_tile(x, k)

    with scope("barrier"):
        pl.semaphore_wait(barrier, greeted)
    with scope("start0"):
        start_x(0, label_tile)
    with scope("pack0"):
        pack(0, label_tile)
    with scope("start_0"):
        start_rest(0)

    cond_copy.wait()
    scale = (0.5, 0.5, 0.5, 0.25, 0.25, 0.25, 1.0)
    count = cond.shape[1]
    tables = []
    for c in range(7):
        table = jnp.zeros((T8, LANES), f32)
        for k in range(count):
            table = jnp.where(row_8 == k, cond[c, k] * scale[c], table)
        tables.append(table)


    with scope("sigma_own"):
        @pl.loop(0, X, unroll=4)
        def _(x):
            for a in tiles:
                index = lab[x, pl.ds(a - PAD, T8), :]
                for c in range(6):
                    S[c, x + 1, pl.ds(a, T8), :] = look(c, index)

    with scope("wait0"):
        wait(0)

    with scope("sigma_halo"):
        for x in (0, X + 1):
            for a in range(0, YE, T8):
                rows = pl.ds(a, T8)
                for c, s in enumerate(look_known(V[0][x, rows, :], range(6))):
                    S[c, x, rows, :] = s

        @pl.loop(1, X + 1, unroll=4)
        def _(x):
            for a in (0, TOP):
                rows = pl.ds(a, T8)
                for c, s in enumerate(look_known(V[0][x, rows, :], range(6))):
                    S[c, x, rows, :] = s

        build_halo(0)
        for a in range(0, YE, T8):
            rows = pl.ds(a, T8)
            for i, s in enumerate(look_known(HB[rows, :], (2, 4, 5))):
                HS[i, rows, :] = s
            for i, s in enumerate(look_known(PS[0, rows, :], (2, 4, 5))):
                PG[i, rows, :] = s
        CP[...] = HS[0]
        rhs_copy.wait()

    def coefficients(p):
        for a in [0] + tiles:
            rows, up = pl.ds(a, T8), pl.ds(a + 1, T8)
            s1, s1u = S[1, p, rows, :], S[1, p, up, :]
            s3, s3u = S[3, p, rows, :], S[3, p, up, :]
            t3, t3u = S[3, p + 1, rows, :], S[3, p + 1, up, :]
            s5, s5u = S[5, p, rows, :], S[5, p, up, :]
            F[1, p, rows, :] = s1 + s1u
            F[3, p, rows, :] = s3 + t3u
            F[4, p, rows, :] = t3 + s3u
            F[7, p, rows, :] = jnp.where(inner, s5 + zp(s5u), 0.0)
            F[8, p, rows, :] = jnp.where(inner, s5u + zp(s5), 0.0)
            if a:
                s2 = S[2, p, rows, :]
                s4, t4 = S[4, p, rows, :], S[4, p + 1, rows, :]
                F[0, p, rows, :] = S[0, p, rows, :] + S[0, p + 1, rows, :]
                F[2, p, rows, :] = jnp.where(inner, s2 + zp(s2), 0.0)
                F[5, p, rows, :] = jnp.where(inner, s4 + zp(t4), 0.0)
                F[6, p, rows, :] = jnp.where(inner, t4 + zp(s4), 0.0)

    def diagonal(x, total):
        p = x + 1
        for a in tiles:
            rows, up, down = pl.ds(a, T8), pl.ds(a + 1, T8), pl.ds(a - 1, T8)
            own = pl.ds(a - PAD, T8)
            s2 = S[2, p, rows, :]
            face = pltpu.roll(CP[rows, :], lax.rem(LANES - 2 * x, LANES), 1)
            diag = look(6, lab[x, own, :]) + 2.0 * ((S[0, p, rows, :] + S[1, p, rows, :]) + s2)
            diag = diag + (S[0, p - 1, rows, :] + S[0, p + 1, rows, :])
            diag = diag + (S[1, p, down, :] + S[1, p, up, :])
            diag = diag + (jnp.where(lane_8 == 0, face, zm(s2)) + jnp.where(inner, zp(s2), face))
            inverse = 1.0 / diag
            DI[x, own, :] = inverse
            r0 = rhs[x, own, :]
            w = r0 * inverse
            V[1][p, rows, :] = w
            total = total + r0 * w
        return total

    def zero():
        return jnp.zeros((T8, LANES), f32)

    with scope("diag_x"):
        MA[0] = diagonal(X - 1, diagonal(0, zero()))
    with scope("startx_1"):
        start_x(1, field_tile(1))
    with scope("diag"):
        width = group_size(X - 2, 6)

        @pl.loop(0, (X - 2) // width)
        def _(g):
            total = zero()
            for i in range(width):
                total = diagonal(1 + g * width + i, total)
            MA[0] = MA[0] + total

    with scope("pack_1"):
        pack(1, field_tile(1))
    with scope("start_1"):
        start_rest(1)
    with scope("coef"):
        width = group_size(X + 1, 4)

        @pl.loop(0, (X + 1) // width)
        def _(g):
            for i in range(width):
                coefficients(g * width + i)

    def planes(r, x0, width):
        odd, evn = zero(), zero()
        field, nxt = V[r], V[r + 1]
        for a in tiles:
            rows, up, down = pl.ds(a, T8), pl.ds(a + 1, T8), pl.ds(a - 1, T8)
            own = pl.ds(a - PAD, T8)
            halo = CP[rows, :]
            m, mu, md = field[x0, rows, :], field[x0, up, :], field[x0, down, :]
            v, vu, vd = field[x0 + 1, rows, :], field[x0 + 1, up, :], field[x0 + 1, down, :]
            tv = zp(v)
            acc = F[0, x0, rows, :] * m + F[3, x0, down, :] * md
            acc = acc - F[4, x0, rows, :] * mu - F[6, x0, rows, :] * zp(m)
            accs = F[5, x0, rows, :] * m
            for i in range(width):
                x = x0 + i
                p = x + 1
                n, nu, nd = field[p + 1, rows, :], field[p + 1, up, :], field[p + 1, down, :]
                tn = zp(n)
                f0 = F[0, p, rows, :]
                f2 = F[2, p, rows, :]
                f3, f3d = F[3, p, rows, :], F[3, p, down, :]
                f4, f4d = F[4, p, rows, :], F[4, p, down, :]
                f5, f6 = F[5, p, rows, :], F[6, p, rows, :]
                f7, f7d = F[7, p, rows, :], F[7, p, down, :]
                f8, f8d = F[8, p, rows, :], F[8, p, down, :]
                s = (accs + f2 * v) + (f7d * vd - f8 * vu) - f6 * n
                q = (acc + f0 * n) + (F[1, p, rows, :] * vu + F[1, p, down, :] * vd)
                q = q + (f3 * nu - f4d * nd) + (f2 * tv + f5 * tn)
                q = q + (f7 * zp(vu) - f8d * zp(vd))
                q = q + zm(s) + unpack(halo, x)
                acc = (f0 * v + f3d * vd) - (f4 * vu + f6 * tv)
                accs = f5 * v
                odd = odd + v * q
                w = q * DI[x, own, :]
                evn = evn + w * q
                nxt[p, rows, :] = w
                v, vu, vd, tv = n, nu, nd, tn
        return odd, evn

    def pairs(r, x0, width):
        total = zero()
        field = V[r]
        for a in tiles:
            rows, up = pl.ds(a, T8), pl.ds(a + 1, T8)
            v, vu = field[x0 + 1, rows, :], field[x0 + 1, up, :]
            tv, tvu = zp(v), zp(vu)
            for i in range(width):
                p = x0 + i + 1
                n, nu = field[p + 1, rows, :], field[p + 1, up, :]
                tn, tnu = zp(n), zp(nu)
                a0 = (F[0, p, rows, :] * n + F[1, p, rows, :] * vu) + (F[3, p, rows, :] * nu + F[5, p, rows, :] * tn)
                a0 = a0 + F[7, p, rows, :] * tvu
                a1 = F[2, p, rows, :] * v - F[6, p, rows, :] * n - F[8, p, rows, :] * vu
                total = total + v * a0 + (tv * a1 - (F[4, p, rows, :] * n) * vu)
                v, vu, tv, tvu = n, nu, tn, tnu
        return total

    def along_x(a):
        return pltpu.roll(a, LANES - 2, 1) - pltpu.roll(a, 2, 1)

    def along_y(a):
        return pltpu.roll(a, YE - 1, 0) - pltpu.roll(a, 1, 0)

    sign = jnp.where(even, f32(-1.0), f32(1.0))
    for step in range(ITERS):
        r = step + 1
        last = step + 1 == ITERS
        if step:
            with scope(f"pack_{r}"):
                pack(r, field_tile(r))
            with scope(f"start_{r}"):
                start_rest(r)
        if last:
            with scope("early_sums"):
                tile = zero()
                for k in range(MOMENTS - 1):
                    value = jnp.sum(jnp.sum(MA[k], axis=0, keepdims=True), axis=1, keepdims=True)
                    tile = jnp.where(lane_8 == k, value, tile)
                CP[pl.ds(0, T8), :] = tile
        with scope(f"wait_{r}"):
            wait(r)
        with scope(f"halo_{r}"):
            build_halo(r)
            h = HB[...]
            full = (PG[0] + HS[0]) * h + sign * (
                PG[1] * along_x(h) + along_x(HS[1] * h) + PG[2] * along_y(h) + along_y(HS[2] * h)
            )
            CP[pl.ds(PAD, Y), :] = full[PAD:TOP]
        if last:
            break
        with scope(f"edge_{r}"):
            o0, e0 = planes(r, 0, 1)
            o1, e1 = planes(r, X - 1, 1)
            MA[2 * step + 1] = o0 + o1
            MA[2 * step + 2] = e0 + e1
        with scope(f"startx_{r + 1}"):
            start_x(r + 1, field_tile(r + 1))
        with scope(f"matvec_{r}"):
            width = group_size(X - 2, 6)

            @pl.loop(0, (X - 2) // width)
            def _(g):
                odd, evn = planes(r, 1 + g * width, width)
                MA[2 * step + 1] = MA[2 * step + 1] + odd
                MA[2 * step + 2] = MA[2 * step + 2] + evn

    with scope("pairs"):
        width = group_size(X, 8)
        mine = jnp.logical_and(lane_8 % 2 == 1, jnp.logical_or(lane_8 < 2 * (X - 1), lane_8 == LANES - 1))
        total = zero()
        for a in tiles:
            rows = pl.ds(a, T8)
            total = total + jnp.where(mine, PS[ROUNDS - 1, rows, :] * CP[rows, :], 0.0)
        MA[MOMENTS - 1] = total

        @pl.loop(0, X // width)
        def _(g):
            MA[MOMENTS - 1] = MA[MOMENTS - 1] + pairs(ROUNDS - 1, g * width, width)

    def leave():
        wait_sent(ROUNDS - 1)

        @pl.loop(0, X, unroll=4)
        def _(x):
            for i in range(ITERS):
                for k in range(KT):
                    W[i, x, pl.ds(T8 * k, T8), :] = V[i + 1][x + 1, pl.ds(PAD + T8 * k, T8), :]

    with scope("allreduce"):
        value = jnp.sum(jnp.sum(MA[MOMENTS - 1], axis=0, keepdims=True), axis=1, keepdims=True)
        tile = jnp.where(lane_8 == MOMENTS - 1, 2.0 * value, CP[pl.ds(0, T8), :])
        for order, group in enumerate(groups):
            slot = 0
            members = 1
            for i in group:
                slot = slot * sizes[i] + me[i]
                members *= sizes[i]
            RS[order] = tile[0:1]
            others = offsets(group)
            for t in others:
                pltpu.make_async_remote_copy(
                    src_ref=RS.at[order],
                    dst_ref=RR.at[order, slot],
                    send_sem=ar_send.at[order],
                    recv_sem=ar_recv.at[order],
                    device_id=partner(t),
                    device_id_type=pl.DeviceIdType.MESH,
                ).start()
            RR[order, slot] = tile[0:1]
            if order == 0:
                leave()
            sent = RR.at[order, pl.ds(0, len(others))]
            pltpu.make_async_copy(sent, sent, ar_send.at[order]).wait()
            pltpu.make_async_copy(sent, sent, ar_recv.at[order]).wait()
            parts = [RR[order, t] for t in range(members)]
            while len(parts) > 1:
                parts = [sum(parts[i + 1 : i + 2], parts[i]) for i in range(0, len(parts), 2)]
            tile = jnp.broadcast_to(parts[0], (T8, LANES))

    n0, n1, n2, n3, n4, n5 = (
        jnp.sum(jnp.where(lane_8 == k, tile, 0.0)[0:1], axis=1, keepdims=True) for k in range(MOMENTS)
    )

    def inverse_of(d):
        return jnp.where(d > 0.0, 1.0 / d, 0.0)

    g00, g01, g02, g12, g22 = n0 - n1, n1 - n2, n2 - n3, n3 - n4, n4 - n5
    i0 = 1.0 / g00
    l1, l2 = g01 * i0, g02 * i0
    i1 = inverse_of(g02 - l1 * g01)
    e = g12 - l2 * g01
    l21 = e * i1
    i2 = inverse_of(g22 - l2 * g02 - l21 * e)
    y1 = n1 - l1 * n0
    y2 = n2 - l2 * n0 - l21 * y1
    c2 = y2 * i2
    c1 = y1 * i1 - l21 * c2
    c0 = n0 * i0 - l1 * c1 - l2 * c2

    for i, c in enumerate((c0, c1, c2)):
        C[pl.ds(i, 1), :] = jnp.broadcast_to(c, (1, LANES))


def combine(W, C, out, part, sem):
    X, Y, Z = out.shape
    rows = C[...]
    c = [jnp.broadcast_to(rows[i : i + 1], (T8, Z)) for i in range(ITERS)]
    pieces = sem.shape[0]
    width = X // pieces
    copies = []
    for g in range(pieces):
        @pl.loop(g * width, (g + 1) * width, unroll=4)
        def _(x):
            for k in range(Y // T8):
                own = pl.ds(T8 * k, T8)
                part[x, own, :] = (c[0] * W[0, x, own, :] + c[1] * W[1, x, own, :]) + c[2] * W[2, x, own, :]

        block = pl.ds(g * width, width)
        copies.append(pltpu.make_async_copy(part.at[block], out.at[block], sem.at[g]))
        copies[-1].start()
    for piece in copies:
        piece.wait()


def solution(mesh):
    sizes = tuple(mesh.shape[a] for a in AXES)

    def local(labels, conductivity, right_side):
        X, Y, Z = right_side.shape
        YE = Y + 2 * PAD
        f32 = jnp.float32
        vmem = pltpu.VMEM
        orders = len(groups_of(sizes))
        fields, factors = pl.pallas_call(
            functools.partial(kernel, sizes),
            out_shape=(vmem((ITERS, X, Y, Z), f32), vmem((T8, Z), f32)),
            in_specs=[
                pl.BlockSpec(memory_space=pl.ANY),
                pl.BlockSpec(memory_space=pl.ANY),
                pl.BlockSpec(memory_space=pl.ANY),
            ],
            out_specs=[pl.BlockSpec(memory_space=vmem)] * 2,
            scratch_shapes=[
                vmem((X, Y, Z), jnp.int32),
                pltpu.SMEM(conductivity.shape, f32),
                vmem((X, Y, Z), f32),
                vmem((X + 2, YE, Z), f32),
                vmem((X + 2, YE, Z), f32),
                vmem((X + 2, YE, Z), f32),
                vmem((X + 2, YE, Z), f32),
                vmem((6, X + 2, YE, Z), f32),
                vmem((9, X + 1, YE, Z), f32),
                vmem((X, Y, Z), f32),
                vmem((ROUNDS, YE, Z), f32),
                vmem((ROUNDS, 2, Y // 4, Z), f32),
                vmem((ROUNDS, 2, 2, T8, Z), f32),
                vmem((ROUNDS, 2, Y // 4, Z), f32),
                vmem((ROUNDS, 8, Z), f32),
                vmem((ROUNDS, 4, 8, Z), f32),
                vmem((YE, Z), f32),
                vmem((3, YE, Z), f32),
                vmem((3, YE, Z), f32),
                vmem((YE, Z), f32),
                vmem((MOMENTS, 8, Z), f32),
                vmem((2, 1, Z), f32),
                vmem((2, 32, 1, Z), f32),
                pltpu.SemaphoreType.DMA((2, 18)),
                pltpu.SemaphoreType.DMA((2, 18)),
                pltpu.SemaphoreType.DMA((orders,)),
                pltpu.SemaphoreType.DMA((orders,)),
                pltpu.SemaphoreType.DMA((3,)),
            ],
            compiler_params=pltpu.CompilerParams(
                collective_id=0, has_side_effects=True, vmem_limit_bytes=60 * 1024 * 1024
            ),
        )(labels, conductivity, right_side)
        return pl.pallas_call(
            combine,
            out_shape=jax.ShapeDtypeStruct((X, Y, Z), f32),
            in_specs=[pl.BlockSpec(memory_space=vmem)] * 2,
            out_specs=pl.BlockSpec(memory_space=pl.ANY),
            scratch_shapes=[vmem((X, Y, Z), f32), pltpu.SemaphoreType.DMA((group_size(X, 4),))],
            compiler_params=pltpu.CompilerParams(vmem_limit_bytes=8 * 1024 * 1024),
        )(fields, factors)

    return jax.shard_map(
        local,
        mesh=mesh,
        in_specs=(P("gx", "gy", "gz"), P(), P("gx", "gy", "gz")),
        out_specs=P("gx", "gy", "gz"),
        check_vma=False,
    )
```

```python
import functools
import itertools
import math
import jax
import jax.numpy as jnp
from jax import lax
from jax.experimental import pallas as pl
from jax.experimental.pallas import tpu as pltpu
from jax.sharding import PartitionSpec as P

ITERS = 3
AXES = ("gx", "gy", "gz")
ROUNDS = ITERS + 1
MOMENTS = 2 * ITERS
LANES = 128
PAD = 8
T8 = 8


def group_size(n, most):
    return max(u for u in range(1, most + 1) if n % u == 0)


def groups_of(sizes):
    return [(0, 1, 2)] if math.prod(sizes) <= 32 else [(0, 1), (2,)]


def kernel(
    sizes, lab_hbm, cond_hbm, rhs_hbm, W, C, lab, cond, rhs, V0, V1, V2, V3, S, F, DI, PS, PZ, PR, ZR, ES, ER, HB, HS, PG, CP,
    DP, MA, RS, RR, send_sem, recv_sem, ar_send, ar_recv, in_sem,
):
    V = (V0, V1, V2, V3)
    X, Y, Z = rhs.shape
    end_copies = []
    for i, x in enumerate((0, X - 1)):
        end_copies.append(pltpu.make_async_copy(lab_hbm.at[x], lab.at[x], in_sem.at[3 + i]))
        end_copies[-1].start()
    inside = pl.ds(1, X - 2)
    lab_copy = pltpu.make_async_copy(lab_hbm.at[inside], lab.at[inside], in_sem.at[0])
    lab_copy.start()
    cond_copy = pltpu.make_async_copy(cond_hbm, cond, in_sem.at[2])
    cond_copy.start()
    rhs_copy = pltpu.make_async_copy(rhs_hbm, rhs, in_sem.at[1])
    YE = Y + 2 * PAD
    TOP = PAD + Y
    KT = Y // T8
    me = [lax.axis_index(a) for a in AXES]
    f32 = jnp.float32
    scope = jax.named_scope

    directions = []
    for dx in (-1, 0, 1):
        for dy in (-1, 0, 1):
            for dz in (-1, 0, 1):
                d = (dx, dy, dz)
                live = sum(1 for t in d if t)
                if live in (1, 2) and all(n > 1 for t, n in zip(d, sizes) if t):
                    directions.append(d)

    def needed(d, r):
        if r < ROUNDS - 1:
            return True
        if d[2]:
            return d[2] < 0
        return d[0] <= 0 and d[1] <= 0

    def present(d):
        ok = None
        for t, m, n in zip(d, me, sizes):
            if t == 0:
                continue
            here = (m < n - 1) if t > 0 else (m > 0)
            ok = here if ok is None else jnp.logical_and(ok, here)
        return ok

    def places(d, r):
        dx, dy, dz = d
        rows_from = pl.ds(PAD, Y) if dy == 0 else (pl.ds(TOP - 1, 1) if dy > 0 else pl.ds(PAD, 1))
        rows_to = pl.ds(PAD, Y) if dy == 0 else (pl.ds(PAD - 1, 1) if dy > 0 else pl.ds(TOP, 1))
        if dz == 0:
            if dx == 0:
                return V[r].at[pl.ds(1, X), rows_from], V[r].at[pl.ds(1, X), rows_to]
            fx, tx = (X, 0) if dx > 0 else (1, X + 1)
            return V[r].at[fx, rows_from], V[r].at[tx, rows_to]
        side = 0 if dz > 0 else 1
        if dx == 0 and dy == 0:
            return PZ.at[r, side], ZR.at[r, side]
        if dx == 0:
            return PS.at[r, rows_from], PR.at[r, side, 0 if dy > 0 else 1, pl.ds(PAD - 1 if dy > 0 else 0, 1)]
        slot = (0 if dx > 0 else 2) + side
        return ES.at[r], ER.at[r, slot]

    def copy(d, r):
        src, dst = places(d, r)
        m = directions.index(d)
        return pltpu.make_async_remote_copy(
            src_ref=src,
            dst_ref=dst,
            send_sem=send_sem.at[r % 2, m],
            recv_sem=recv_sem.at[r % 2, m],
            device_id=tuple(a + t for a, t in zip(me, d)),
            device_id_type=pl.DeviceIdType.MESH,
        )

    groups = groups_of(sizes)
    near = len(groups) == 1 and max(sizes) <= ROUNDS and sum(n - 1 for n in sizes) <= 2 * ROUNDS - 1

    def offsets(group):
        ranges = [range(n) if i in group else (0,) for i, n in enumerate(sizes)]
        return [t for t in itertools.product(*ranges) if any(t)]

    def partner(t):
        return tuple(lax.rem(m + k, n) for m, k, n in zip(me, t, sizes))

    barrier = pltpu.get_barrier_semaphore()
    greeted = 0
    if not near:
        for group in groups:
            for t in offsets(group):
                pl.semaphore_signal(
                    barrier, inc=1, device_id=partner(t), device_id_type=pl.DeviceIdType.MESH
                )
                greeted += 1
    if near or len(groups) > 1:
        for d in directions:
            pl.when(present(d))(
                lambda d=d: pl.semaphore_signal(
                    barrier,
                    inc=1,
                    device_id=tuple(a + t for a, t in zip(me, d)),
                    device_id_type=pl.DeviceIdType.MESH,
                )
            )
            greeted = greeted + jnp.where(present(d), 1, 0)

    for d in [
        (dx, dy, dz)
        for dx in (-1, 0, 1)
        for dy in (-1, 0, 1)
        for dz in (-1, 0, 1)
        if sum(1 for t in (dx, dy, dz) if t) in (1, 2)
    ]:
        def clear(d=d):
            for r in range(ROUNDS):
                if needed(d, r):
                    _, dst = places(d, r)
                    dst[...] = jnp.zeros(dst.shape, f32)

        if d in directions:
            back = tuple(-t for t in d)
            pl.when(jnp.logical_not(present(back)))(clear)
        else:
            clear()

    for r in range(ROUNDS):
        for a in (0, TOP):
            PS[r, pl.ds(a, PAD), :] = jnp.zeros((PAD, LANES), f32)
    for r in range(ROUNDS):
        for side in range(2):
            PR[r, side, 0, pl.ds(0, PAD - 1), :] = jnp.zeros((PAD - 1, LANES), f32)
            PR[r, side, 1, pl.ds(1, PAD - 1), :] = jnp.zeros((PAD - 1, LANES), f32)
    for x in range(X + 2):
        V[0][x, pl.ds(0, PAD - 1), :] = jnp.zeros((PAD - 1, LANES), f32)
        V[0][x, pl.ds(TOP + 1, PAD - 1), :] = jnp.zeros((PAD - 1, LANES), f32)
    MA[...] = jnp.zeros(MA.shape, f32)

    lane_e = lax.broadcasted_iota(jnp.int32, (YE, LANES), 1)
    lane_8 = lax.broadcasted_iota(jnp.int32, (T8, LANES), 1)
    row_8 = lax.broadcasted_iota(jnp.int32, (T8, LANES), 0)
    even = lane_e % 2 == 0
    ends = jnp.logical_or(lane_8 == 0, lane_8 == LANES - 1)
    inner = lane_8 < LANES - 1
    tiles = [PAD + T8 * k for k in range(KT)]

    def look(c, index):
        return jnp.take_along_axis(tables[c], index, axis=0, mode="promise_in_bounds")

    def look_known(values, components):
        index = jnp.maximum(values.astype(jnp.int32) - 1, 0)
        hit = values > 0.0
        return [jnp.where(hit, look(c, index), 0.0) for c in components]

    half = LANES // 2
    offs = (0, 1, half, half + 1)
    slots_of = [jnp.logical_and(lane_8 % 2 == off % 2, (lane_8 < half) == (off < half)) for off in offs]

    def send(d, r):
        if d in directions and needed(d, r):
            pl.when(present(d))(lambda: copy(d, r).start())

    def start_x(r, plane):
        tile = jnp.zeros((T8, LANES), f32)
        for col, (x, at) in enumerate(((0, 0), (0, LANES - 1), (X - 1, 0), (X - 1, LANES - 1))):
            for k in range(KT):
                to = col * KT + k
                part = plane(x, k)
                tile = jnp.where(lane_8 == to, pltpu.roll(part, (to - at) % LANES, 1), tile)
        ES[r] = tile
        for d in sorted(directions, key=lambda d: (-abs(d[2]), -abs(d[1]))):
            if d[0]:
                send(d, r)

    def start_rest(r):
        for d in sorted(directions, key=lambda d: (-abs(d[2]), -abs(d[1]))):
            if not d[0]:
                send(d, r)

    def wait_sent(r):
        for d in directions:
            if needed(d, r):
                pl.when(present(d))(lambda d=d: copy(d, r).wait_send())

    def wait(r):
        if r:
            wait_sent(r - 1)
        for d in directions:
            if needed(d, r):
                back = tuple(-t for t in d)
                pl.when(present(back))(lambda d=d: copy(d, r).wait_recv())

    def spread(r):
        for side in range(2):
            if side == 0 and r == ROUNDS - 1:
                continue
            for t in range(KT // 4):
                tile = None
                for j, off in enumerate(offs):
                    part = PS[r, pl.ds(PAD + T8 * (4 * t + j), T8), :]
                    part = pltpu.roll(part, (off + 1 - side) % LANES, 1) if off + 1 - side else part
                    tile = part if tile is None else jnp.where(slots_of[j], part, tile)
                PZ[r, side, pl.ds(T8 * t, T8), :] = tile

    def build_halo(r):
        valid = jnp.logical_or(lane_8 <= 2 * (X - 1), lane_8 == LANES - 1)
        even = lane_8 % 2 == 0
        last = r == ROUNDS - 1

        def join(low, high):
            return jnp.where(valid, jnp.where(even, 0.0 if last else low, high), 0.0)

        for i, a in enumerate((0, TOP)):
            low = None if last else pltpu.roll(PR[r, 0, i], 1, 1)
            HB[pl.ds(a, T8), :] = join(low, pltpu.roll(PR[r, 1, i], LANES - 1, 1))
        for k in range(KT):
            t, off = pl.ds(T8 * (k // 4), T8), offs[k % 4]
            low = None if last else pltpu.roll(ZR[r, 0, t, :], (LANES - off) % LANES, 1)
            high = pltpu.roll(ZR[r, 1, t, :], LANES - 1 - off, 1)
            HB[pl.ds(PAD + T8 * k, T8), :] = join(low, high)
        targets = (((LANES - 2), 3), ((LANES - 3), 2), (2 * X, 1), (2 * X - 1, 0))
        slots = (1, 3) if last else (0, 1, 2, 3)
        got = {slot: ER[r, slot] for slot in slots}
        for k in range(KT):
            rows = pl.ds(PAD + T8 * k, T8)
            part = HB[rows, :]
            for slot in slots:
                target, col = targets[slot]
                at = col * KT + k
                part = jnp.where(
                    lane_8 == target, pltpu.roll(got[slot], (target - at) % LANES, 1), part
                )
            HB[rows, :] = part

    def zm(a):
        return pltpu.roll(a, 1, 1)

    def zp(a):
        return pltpu.roll(a, LANES - 1, 1)

    def unpack(part, x):
        return jnp.where(ends, pltpu.roll(part, lax.rem(LANES - 2 * x, LANES), 1), 0.0)

    def packed(plane, k, first, last):
        tile = None
        for x in range(first, last):
            part = pltpu.roll(plane(x, k), 2 * x, 1) if x else plane(x, k)
            tile = part if tile is None else jnp.where(jnp.logical_and(lane_8 >= 2 * x - 1, inner), part, tile)
        return tile

    def pack(r, plane):
        for k in range(KT):
            PS[r, pl.ds(PAD + T8 * k, T8), :] = packed(plane, k, 0, X)

    def label_tile(x, k):
        return (lab[x, pl.ds(T8 * k, T8), :] + 1).astype(f32)

    def field_tile(r):
        return lambda x, k: V[r][x + 1, pl.ds(PAD + T8 * k, T8), :]

    with scope("endwait"):
        for end_copy in end_copies:
            end_copy.wait()
    with scope("conv"):
        for x in (0, X - 1):
            for k in range(KT):
                V[0][x + 1, pl.ds(PAD + T8 * k, T8), :] = label_tile(x, k)
    with scope("barrier"):
        pl.semaphore_wait(barrier, greeted)
    with scope("start0"):
        start_x(0, label_tile)
    with scope("labwait"):
        lab_copy.wait()
        rhs_copy.start()
    with scope("pack0"):
        for x in range(1, X - 1):
            for k in (0, KT - 1):
                V[0][x + 1, pl.ds(PAD + T8 * k, T8), :] = label_tile(x, k)
        pack(0, label_tile)
        spread(0)
    with scope("start_0"):
        start_rest(0)

    cond_copy.wait()
    scale = (0.5, 0.5, 0.5, 0.25, 0.25, 0.25, 1.0)
    count = cond.shape[1]
    tables = []
    for c in range(7):
        table = jnp.zeros((T8, LANES), f32)
        for k in range(count):
            table = jnp.where(row_8 == k, cond[c, k] * scale[c], table)
        tables.append(table)


    with scope("sigma_own"):
        @pl.loop(0, X, unroll=4)
        def _(x):
            for a in tiles:
                index = lab[x, pl.ds(a - PAD, T8), :]
                for c in range(6):
                    S[c, x + 1, pl.ds(a, T8), :] = look(c, index)

    def coefficients(p, where, inside=True):
        for a in where:
            rows, up = pl.ds(a, T8), pl.ds(a + 1, T8)
            s3, s3u = S[3, p, rows, :], S[3, p, up, :]
            t3, t3u = S[3, p + 1, rows, :], S[3, p + 1, up, :]
            F[3, p, rows, :] = s3 + t3u
            F[4, p, rows, :] = t3 + s3u
            if inside:
                s5, s5u = S[5, p, rows, :], S[5, p, up, :]
                F[1, p, rows, :] = S[1, p, rows, :] + S[1, p, up, :]
                F[7, p, rows, :] = jnp.where(inner, s5 + zp(s5u), 0.0)
                F[8, p, rows, :] = jnp.where(inner, s5u + zp(s5), 0.0)
            if a:
                s4, t4 = S[4, p, rows, :], S[4, p + 1, rows, :]
                F[0, p, rows, :] = S[0, p, rows, :] + S[0, p + 1, rows, :]
                F[5, p, rows, :] = jnp.where(inner, s4 + zp(t4), 0.0)
                F[6, p, rows, :] = jnp.where(inner, t4 + zp(s4), 0.0)
                if inside:
                    s2 = S[2, p, rows, :]
                    F[2, p, rows, :] = jnp.where(inner, s2 + zp(s2), 0.0)

    with scope("coef_in"):
        width = group_size(X - 2, 3)

        @pl.loop(0, (X - 2) // width)
        def _(g):
            for i in range(width):
                coefficients(1 + g * width + i, tiles[:-1])
        coefficients(X - 1, tiles[:-1])

    with scope("wait0"):
        wait(0)

    halo_tiles = [pl.ds(a, T8) for a in range(0, YE, T8)]

    def sigma_halo(x, rows, components):
        for c, s in zip(components, look_known(V[0][x, rows, :], components)):
            S[c, x, rows, :] = s

    with scope("sigma_halo"):
        build_halo(0)
        for rows in halo_tiles:
            (HS[0, rows, :],) = look_known(HB[rows, :], (2,))
        CP[...] = HS[0]
        for x in (0, X + 1):
            for a in tiles:
                sigma_halo(x, pl.ds(a, T8), (0,))
        for x in range(1, X + 1):
            for a in (0, TOP):
                sigma_halo(x, pl.ds(a, T8), (1,))
        rhs_copy.wait()

    def diagonal(x, total):
        p = x + 1
        for a in tiles:
            rows, up, down = pl.ds(a, T8), pl.ds(a + 1, T8), pl.ds(a - 1, T8)
            own = pl.ds(a - PAD, T8)
            s2 = S[2, p, rows, :]
            face = pltpu.roll(CP[rows, :], lax.rem(LANES - 2 * x, LANES), 1)
            diag = look(6, lab[x, own, :]) + 2.0 * ((S[0, p, rows, :] + S[1, p, rows, :]) + s2)
            diag = diag + (S[0, p - 1, rows, :] + S[0, p + 1, rows, :])
            diag = diag + (S[1, p, down, :] + S[1, p, up, :])
            diag = diag + (jnp.where(lane_8 == 0, face, zm(s2)) + jnp.where(inner, zp(s2), face))
            inverse = 1.0 / diag
            DI[x, own, :] = inverse
            r0 = rhs[x, own, :]
            w = r0 * inverse
            V[1][p, rows, :] = w
            total = total + r0 * w
        return total

    def zero():
        return jnp.zeros((T8, LANES), f32)

    with scope("diag_x"):
        MA[0] = diagonal(X - 1, diagonal(0, zero()))
    with scope("startx_1"):
        start_x(1, field_tile(1))
    with scope("diag"):
        width = group_size(X - 2, 6)

        @pl.loop(0, (X - 2) // width)
        def _(g):
            total = zero()
            for i in range(width):
                total = diagonal(1 + g * width + i, total)
            MA[0] = MA[0] + total

    with scope("pack_1"):
        pack(1, field_tile(1))
        spread(1)
    with scope("start_1"):
        start_rest(1)
    with scope("coef"):
        for rows in halo_tiles:
            for i, s in enumerate(look_known(HB[rows, :], (4, 5))):
                HS[i + 1, rows, :] = s
            for i, s in enumerate(look_known(PS[0, rows, :], (2, 4, 5))):
                PG[i, rows, :] = s
            for x in (0, X + 1):
                sigma_halo(x, rows, (3, 4))

        @pl.loop(1, X + 1, unroll=4)
        def _(x):
            for a in (0, TOP):
                sigma_halo(x, pl.ds(a, T8), (3, 5))

        coefficients(0, [0] + tiles, False)
        coefficients(X, [0] + tiles)
        coefficients(X - 1, (0, TOP - T8))
        width = group_size(X - 2, 10)

        @pl.loop(0, (X - 2) // width)
        def _(g):
            for i in range(width):
                coefficients(1 + g * width + i, (0, TOP - T8))

    def planes(r, x0, width, where, ready=True):
        odd, evn = zero(), zero()
        field, nxt = V[r], V[r + 1]
        for a in where:
            rows, up, down = pl.ds(a, T8), pl.ds(a + 1, T8), pl.ds(a - 1, T8)
            own = pl.ds(a - PAD, T8)
            halo = CP[rows, :] if ready else None
            m, mu, md = field[x0, rows, :], field[x0, up, :], field[x0, down, :]
            v, vu, vd = field[x0 + 1, rows, :], field[x0 + 1, up, :], field[x0 + 1, down, :]
            tv = zp(v)
            acc = F[0, x0, rows, :] * m + F[3, x0, down, :] * md
            acc = acc - F[4, x0, rows, :] * mu - F[6, x0, rows, :] * zp(m)
            accs = F[5, x0, rows, :] * m
            for i in range(width):
                x = x0 + i
                p = x + 1
                n, nu, nd = field[p + 1, rows, :], field[p + 1, up, :], field[p + 1, down, :]
                tn = zp(n)
                f0 = F[0, p, rows, :]
                f2 = F[2, p, rows, :]
                f3, f3d = F[3, p, rows, :], F[3, p, down, :]
                f4, f4d = F[4, p, rows, :], F[4, p, down, :]
                f5, f6 = F[5, p, rows, :], F[6, p, rows, :]
                f7, f7d = F[7, p, rows, :], F[7, p, down, :]
                f8, f8d = F[8, p, rows, :], F[8, p, down, :]
                s = (accs + f2 * v) + (f7d * vd - f8 * vu) - f6 * n
                q = (acc + f0 * n) + (F[1, p, rows, :] * vu + F[1, p, down, :] * vd)
                q = q + (f3 * nu - f4d * nd) + (f2 * tv + f5 * tn)
                q = q + (f7 * zp(vu) - f8d * zp(vd))
                q = q + zm(s)
                if ready:
                    q = q + unpack(halo, x)
                acc = (f0 * v + f3d * vd) - (f4 * vu + f6 * tv)
                accs = f5 * v
                odd = odd + v * q
                w = q * DI[x, own, :]
                evn = evn + w * q
                nxt[p, rows, :] = w
                v, vu, vd, tv = n, nu, nd, tn
        return odd, evn

    def settle(r, x0, width, where):
        odd, evn = zero(), zero()
        for a in where:
            rows, own = pl.ds(a, T8), pl.ds(a - PAD, T8)
            halo = CP[rows, :]
            for i in range(width):
                x = x0 + i
                c = unpack(halo, x)
                w = V[r + 1][x + 1, rows, :]
                full = w + c * DI[x, own, :]
                V[r + 1][x + 1, rows, :] = full
                odd = odd + c * V[r][x + 1, rows, :]
                evn = evn + c * (w + full)
        return odd, evn

    def pairs(r, x0, width, where):
        total = zero()
        field = V[r]
        for a in where:
            rows, up = pl.ds(a, T8), pl.ds(a + 1, T8)
            v, vu = field[x0 + 1, rows, :], field[x0 + 1, up, :]
            tv, tvu = zp(v), zp(vu)
            for i in range(width):
                p = x0 + i + 1
                n, nu = field[p + 1, rows, :], field[p + 1, up, :]
                tn, tnu = zp(n), zp(nu)
                a0 = (F[0, p, rows, :] * n + F[1, p, rows, :] * vu) + (F[3, p, rows, :] * nu + F[5, p, rows, :] * tn)
                a0 = a0 + F[7, p, rows, :] * tvu
                a1 = F[2, p, rows, :] * v - F[6, p, rows, :] * n - F[8, p, rows, :] * vu
                total = total + v * a0 + (tv * a1 - (F[4, p, rows, :] * n) * vu)
                v, vu, tv, tvu = n, nu, tn, tnu
        return total

    def along_x(a):
        return pltpu.roll(a, LANES - 2, 1) - pltpu.roll(a, 2, 1)

    def along_y(a):
        return pltpu.roll(a, YE - 1, 0) - pltpu.roll(a, 1, 0)

    def sums(step, parts):
        for i, part in enumerate(parts):
            MA[2 * step + 1 + i] = MA[2 * step + 1 + i] + part

    sign = jnp.where(even, f32(-1.0), f32(1.0))
    for step in range(ITERS):
        r = step + 1
        last = step + 1 == ITERS
        if last:
            with scope("early_sums"):
                tile = zero()
                for k in range(MOMENTS - 1):
                    value = jnp.sum(jnp.sum(MA[k], axis=0, keepdims=True), axis=1, keepdims=True)
                    tile = jnp.where(lane_8 == k, value, tile)
                CP[pl.ds(0, T8), :] = tile
        with scope(f"inner_{r}"):
            if last:
                width = group_size(X - 2, 6)
                MA[MOMENTS - 1] = pairs(r, X - 2, 1, tiles[:-1])

                @pl.loop(0, (X - 2) // width)
                def _(g):
                    MA[MOMENTS - 1] = MA[MOMENTS - 1] + pairs(r, g * width, width, tiles[:-1])
            else:
                width = group_size(X - 2, 6)

                @pl.loop(0, (X - 2) // width)
                def _(g):
                    sums(step, planes(r, 1 + g * width, width, tiles[1:-1], False))

        if not last:
            with scope(f"pack_in_{r}"):
                for k in range(1, KT - 1):
                    PS[r + 1, pl.ds(PAD + T8 * k, T8), :] = packed(field_tile(r + 1), k, 1, X - 1)
                if not step:
                    for k in range(1, KT - 1):
                        DP[pl.ds(PAD + T8 * k, T8), :] = packed(lambda x, k: DI[x, pl.ds(T8 * k, T8), :], k, 1, X - 1)
        with scope(f"wait_{r}"):
            wait(r)
        with scope(f"halo_{r}"):
            build_halo(r)
            h = HB[...]
            full = (PG[0] + HS[0]) * h + sign * (
                PG[1] * along_x(h) + along_x(HS[1] * h) + PG[2] * along_y(h) + along_y(HS[2] * h)
            )
            CP[pl.ds(PAD, Y), :] = full[PAD:TOP]
        if last:
            break
        with scope(f"edge_{r}"):
            sums(step, planes(r, 0, 1, tiles))
            sums(step, planes(r, X - 1, 1, tiles))
        with scope(f"startx_{r + 1}"):
            start_x(r + 1, field_tile(r + 1))
        with scope(f"rim_{r}"):
            width = group_size(X - 2, 15)

            @pl.loop(0, (X - 2) // width)
            def _(g):
                sums(step, planes(r, 1 + g * width, width, (PAD, TOP - T8)))

        with scope(f"pack_{r + 1}"):
            for k in range(KT):
                rows = pl.ds(PAD + T8 * k, T8)
                if k in (0, KT - 1):
                    tile = packed(field_tile(r + 1), k, 0, X)
                else:
                    tile = PS[r + 1, rows, :] + CP[rows, :] * DP[rows, :]
                    tile = jnp.where(lane_8 >= 2 * X - 3, pltpu.roll(V[r + 1][X, rows, :], 2 * X - 2, 1), tile)
                    tile = jnp.where(ends, V[r + 1][1, rows, :], tile)
                PS[r + 1, rows, :] = tile
            spread(r + 1)
        with scope(f"start_{r + 1}"):
            start_rest(r + 1)
        with scope(f"settle_{r}"):
            width = group_size(X - 2, 6)

            @pl.loop(0, (X - 2) // width)
            def _(g):
                sums(step, settle(r, 1 + g * width, width, tiles[1:-1]))

    with scope("pairs"):
        mine = jnp.logical_and(lane_8 % 2 == 1, jnp.logical_or(lane_8 < 2 * (X - 1), lane_8 == LANES - 1))
        total = pairs(ROUNDS - 1, X - 1, 1, tiles)
        for a in tiles:
            rows = pl.ds(a, T8)
            total = total + jnp.where(mine, PS[ROUNDS - 1, rows, :] * CP[rows, :], 0.0)
        MA[MOMENTS - 1] = MA[MOMENTS - 1] + (total + pairs(ROUNDS - 1, 0, X - 1, (TOP - T8,)))

    def leave():
        wait_sent(ROUNDS - 1)

        @pl.loop(0, X, unroll=4)
        def _(x):
            for i in range(ITERS):
                for k in range(KT):
                    W[i, x, pl.ds(T8 * k, T8), :] = V[i + 1][x + 1, pl.ds(PAD + T8 * k, T8), :]

    with scope("allreduce"):
        value = jnp.sum(jnp.sum(MA[MOMENTS - 1], axis=0, keepdims=True), axis=1, keepdims=True)
        tile = jnp.where(lane_8 == MOMENTS - 1, 2.0 * value, CP[pl.ds(0, T8), :])
        for order, group in enumerate(groups):
            slot = 0
            members = 1
            for i in group:
                slot = slot * sizes[i] + me[i]
                members *= sizes[i]
            RS[order] = tile[0:1]
            others = offsets(group)
            for t in others:
                pltpu.make_async_remote_copy(
                    src_ref=RS.at[order],
                    dst_ref=RR.at[order, slot],
                    send_sem=ar_send.at[order],
                    recv_sem=ar_recv.at[order],
                    device_id=partner(t),
                    device_id_type=pl.DeviceIdType.MESH,
                ).start()
            RR[order, slot] = tile[0:1]
            if order == 0:
                leave()
            sent = RR.at[order, pl.ds(0, len(others))]
            pltpu.make_async_copy(sent, sent, ar_send.at[order]).wait()
            pltpu.make_async_copy(sent, sent, ar_recv.at[order]).wait()
            parts = [RR[order, t] for t in range(members)]
            while len(parts) > 1:
                parts = [sum(parts[i + 1 : i + 2], parts[i]) for i in range(0, len(parts), 2)]
            tile = jnp.broadcast_to(parts[0], (T8, LANES))

    n0, n1, n2, n3, n4, n5 = (
        jnp.sum(jnp.where(lane_8 == k, tile, 0.0)[0:1], axis=1, keepdims=True) for k in range(MOMENTS)
    )

    def inverse_of(d):
        return jnp.where(d > 0.0, 1.0 / d, 0.0)

    g00, g01, g02, g12, g22 = n0 - n1, n1 - n2, n2 - n3, n3 - n4, n4 - n5
    i0 = 1.0 / g00
    l1, l2 = g01 * i0, g02 * i0
    i1 = inverse_of(g02 - l1 * g01)
    e = g12 - l2 * g01
    l21 = e * i1
    i2 = inverse_of(g22 - l2 * g02 - l21 * e)
    y1 = n1 - l1 * n0
    y2 = n2 - l2 * n0 - l21 * y1
    c2 = y2 * i2
    c1 = y1 * i1 - l21 * c2
    c0 = n0 * i0 - l1 * c1 - l2 * c2

    for i, c in enumerate((c0, c1, c2)):
        C[pl.ds(i, 1), :] = jnp.broadcast_to(c, (1, LANES))


def combine(W, C, out, part, sem):
    X, Y, Z = out.shape
    rows = C[...]
    c = [jnp.broadcast_to(rows[i : i + 1], (T8, Z)) for i in range(ITERS)]
    pieces = sem.shape[0]
    width = X // pieces
    copies = []
    for g in range(pieces):
        @pl.loop(g * width, (g + 1) * width, unroll=4)
        def _(x):
            for k in range(Y // T8):
                own = pl.ds(T8 * k, T8)
                part[x, own, :] = (c[0] * W[0, x, own, :] + c[1] * W[1, x, own, :]) + c[2] * W[2, x, own, :]

        block = pl.ds(g * width, width)
        copies.append(pltpu.make_async_copy(part.at[block], out.at[block], sem.at[g]))
        copies[-1].start()
    for piece in copies:
        piece.wait()


def solution(mesh):
    sizes = tuple(mesh.shape[a] for a in AXES)

    def local(labels, conductivity, right_side):
        X, Y, Z = right_side.shape
        YE = Y + 2 * PAD
        f32 = jnp.float32
        vmem = pltpu.VMEM
        orders = len(groups_of(sizes))
        fields, factors = pl.pallas_call(
            functools.partial(kernel, sizes),
            out_shape=(vmem((ITERS, X, Y, Z), f32), vmem((T8, Z), f32)),
            in_specs=[
                pl.BlockSpec(memory_space=pl.ANY),
                pl.BlockSpec(memory_space=pl.ANY),
                pl.BlockSpec(memory_space=pl.ANY),
            ],
            out_specs=[pl.BlockSpec(memory_space=vmem)] * 2,
            scratch_shapes=[
                vmem((X, Y, Z), jnp.int32),
                pltpu.SMEM(conductivity.shape, f32),
                vmem((X, Y, Z), f32),
                vmem((X + 2, YE, Z), f32),
                vmem((X + 2, YE, Z), f32),
                vmem((X + 2, YE, Z), f32),
                vmem((X + 2, YE, Z), f32),
                vmem((6, X + 2, YE, Z), f32),
                vmem((9, X + 1, YE, Z), f32),
                vmem((X, Y, Z), f32),
                vmem((ROUNDS, YE, Z), f32),
                vmem((ROUNDS, 2, Y // 4, Z), f32),
                vmem((ROUNDS, 2, 2, T8, Z), f32),
                vmem((ROUNDS, 2, Y // 4, Z), f32),
                vmem((ROUNDS, 8, Z), f32),
                vmem((ROUNDS, 4, 8, Z), f32),
                vmem((YE, Z), f32),
                vmem((3, YE, Z), f32),
                vmem((3, YE, Z), f32),
                vmem((YE, Z), f32),
                vmem((YE, Z), f32),
                vmem((MOMENTS, 8, Z), f32),
                vmem((2, 1, Z), f32),
                vmem((2, 32, 1, Z), f32),
                pltpu.SemaphoreType.DMA((2, 18)),
                pltpu.SemaphoreType.DMA((2, 18)),
                pltpu.SemaphoreType.DMA((orders,)),
                pltpu.SemaphoreType.DMA((orders,)),
                pltpu.SemaphoreType.DMA((5,)),
            ],
            compiler_params=pltpu.CompilerParams(
                collective_id=0, has_side_effects=True, vmem_limit_bytes=60 * 1024 * 1024
            ),
        )(labels, conductivity, right_side)
        return pl.pallas_call(
            combine,
            out_shape=jax.ShapeDtypeStruct((X, Y, Z), f32),
            in_specs=[pl.BlockSpec(memory_space=vmem)] * 2,
            out_specs=pl.BlockSpec(memory_space=pl.ANY),
            scratch_shapes=[vmem((X, Y, Z), f32), pltpu.SemaphoreType.DMA((group_size(X, 4),))],
            compiler_params=pltpu.CompilerParams(vmem_limit_bytes=8 * 1024 * 1024),
        )(fields, factors)

    return jax.shard_map(
        local,
        mesh=mesh,
        in_specs=(P("gx", "gy", "gz"), P(), P("gx", "gy", "gz")),
        out_specs=P("gx", "gy", "gz"),
        check_vma=False,
    )
```

```python
import functools
import itertools
import math
import jax
import jax.numpy as jnp
from jax import lax
from jax.experimental import pallas as pl
from jax.experimental.pallas import tpu as pltpu
from jax.sharding import PartitionSpec as P

ITERS = 3
AXES = ("gx", "gy", "gz")
ROUNDS = ITERS + 1
MOMENTS = 2 * ITERS
LANES = 128
PAD = 8
T8 = 8


def group_size(n, most):
    return max(u for u in range(1, most + 1) if n % u == 0)


def groups_of(sizes):
    return [(0, 1, 2)] if math.prod(sizes) <= 32 else [(0, 1), (2,)]


def kernel(
    sizes, lab_hbm, cond_hbm, rhs_hbm, W, C, lab, cond, rhs, V0, V1, V2, V3, S, F, DI, PS, PZ, PR, ZR, ES, ER, HB, HS, PG, CP,
    DP, MA, RS, RR, send_sem, recv_sem, ar_send, ar_recv, in_sem,
):
    V = (V0, V1, V2, V3)
    X, Y, Z = rhs.shape
    end_copies = []
    for i, x in enumerate((0, X - 1)):
        end_copies.append(pltpu.make_async_copy(lab_hbm.at[x], lab.at[x], in_sem.at[3 + i]))
        end_copies[-1].start()
    inside = pl.ds(1, X - 2)
    lab_copy = pltpu.make_async_copy(lab_hbm.at[inside], lab.at[inside], in_sem.at[0])
    lab_copy.start()
    cond_copy = pltpu.make_async_copy(cond_hbm, cond, in_sem.at[2])
    cond_copy.start()
    rhs_copy = pltpu.make_async_copy(rhs_hbm, rhs, in_sem.at[1])
    YE = Y + 2 * PAD
    TOP = PAD + Y
    KT = Y // T8
    me = [lax.axis_index(a) for a in AXES]
    f32 = jnp.float32
    scope = jax.named_scope

    directions = []
    for dx in (-1, 0, 1):
        for dy in (-1, 0, 1):
            for dz in (-1, 0, 1):
                d = (dx, dy, dz)
                live = sum(1 for t in d if t)
                if live in (1, 2) and all(n > 1 for t, n in zip(d, sizes) if t):
                    directions.append(d)

    def opposite(d):
        return tuple(-t for t in d)

    axes_of = [d for d in directions if d > opposite(d)]

    def needed(d, r):
        if r < ROUNDS - 1:
            return True
        if d[2]:
            return d[2] < 0
        return d[0] <= 0 and d[1] <= 0

    def present(d):
        ok = None
        for t, m, n in zip(d, me, sizes):
            if t == 0:
                continue
            here = (m < n - 1) if t > 0 else (m > 0)
            ok = here if ok is None else jnp.logical_and(ok, here)
        return ok

    def places(d, r):
        dx, dy, dz = d
        rows_from = pl.ds(PAD, Y) if dy == 0 else (pl.ds(TOP - 1, 1) if dy > 0 else pl.ds(PAD, 1))
        rows_to = pl.ds(PAD, Y) if dy == 0 else (pl.ds(PAD - 1, 1) if dy > 0 else pl.ds(TOP, 1))
        if dz == 0:
            if dx == 0:
                return V[r].at[pl.ds(1, X), rows_from], V[r].at[pl.ds(1, X), rows_to]
            fx, tx = (X, 0) if dx > 0 else (1, X + 1)
            return V[r].at[fx, rows_from], V[r].at[tx, rows_to]
        side = 0 if dz > 0 else 1
        if dx == 0 and dy == 0:
            return PZ.at[r, side], ZR.at[r, side]
        if dx == 0:
            return PS.at[r, rows_from], PR.at[r, side, 0 if dy > 0 else 1, pl.ds(PAD - 1 if dy > 0 else 0, 1)]
        slot = (0 if dx > 0 else 2) + side
        return ES.at[r], ER.at[r, slot]

    def copy(d, r):
        src, dst = places(d, r)
        m = axes_of.index(max(d, opposite(d)))
        return pltpu.make_async_remote_copy(
            src_ref=src,
            dst_ref=dst,
            send_sem=send_sem.at[r % 2, m],
            recv_sem=recv_sem.at[r % 2, m],
            device_id=tuple(a + t for a, t in zip(me, d)),
            device_id_type=pl.DeviceIdType.MESH,
        )

    groups = groups_of(sizes)
    near = len(groups) == 1 and max(sizes) <= ROUNDS and sum(n - 1 for n in sizes) <= 2 * ROUNDS - 1

    def offsets(group):
        ranges = [range(n) if i in group else (0,) for i, n in enumerate(sizes)]
        return [t for t in itertools.product(*ranges) if any(t)]

    def partner(t):
        return tuple(lax.rem(m + k, n) for m, k, n in zip(me, t, sizes))

    barrier = pltpu.get_barrier_semaphore()
    greeted = 0
    if not near:
        for group in groups:
            for t in offsets(group):
                pl.semaphore_signal(
                    barrier, inc=1, device_id=partner(t), device_id_type=pl.DeviceIdType.MESH
                )
                greeted += 1
    if near or len(groups) > 1:
        for d in directions:
            pl.when(present(d))(
                lambda d=d: pl.semaphore_signal(
                    barrier,
                    inc=1,
                    device_id=tuple(a + t for a, t in zip(me, d)),
                    device_id_type=pl.DeviceIdType.MESH,
                )
            )
            greeted = greeted + jnp.where(present(d), 1, 0)

    for d in [
        (dx, dy, dz)
        for dx in (-1, 0, 1)
        for dy in (-1, 0, 1)
        for dz in (-1, 0, 1)
        if sum(1 for t in (dx, dy, dz) if t) in (1, 2)
    ]:
        def clear(d=d):
            for r in range(ROUNDS):
                if needed(d, r):
                    _, dst = places(d, r)
                    dst[...] = jnp.zeros(dst.shape, f32)

        if d in directions:
            back = tuple(-t for t in d)
            pl.when(jnp.logical_not(present(back)))(clear)
        else:
            clear()

    for r in range(ROUNDS):
        for a in (0, TOP):
            PS[r, pl.ds(a, PAD), :] = jnp.zeros((PAD, LANES), f32)
    for r in range(ROUNDS):
        for side in range(2):
            PR[r, side, 0, pl.ds(0, PAD - 1), :] = jnp.zeros((PAD - 1, LANES), f32)
            PR[r, side, 1, pl.ds(1, PAD - 1), :] = jnp.zeros((PAD - 1, LANES), f32)
    for x in range(X + 2):
        V[0][x, pl.ds(0, PAD - 1), :] = jnp.zeros((PAD - 1, LANES), f32)
        V[0][x, pl.ds(TOP + 1, PAD - 1), :] = jnp.zeros((PAD - 1, LANES), f32)
    MA[...] = jnp.zeros(MA.shape, f32)

    lane_e = lax.broadcasted_iota(jnp.int32, (YE, LANES), 1)
    lane_8 = lax.broadcasted_iota(jnp.int32, (T8, LANES), 1)
    row_8 = lax.broadcasted_iota(jnp.int32, (T8, LANES), 0)
    even = lane_e % 2 == 0
    ends = jnp.logical_or(lane_8 == 0, lane_8 == LANES - 1)
    inner = lane_8 < LANES - 1
    tiles = [PAD + T8 * k for k in range(KT)]

    by_row = lax.GatherDimensionNumbers(
        offset_dims=(),
        collapsed_slice_dims=(0,),
        start_index_map=(0,),
        operand_batching_dims=(1,),
        start_indices_batching_dims=(1,),
    )

    def look(c, index):
        return lax.gather(
            tables[c], index[..., None], by_row, (1, 1), mode=lax.GatherScatterMode.PROMISE_IN_BOUNDS
        )

    def look_known(values, components):
        index = jnp.maximum(values.astype(jnp.int32) - 1, 0)
        hit = values > 0.0
        return [jnp.where(hit, look(c, index), 0.0) for c in components]

    half = LANES // 2
    offs = (0, 1, half, half + 1)
    slots_of = [jnp.logical_and(lane_8 % 2 == off % 2, (lane_8 < half) == (off < half)) for off in offs]

    def send(d, r):
        if d in directions and needed(d, r):
            pl.when(present(d))(lambda: copy(d, r).start())

    def start_x(r, plane):
        tile = jnp.zeros((T8, LANES), f32)
        for col, (x, at) in enumerate(((0, 0), (0, LANES - 1), (X - 1, 0), (X - 1, LANES - 1))):
            for k in range(KT):
                to = col * KT + k
                part = plane(x, k)
                tile = jnp.where(lane_8 == to, pltpu.roll(part, (to - at) % LANES, 1), tile)
        ES[r] = tile
        for d in sorted(directions, key=lambda d: (-abs(d[2]), -abs(d[1]))):
            if d[0]:
                send(d, r)

    def start_rest(r):
        for d in sorted(directions, key=lambda d: (-abs(d[2]), -abs(d[1]))):
            if not d[0]:
                send(d, r)

    def two(d):
        dx, dy, dz = map(abs, d)
        if dx + dy + dz == 2:
            return F.at[0, 0, pl.ds(0, 2 * T8 if dx and dz else 2)]
        if dz:
            return F.at[0, 0, pl.ds(0, Y // 2)]
        return F.at[0, pl.ds(0, 2), pl.ds(0, Y)] if dx else F.at[0, pl.ds(0, X), pl.ds(0, 2)]

    def settle_pair(d, r, sent):
        back = opposite(d)
        ways = [t for t in (d, back) if needed(t, r)]
        here = [present(t if sent else opposite(t)) for t in ways]

        def one():
            c = copy(ways[0], r)
            c.wait_send() if sent else c.wait_recv()

        if len(ways) == 1:
            pl.when(here[0])(one)
        elif ways:
            sems = send_sem if sent else recv_sem

            @pl.when(jnp.logical_and(*here))
            def _():
                pltpu.make_async_copy(two(d), two(d), sems.at[r % 2, axes_of.index(d)]).wait()

            pl.when(jnp.logical_xor(*here))(one)

    def wait_sent(r):
        for d in axes_of:
            settle_pair(d, r, True)

    def wait(r):
        if r:
            wait_sent(r - 1)
        for d in axes_of:
            settle_pair(d, r, False)

    def spread(r):
        for side in range(2):
            if side == 0 and r == ROUNDS - 1:
                continue
            for t in range(KT // 4):
                tile = None
                for j, off in enumerate(offs):
                    part = PS[r, pl.ds(PAD + T8 * (4 * t + j), T8), :]
                    part = pltpu.roll(part, (off + 1 - side) % LANES, 1) if off + 1 - side else part
                    tile = part if tile is None else jnp.where(slots_of[j], part, tile)
                PZ[r, side, pl.ds(T8 * t, T8), :] = tile

    def build_halo(r):
        valid = jnp.logical_or(lane_8 <= 2 * (X - 1), lane_8 == LANES - 1)
        even = lane_8 % 2 == 0
        last = r == ROUNDS - 1

        def join(low, high):
            return jnp.where(valid, jnp.where(even, 0.0 if last else low, high), 0.0)

        for i, a in enumerate((0, TOP)):
            low = None if last else pltpu.roll(PR[r, 0, i], 1, 1)
            HB[pl.ds(a, T8), :] = join(low, pltpu.roll(PR[r, 1, i], LANES - 1, 1))
        for k in range(KT):
            t, off = pl.ds(T8 * (k // 4), T8), offs[k % 4]
            low = None if last else pltpu.roll(ZR[r, 0, t, :], (LANES - off) % LANES, 1)
            high = pltpu.roll(ZR[r, 1, t, :], LANES - 1 - off, 1)
            HB[pl.ds(PAD + T8 * k, T8), :] = join(low, high)
        targets = (((LANES - 2), 3), ((LANES - 3), 2), (2 * X, 1), (2 * X - 1, 0))
        slots = (1, 3) if last else (0, 1, 2, 3)
        got = {slot: ER[r, slot] for slot in slots}
        for k in range(KT):
            rows = pl.ds(PAD + T8 * k, T8)
            part = HB[rows, :]
            for slot in slots:
                target, col = targets[slot]
                at = col * KT + k
                part = jnp.where(
                    lane_8 == target, pltpu.roll(got[slot], (target - at) % LANES, 1), part
                )
            HB[rows, :] = part

    def zm(a):
        return pltpu.roll(a, 1, 1)

    def zp(a):
        return pltpu.roll(a, LANES - 1, 1)

    def unpack(part, x):
        return jnp.where(ends, pltpu.roll(part, lax.rem(LANES - 2 * x, LANES), 1), 0.0)

    def packed(plane, k, first, last):
        tile = None
        for x in range(first, last):
            part = pltpu.roll(plane(x, k), 2 * x, 1) if x else plane(x, k)
            tile = part if tile is None else jnp.where(jnp.logical_and(lane_8 >= 2 * x - 1, inner), part, tile)
        return tile

    def pack(r, plane):
        for k in range(KT):
            PS[r, pl.ds(PAD + T8 * k, T8), :] = packed(plane, k, 0, X)

    def label_tile(x, k):
        return (lab[x, pl.ds(T8 * k, T8), :] + 1).astype(f32)

    def field_tile(r):
        return lambda x, k: V[r][x + 1, pl.ds(PAD + T8 * k, T8), :]

    with scope("endwait"):
        for end_copy in end_copies:
            end_copy.wait()
    with scope("conv"):
        for x in (0, X - 1):
            for k in range(KT):
                V[0][x + 1, pl.ds(PAD + T8 * k, T8), :] = label_tile(x, k)
    with scope("barrier"):
        pl.semaphore_wait(barrier, greeted)
    with scope("start0"):
        start_x(0, label_tile)
    with scope("labwait"):
        lab_copy.wait()
        rhs_copy.start()
    with scope("pack0"):
        for x in range(1, X - 1):
            for k in (0, KT - 1):
                V[0][x + 1, pl.ds(PAD + T8 * k, T8), :] = label_tile(x, k)
        pack(0, label_tile)
        spread(0)
    with scope("start_0"):
        start_rest(0)

    cond_copy.wait()
    scale = (0.5, 0.5, 0.5, 0.25, 0.25, 0.25, 1.0)
    count = cond.shape[1]
    tables = []
    for c in range(7):
        table = jnp.zeros((T8, LANES), f32)
        for k in range(count):
            table = jnp.where(row_8 == k, cond[c, k] * scale[c], table)
        tables.append(table)


    def sigma_own(x, where):
        for a in where:
            index = lab[x, pl.ds(a - PAD, T8), :]
            for c in range(6):
                S[c, x + 1, pl.ds(a, T8), :] = look(c, index)

    with scope("sigma_own"):
        @pl.loop(0, X, unroll=4)
        def _(x):
            sigma_own(x, tiles[:2] + tiles[-2:])

        for x in (0, 1, X - 2, X - 1):
            sigma_own(x, tiles[2:-2])

    def coefficients(p, where, inside=True):
        for a in where:
            rows, up = pl.ds(a, T8), pl.ds(a + 1, T8)
            s3, s3u = S[3, p, rows, :], S[3, p, up, :]
            t3, t3u = S[3, p + 1, rows, :], S[3, p + 1, up, :]
            F[3, p, rows, :] = s3 + t3u
            F[4, p, rows, :] = t3 + s3u
            if inside:
                s5, s5u = S[5, p, rows, :], S[5, p, up, :]
                F[1, p, rows, :] = S[1, p, rows, :] + S[1, p, up, :]
                F[7, p, rows, :] = jnp.where(inner, s5 + zp(s5u), 0.0)
                F[8, p, rows, :] = jnp.where(inner, s5u + zp(s5), 0.0)
            if a:
                s4, t4 = S[4, p, rows, :], S[4, p + 1, rows, :]
                F[0, p, rows, :] = S[0, p, rows, :] + S[0, p + 1, rows, :]
                F[5, p, rows, :] = jnp.where(inner, s4 + zp(t4), 0.0)
                F[6, p, rows, :] = jnp.where(inner, t4 + zp(s4), 0.0)
                if inside:
                    s2 = S[2, p, rows, :]
                    F[2, p, rows, :] = jnp.where(inner, s2 + zp(s2), 0.0)

    def inside_of(x0, width, where):
        for a in where:
            rows = pl.ds(a, T8)
            own, up, down = (pl.ds(a - PAD + i, T8) for i in (0, 1, -1))
            here, above = lab[x0, own, :], lab[x0, up, :]
            s0, s3, s4, s3u = look(0, here), look(3, here), look(4, here), look(3, above)
            f0m = look(0, lab[x0 - 1, own, :]) + s0
            for i in range(width):
                x = x0 + i
                p = x + 1
                there, beyond = lab[x + 1, own, :], lab[x + 1, up, :]
                n0, n3, n4, n3u = look(0, there), look(3, there), look(4, there), look(3, beyond)
                s1, s2, s5 = look(1, here), look(2, here), look(5, here)
                s1u, s5u = look(1, above), look(5, above)
                f0, f1 = s0 + n0, s1 + s1u
                f2 = jnp.where(inner, s2 + zp(s2), 0.0)
                F[0, p, rows, :] = f0
                F[1, p, rows, :] = f1
                F[2, p, rows, :] = f2
                F[3, p, rows, :] = s3 + n3u
                F[4, p, rows, :] = n3 + s3u
                F[5, p, rows, :] = jnp.where(inner, s4 + zp(n4), 0.0)
                F[6, p, rows, :] = jnp.where(inner, n4 + zp(s4), 0.0)
                F[7, p, rows, :] = jnp.where(inner, s5 + zp(s5u), 0.0)
                F[8, p, rows, :] = jnp.where(inner, s5u + zp(s5), 0.0)
                diag = (look(6, here) + (f0m + f0)) + (f1 + (s1 + look(1, lab[x, down, :])))
                DI[x, own, :] = diag + ((f2 + zm(f2)) + jnp.where(ends, s2, 0.0))
                here, above, f0m = there, beyond, f0
                s0, s3, s4, s3u = n0, n3, n4, n3u

    with scope("coef_in"):
        width = group_size(X - 2, 5)
        for t in range(1, KT - 1, 3):
            @pl.loop(0, (X - 2) // width)
            def _(g, t=t):
                inside_of(1 + g * width, width, tiles[t : min(t + 3, KT - 1)])

        coefficients(1, tiles[1:-1])
        width = group_size(X - 2, 10)

        @pl.loop(0, (X - 2) // width)
        def _(g):
            for i in range(width):
                coefficients(1 + g * width + i, tiles[:1])
        coefficients(X - 1, tiles[:1])

    with scope("pack_d"):
        rhs_copy.wait()
        for k in range(1, KT - 1):
            rows = pl.ds(PAD + T8 * k, T8)
            DP[rows, :] = packed(lambda x, k: DI[x, pl.ds(T8 * k, T8), :], k, 1, X - 1)
            PS[1, rows, :] = packed(lambda x, k: rhs[x, pl.ds(T8 * k, T8), :], k, 1, X - 1)

    with scope("wait0"):
        wait(0)

    halo_tiles = [pl.ds(a, T8) for a in range(0, YE, T8)]

    def sigma_halo(x, rows, components):
        for c, s in zip(components, look_known(V[0][x, rows, :], components)):
            S[c, x, rows, :] = s

    with scope("sigma_halo"):
        build_halo(0)
        for rows in halo_tiles:
            (HS[0, rows, :],) = look_known(HB[rows, :], (2,))
        CP[...] = HS[0]
        for x in (0, X + 1):
            for a in tiles:
                sigma_halo(x, pl.ds(a, T8), (0,))
        for x in range(1, X + 1):
            for a in (0, TOP):
                sigma_halo(x, pl.ds(a, T8), (1,))

    def diagonal(x, total, where):
        p = x + 1
        for a in where:
            rows, up, down = pl.ds(a, T8), pl.ds(a + 1, T8), pl.ds(a - 1, T8)
            own = pl.ds(a - PAD, T8)
            s2 = S[2, p, rows, :]
            face = pltpu.roll(CP[rows, :], lax.rem(LANES - 2 * x, LANES), 1)
            diag = look(6, lab[x, own, :]) + 2.0 * ((S[0, p, rows, :] + S[1, p, rows, :]) + s2)
            diag = diag + (S[0, p - 1, rows, :] + S[0, p + 1, rows, :])
            diag = diag + (S[1, p, down, :] + S[1, p, up, :])
            diag = diag + (jnp.where(lane_8 == 0, face, zm(s2)) + jnp.where(inner, zp(s2), face))
            inverse = 1.0 / diag
            DI[x, own, :] = inverse
            r0 = rhs[x, own, :]
            w = r0 * inverse
            V[1][p, rows, :] = w
            total = total + r0 * w
        return total

    def zero():
        return jnp.zeros((T8, LANES), f32)

    with scope("diag_x"):
        MA[0] = diagonal(X - 1, diagonal(0, zero(), tiles), tiles)
    with scope("startx_1"):
        start_x(1, field_tile(1))
    with scope("diag_rim"):
        width = group_size(X - 2, 15)

        @pl.loop(0, (X - 2) // width)
        def _(g):
            total = zero()
            for i in range(width):
                total = diagonal(1 + g * width + i, total, (PAD, TOP - T8))
            MA[0] = MA[0] + total

    def assemble(r, known):
        for k in range(KT):
            rows = pl.ds(PAD + T8 * k, T8)
            if k in (0, KT - 1):
                tile = packed(field_tile(r), k, 0, X)
            else:
                tile = jnp.where(lane_8 >= 2 * X - 3, pltpu.roll(V[r][X, rows, :], 2 * X - 2, 1), known(rows))
                tile = jnp.where(ends, V[r][1, rows, :], tile)
            PS[r, rows, :] = tile
        spread(r)

    def first(rows):
        inverse = 1.0 / (DP[rows, :] + CP[rows, :])
        DP[rows, :] = inverse
        return PS[1, rows, :] * inverse

    with scope("pack_1"):
        assemble(1, first)
    with scope("start_1"):
        start_rest(1)
    with scope("diag_in"):
        width = group_size(X - 2, 10)

        @pl.loop(0, (X - 2) // width)
        def _(g):
            total = zero()
            for a in tiles[1:-1]:
                own, halo = pl.ds(a - PAD, T8), CP[pl.ds(a, T8), :]
                for i in range(width):
                    x = 1 + g * width + i
                    inverse = 1.0 / (DI[x, own, :] + unpack(halo, x))
                    DI[x, own, :] = inverse
                    r0 = rhs[x, own, :]
                    w = r0 * inverse
                    V[1][x + 1, pl.ds(a, T8), :] = w
                    total = total + r0 * w
            MA[0] = MA[0] + total

    with scope("coef"):
        for rows in halo_tiles:
            for i, s in enumerate(look_known(HB[rows, :], (4, 5))):
                HS[i + 1, rows, :] = s
            for i, s in enumerate(look_known(PS[0, rows, :], (2, 4, 5))):
                PG[i, rows, :] = s
            for x in (0, X + 1):
                sigma_halo(x, rows, (3, 4))

        @pl.loop(1, X + 1, unroll=4)
        def _(x):
            for a in (0, TOP):
                sigma_halo(x, pl.ds(a, T8), (3, 5))

        coefficients(0, [0] + tiles, False)
        coefficients(X, [0] + tiles)
        coefficients(X - 1, (0, TOP - T8))
        width = group_size(X - 2, 10)

        @pl.loop(0, (X - 2) // width)
        def _(g):
            for i in range(width):
                coefficients(1 + g * width + i, (0, TOP - T8))

    def planes(r, x0, width, where, ready=True):
        odd, evn = zero(), zero()
        field, nxt = V[r], V[r + 1]
        for a in where:
            rows, up, down = pl.ds(a, T8), pl.ds(a + 1, T8), pl.ds(a - 1, T8)
            own = pl.ds(a - PAD, T8)
            halo = CP[rows, :] if ready else None
            m, mu, md = field[x0, rows, :], field[x0, up, :], field[x0, down, :]
            v, vu, vd = field[x0 + 1, rows, :], field[x0 + 1, up, :], field[x0 + 1, down, :]
            tv = zp(v)
            acc = F[0, x0, rows, :] * m + F[3, x0, down, :] * md
            acc = acc - F[4, x0, rows, :] * mu - F[6, x0, rows, :] * zp(m)
            accs = F[5, x0, rows, :] * m
            for i in range(width):
                x = x0 + i
                p = x + 1
                n, nu, nd = field[p + 1, rows, :], field[p + 1, up, :], field[p + 1, down, :]
                tn = zp(n)
                f0 = F[0, p, rows, :]
                f2 = F[2, p, rows, :]
                f3, f3d = F[3, p, rows, :], F[3, p, down, :]
                f4, f4d = F[4, p, rows, :], F[4, p, down, :]
                f5, f6 = F[5, p, rows, :], F[6, p, rows, :]
                f7, f7d = F[7, p, rows, :], F[7, p, down, :]
                f8, f8d = F[8, p, rows, :], F[8, p, down, :]
                s = (accs + f2 * v) + (f7d * vd - f8 * vu) - f6 * n
                q = (acc + f0 * n) + (F[1, p, rows, :] * vu + F[1, p, down, :] * vd)
                q = q + (f3 * nu - f4d * nd) + (f2 * tv + f5 * tn)
                q = q + (f7 * zp(vu) - f8d * zp(vd))
                q = q + zm(s)
                if ready:
                    q = q + unpack(halo, x)
                acc = (f0 * v + f3d * vd) - (f4 * vu + f6 * tv)
                accs = f5 * v
                odd = odd + v * q
                w = q * DI[x, own, :]
                evn = evn + w * q
                nxt[p, rows, :] = w
                v, vu, vd, tv = n, nu, nd, tn
        return odd, evn

    def settle(r, x0, width, where):
        odd, evn = zero(), zero()
        for a in where:
            rows, own = pl.ds(a, T8), pl.ds(a - PAD, T8)
            halo = CP[rows, :]
            for i in range(width):
                x = x0 + i
                c = unpack(halo, x)
                w = V[r + 1][x + 1, rows, :]
                full = w + c * DI[x, own, :]
                V[r + 1][x + 1, rows, :] = full
                odd = odd + c * V[r][x + 1, rows, :]
                evn = evn + c * (w + full)
        return odd, evn

    def pairs(r, x0, width, where):
        total = zero()
        field = V[r]
        for a in where:
            rows, up = pl.ds(a, T8), pl.ds(a + 1, T8)
            v, vu = field[x0 + 1, rows, :], field[x0 + 1, up, :]
            tv, tvu = zp(v), zp(vu)
            for i in range(width):
                p = x0 + i + 1
                n, nu = field[p + 1, rows, :], field[p + 1, up, :]
                tn, tnu = zp(n), zp(nu)
                a0 = (F[0, p, rows, :] * n + F[1, p, rows, :] * vu) + (F[3, p, rows, :] * nu + F[5, p, rows, :] * tn)
                a0 = a0 + F[7, p, rows, :] * tvu
                a1 = F[2, p, rows, :] * v - F[6, p, rows, :] * n - F[8, p, rows, :] * vu
                total = total + v * a0 + (tv * a1 - (F[4, p, rows, :] * n) * vu)
                v, vu, tv, tvu = n, nu, tn, tnu
        return total

    def along_x(a):
        return pltpu.roll(a, LANES - 2, 1) - pltpu.roll(a, 2, 1)

    def along_y(a):
        return pltpu.roll(a, YE - 1, 0) - pltpu.roll(a, 1, 0)

    def sums(step, parts):
        for i, part in enumerate(parts):
            MA[2 * step + 1 + i] = MA[2 * step + 1 + i] + part

    sign = jnp.where(even, f32(-1.0), f32(1.0))
    for step in range(ITERS):
        r = step + 1
        last = step + 1 == ITERS
        if last:
            with scope("early_sums"):
                tile = zero()
                for k in range(MOMENTS - 1):
                    value = jnp.sum(jnp.sum(MA[k], axis=0, keepdims=True), axis=1, keepdims=True)
                    tile = jnp.where(lane_8 == k, value, tile)
                CP[pl.ds(0, T8), :] = tile
        with scope(f"inner_{r}"):
            if last:
                width = group_size(X - 2, 10)
                MA[MOMENTS - 1] = pairs(r, X - 2, 1, tiles[:-1])

                @pl.loop(0, (X - 2) // width)
                def _(g):
                    MA[MOMENTS - 1] = MA[MOMENTS - 1] + pairs(r, g * width, width, tiles[:-1])
            else:
                width = group_size(X - 2, 10)

                @pl.loop(0, (X - 2) // width)
                def _(g):
                    sums(step, planes(r, 1 + g * width, width, tiles[1:-1], False))

        if not last:
            with scope(f"pack_in_{r}"):
                for k in range(1, KT - 1):
                    PS[r + 1, pl.ds(PAD + T8 * k, T8), :] = packed(field_tile(r + 1), k, 1, X - 1)
        with scope(f"wait_{r}"):
            wait(r)
        with scope(f"halo_{r}"):
            build_halo(r)
            h = HB[...]
            full = (PG[0] + HS[0]) * h + sign * (
                PG[1] * along_x(h) + along_x(HS[1] * h) + PG[2] * along_y(h) + along_y(HS[2] * h)
            )
            CP[pl.ds(PAD, Y), :] = full[PAD:TOP]
        if last:
            break
        with scope(f"edge_{r}"):
            sums(step, planes(r, 0, 1, tiles))
            sums(step, planes(r, X - 1, 1, tiles))
        with scope(f"startx_{r + 1}"):
            start_x(r + 1, field_tile(r + 1))
        with scope(f"rim_{r}"):
            width = group_size(X - 2, 15)

            @pl.loop(0, (X - 2) // width)
            def _(g):
                sums(step, planes(r, 1 + g * width, width, (PAD, TOP - T8)))

        with scope(f"pack_{r + 1}"):
            assemble(r + 1, lambda rows: PS[r + 1, rows, :] + CP[rows, :] * DP[rows, :])
        with scope(f"start_{r + 1}"):
            start_rest(r + 1)
        with scope(f"settle_{r}"):
            width = group_size(X - 2, 15)

            @pl.loop(0, (X - 2) // width)
            def _(g):
                sums(step, settle(r, 1 + g * width, width, tiles[1:-1]))

    with scope("pairs"):
        mine = jnp.logical_and(lane_8 % 2 == 1, jnp.logical_or(lane_8 < 2 * (X - 1), lane_8 == LANES - 1))
        total = pairs(ROUNDS - 1, X - 1, 1, tiles)
        for a in tiles:
            rows = pl.ds(a, T8)
            total = total + jnp.where(mine, PS[ROUNDS - 1, rows, :] * CP[rows, :], 0.0)
        MA[MOMENTS - 1] = MA[MOMENTS - 1] + (total + pairs(ROUNDS - 1, 0, X - 1, (TOP - T8,)))

    def leave():
        wait_sent(ROUNDS - 1)

        @pl.loop(0, X, unroll=4)
        def _(x):
            for i in range(ITERS):
                for k in range(KT):
                    W[i, x, pl.ds(T8 * k, T8), :] = V[i + 1][x + 1, pl.ds(PAD + T8 * k, T8), :]

    with scope("allreduce"):
        value = jnp.sum(jnp.sum(MA[MOMENTS - 1], axis=0, keepdims=True), axis=1, keepdims=True)
        tile = jnp.where(lane_8 == MOMENTS - 1, 2.0 * value, CP[pl.ds(0, T8), :])
        for order, group in enumerate(groups):
            slot = 0
            members = 1
            for i in group:
                slot = slot * sizes[i] + me[i]
                members *= sizes[i]
            RS[order] = tile[0:1]
            others = offsets(group)
            for t in others:
                pltpu.make_async_remote_copy(
                    src_ref=RS.at[order],
                    dst_ref=RR.at[order, slot],
                    send_sem=ar_send.at[order],
                    recv_sem=ar_recv.at[order],
                    device_id=partner(t),
                    device_id_type=pl.DeviceIdType.MESH,
                ).start()
            RR[order, slot] = tile[0:1]
            if order == 0:
                leave()
            sent = RR.at[order, pl.ds(0, len(others))]
            pltpu.make_async_copy(sent, sent, ar_send.at[order]).wait()
            pltpu.make_async_copy(sent, sent, ar_recv.at[order]).wait()
            parts = [RR[order, t] for t in range(members)]
            while len(parts) > 1:
                parts = [sum(parts[i + 1 : i + 2], parts[i]) for i in range(0, len(parts), 2)]
            tile = jnp.broadcast_to(parts[0], (T8, LANES))

    n0, n1, n2, n3, n4, n5 = (
        jnp.sum(jnp.where(lane_8 == k, tile, 0.0)[0:1], axis=1, keepdims=True) for k in range(MOMENTS)
    )

    def inverse_of(d):
        return jnp.where(d > 0.0, 1.0 / d, 0.0)

    g00, g01, g02, g12, g22 = n0 - n1, n1 - n2, n2 - n3, n3 - n4, n4 - n5
    i0 = 1.0 / g00
    l1, l2 = g01 * i0, g02 * i0
    i1 = inverse_of(g02 - l1 * g01)
    e = g12 - l2 * g01
    l21 = e * i1
    i2 = inverse_of(g22 - l2 * g02 - l21 * e)
    y1 = n1 - l1 * n0
    y2 = n2 - l2 * n0 - l21 * y1
    c2 = y2 * i2
    c1 = y1 * i1 - l21 * c2
    c0 = n0 * i0 - l1 * c1 - l2 * c2

    for i, c in enumerate((c0, c1, c2)):
        C[pl.ds(i, 1), :] = jnp.broadcast_to(c, (1, LANES))


def combine(W, C, out, part, sem):
    X, Y, Z = out.shape
    rows = C[...]
    c = [jnp.broadcast_to(rows[i : i + 1], (T8, Z)) for i in range(ITERS)]
    pieces = sem.shape[0]
    width = X // pieces
    copies = []
    for g in range(pieces):
        @pl.loop(g * width, (g + 1) * width, unroll=4)
        def _(x):
            for k in range(Y // T8):
                own = pl.ds(T8 * k, T8)
                part[x, own, :] = (c[0] * W[0, x, own, :] + c[1] * W[1, x, own, :]) + c[2] * W[2, x, own, :]

        block = pl.ds(g * width, width)
        copies.append(pltpu.make_async_copy(part.at[block], out.at[block], sem.at[g]))
        copies[-1].start()
    for piece in copies:
        piece.wait()


def solution(mesh):
    sizes = tuple(mesh.shape[a] for a in AXES)

    def local(labels, conductivity, right_side):
        X, Y, Z = right_side.shape
        YE = Y + 2 * PAD
        f32 = jnp.float32
        vmem = pltpu.VMEM
        orders = len(groups_of(sizes))
        fields, factors = pl.pallas_call(
            functools.partial(kernel, sizes),
            out_shape=(vmem((ITERS, X, Y, Z), f32), vmem((T8, Z), f32)),
            in_specs=[
                pl.BlockSpec(memory_space=pl.ANY),
                pl.BlockSpec(memory_space=pl.ANY),
                pl.BlockSpec(memory_space=pl.ANY),
            ],
            out_specs=[pl.BlockSpec(memory_space=vmem)] * 2,
            scratch_shapes=[
                vmem((X, Y, Z), jnp.int32),
                pltpu.SMEM(conductivity.shape, f32),
                vmem((X, Y, Z), f32),
                vmem((X + 2, YE, Z), f32),
                vmem((X + 2, YE, Z), f32),
                vmem((X + 2, YE, Z), f32),
                vmem((X + 2, YE, Z), f32),
                vmem((6, X + 2, YE, Z), f32),
                vmem((9, X + 1, YE, Z), f32),
                vmem((X, Y, Z), f32),
                vmem((ROUNDS, YE, Z), f32),
                vmem((ROUNDS, 2, Y // 4, Z), f32),
                vmem((ROUNDS, 2, 2, T8, Z), f32),
                vmem((ROUNDS, 2, Y // 4, Z), f32),
                vmem((ROUNDS, 8, Z), f32),
                vmem((ROUNDS, 4, 8, Z), f32),
                vmem((YE, Z), f32),
                vmem((3, YE, Z), f32),
                vmem((3, YE, Z), f32),
                vmem((YE, Z), f32),
                vmem((YE, Z), f32),
                vmem((MOMENTS, 8, Z), f32),
                vmem((2, 1, Z), f32),
                vmem((2, 32, 1, Z), f32),
                pltpu.SemaphoreType.DMA((2, 9)),
                pltpu.SemaphoreType.DMA((2, 9)),
                pltpu.SemaphoreType.DMA((orders,)),
                pltpu.SemaphoreType.DMA((orders,)),
                pltpu.SemaphoreType.DMA((5,)),
            ],
            compiler_params=pltpu.CompilerParams(
                collective_id=0, has_side_effects=True, vmem_limit_bytes=60 * 1024 * 1024
            ),
        )(labels, conductivity, right_side)
        return pl.pallas_call(
            combine,
            out_shape=jax.ShapeDtypeStruct((X, Y, Z), f32),
            in_specs=[pl.BlockSpec(memory_space=vmem)] * 2,
            out_specs=pl.BlockSpec(memory_space=pl.ANY),
            scratch_shapes=[vmem((X, Y, Z), f32), pltpu.SemaphoreType.DMA((group_size(X, 4),))],
            compiler_params=pltpu.CompilerParams(vmem_limit_bytes=8 * 1024 * 1024),
        )(fields, factors)

    return jax.shard_map(
        local,
        mesh=mesh,
        in_specs=(P("gx", "gy", "gz"), P(), P("gx", "gy", "gz")),
        out_specs=P("gx", "gy", "gz"),
        check_vma=False,
    )
```

```python
import functools
import itertools
import math
import jax
import jax.numpy as jnp
from jax import lax
from jax.experimental import pallas as pl
from jax.experimental.pallas import tpu as pltpu
from jax.sharding import PartitionSpec as P

ITERS = 3
AXES = ("gx", "gy", "gz")
ROUNDS = ITERS + 1
MOMENTS = 2 * ITERS
LANES = 128
PAD = 8
T8 = 8


def group_size(n, most):
    return max(u for u in range(1, most + 1) if n % u == 0)


def groups_of(sizes):
    return [(0, 1, 2)] if math.prod(sizes) <= 32 else [(0, 1), (2,)]


def kernel(
    sizes, lab_hbm, cond_hbm, rhs_hbm, W, C, lab, cond, rhs, V0, V1, V2, V3, S, F, DI, PS, PZ, PR, ZR, ES, ER, HB, HS, PG, CP,
    DP, K, MA, RS, RR, send_sem, recv_sem, ar_send, ar_recv, in_sem,
):
    V = (V0, V1, V2, V3)
    X, Y, Z = rhs.shape
    end_copies = []
    for i, x in enumerate((0, X - 1)):
        end_copies.append(pltpu.make_async_copy(lab_hbm.at[x], lab.at[x], in_sem.at[3 + i]))
        end_copies[-1].start()
    inside = pl.ds(1, X - 2)
    lab_copy = pltpu.make_async_copy(lab_hbm.at[inside], lab.at[inside], in_sem.at[0])
    lab_copy.start()
    cond_copy = pltpu.make_async_copy(cond_hbm, cond, in_sem.at[2])
    cond_copy.start()
    rhs_copy = pltpu.make_async_copy(rhs_hbm, rhs, in_sem.at[1])
    YE = Y + 2 * PAD
    TOP = PAD + Y
    KT = Y // T8
    me = [lax.axis_index(a) for a in AXES]
    f32 = jnp.float32
    scope = jax.named_scope

    directions = []
    for dx in (-1, 0, 1):
        for dy in (-1, 0, 1):
            for dz in (-1, 0, 1):
                d = (dx, dy, dz)
                live = sum(1 for t in d if t)
                if live in (1, 2) and all(n > 1 for t, n in zip(d, sizes) if t):
                    directions.append(d)

    def opposite(d):
        return tuple(-t for t in d)

    axes_of = [d for d in directions if d > opposite(d)]

    def needed(d, r):
        if r < ROUNDS - 1:
            return True
        if d[2]:
            return d[2] < 0
        return d[0] <= 0 and d[1] <= 0

    def present(d):
        ok = None
        for t, m, n in zip(d, me, sizes):
            if t == 0:
                continue
            here = (m < n - 1) if t > 0 else (m > 0)
            ok = here if ok is None else jnp.logical_and(ok, here)
        return ok

    def places(d, r):
        dx, dy, dz = d
        rows_from = pl.ds(PAD, Y) if dy == 0 else (pl.ds(TOP - 1, 1) if dy > 0 else pl.ds(PAD, 1))
        rows_to = pl.ds(PAD, Y) if dy == 0 else (pl.ds(PAD - 1, 1) if dy > 0 else pl.ds(TOP, 1))
        if dz == 0:
            if dx == 0:
                return V[r].at[pl.ds(1, X), rows_from], V[r].at[pl.ds(1, X), rows_to]
            fx, tx = (X, 0) if dx > 0 else (1, X + 1)
            return V[r].at[fx, rows_from], V[r].at[tx, rows_to]
        side = 0 if dz > 0 else 1
        if dx == 0 and dy == 0:
            return PZ.at[r, side], ZR.at[r, side]
        if dx == 0:
            return PS.at[r, rows_from], PR.at[r, side, 0 if dy > 0 else 1, pl.ds(PAD - 1 if dy > 0 else 0, 1)]
        slot = (0 if dx > 0 else 2) + side
        return ES.at[r], ER.at[r, slot]

    def copy(d, r):
        src, dst = places(d, r)
        m = axes_of.index(max(d, opposite(d)))
        return pltpu.make_async_remote_copy(
            src_ref=src,
            dst_ref=dst,
            send_sem=send_sem.at[r % 2, m],
            recv_sem=recv_sem.at[r % 2, m],
            device_id=tuple(a + t for a, t in zip(me, d)),
            device_id_type=pl.DeviceIdType.MESH,
        )

    groups = groups_of(sizes)
    near = len(groups) == 1 and max(sizes) <= ROUNDS and sum(n - 1 for n in sizes) <= 2 * ROUNDS - 1

    def offsets(group):
        ranges = [range(n) if i in group else (0,) for i, n in enumerate(sizes)]
        return [t for t in itertools.product(*ranges) if any(t)]

    def partner(t):
        return tuple(lax.rem(m + k, n) for m, k, n in zip(me, t, sizes))

    barrier = pltpu.get_barrier_semaphore()
    greeted = 0
    if not near:
        for group in groups:
            for t in offsets(group):
                pl.semaphore_signal(
                    barrier, inc=1, device_id=partner(t), device_id_type=pl.DeviceIdType.MESH
                )
                greeted += 1
    if near or len(groups) > 1:
        for d in directions:
            pl.when(present(d))(
                lambda d=d: pl.semaphore_signal(
                    barrier,
                    inc=1,
                    device_id=tuple(a + t for a, t in zip(me, d)),
                    device_id_type=pl.DeviceIdType.MESH,
                )
            )
            greeted = greeted + jnp.where(present(d), 1, 0)

    for d in [
        (dx, dy, dz)
        for dx in (-1, 0, 1)
        for dy in (-1, 0, 1)
        for dz in (-1, 0, 1)
        if sum(1 for t in (dx, dy, dz) if t) in (1, 2)
    ]:
        def clear(d=d):
            for r in range(ROUNDS):
                if needed(d, r):
                    _, dst = places(d, r)
                    dst[...] = jnp.zeros(dst.shape, f32)

        if d in directions:
            back = tuple(-t for t in d)
            pl.when(jnp.logical_not(present(back)))(clear)
        else:
            clear()

    for r in range(ROUNDS):
        for a in (0, TOP):
            PS[r, pl.ds(a, PAD), :] = jnp.zeros((PAD, LANES), f32)
    for r in range(ROUNDS):
        for side in range(2):
            PR[r, side, 0, pl.ds(0, PAD - 1), :] = jnp.zeros((PAD - 1, LANES), f32)
            PR[r, side, 1, pl.ds(1, PAD - 1), :] = jnp.zeros((PAD - 1, LANES), f32)
    for x in range(X + 2):
        V[0][x, pl.ds(0, PAD - 1), :] = jnp.zeros((PAD - 1, LANES), f32)
        V[0][x, pl.ds(TOP + 1, PAD - 1), :] = jnp.zeros((PAD - 1, LANES), f32)
    MA[...] = jnp.zeros(MA.shape, f32)

    lane_8 = lax.broadcasted_iota(jnp.int32, (T8, LANES), 1)
    row_8 = lax.broadcasted_iota(jnp.int32, (T8, LANES), 0)
    ends = jnp.logical_or(lane_8 == 0, lane_8 == LANES - 1)
    inner = lane_8 < LANES - 1
    tiles = [PAD + T8 * k for k in range(KT)]

    by_row = lax.GatherDimensionNumbers(
        offset_dims=(),
        collapsed_slice_dims=(0,),
        start_index_map=(0,),
        operand_batching_dims=(1,),
        start_indices_batching_dims=(1,),
    )

    def look(c, index):
        return lax.gather(
            tables[c], index[..., None], by_row, (1, 1), mode=lax.GatherScatterMode.PROMISE_IN_BOUNDS
        )

    def look_known(values, components):
        index = jnp.maximum(values.astype(jnp.int32) - 1, 0)
        hit = values > 0.0
        return [jnp.where(hit, look(c, index), 0.0) for c in components]

    half = LANES // 2
    span = LANES - 2 - 2 * X
    offs = (0, 1, half, half + 1)
    slots_of = [jnp.logical_and(lane_8 % 2 == off % 2, (lane_8 < half) == (off < half)) for off in offs]

    def send(d, r):
        if d in directions and needed(d, r):
            pl.when(present(d))(lambda: copy(d, r).start())

    def start_x(r, plane):
        tile = jnp.zeros((T8, LANES), f32)
        for x, base in ((0, 0), (X - 1, span)):
            for k in range(KT):
                to = base + 2 * k
                here = jnp.logical_or(lane_8 == to, lane_8 == to + 1)
                tile = jnp.where(here, pltpu.roll(plane(x, k), to + 1, 1), tile)
        ES[r] = tile
        outer = sorted((d for d in directions if d[0]), key=lambda d: (-abs(d[2]), -abs(d[1])))

        def both(side):
            for t in (side, -side):
                for d in outer:
                    if d[0] == t:
                        send(d, r)

        far = lax.rem(me[0], 2) == 1
        pl.when(far)(lambda: both(1))
        pl.when(jnp.logical_not(far))(lambda: both(-1))

    def start_rest(r):
        for d in sorted(directions, key=lambda d: (-abs(d[2]), -abs(d[1]))):
            if not d[0]:
                send(d, r)

    def two(d):
        dx, dy, dz = map(abs, d)
        if dx + dy + dz == 2:
            return F.at[0, 0, pl.ds(0, 2 * T8 if dx and dz else 2)]
        if dz:
            return F.at[0, 0, pl.ds(0, Y // 2)]
        return F.at[0, pl.ds(0, 2), pl.ds(0, Y)] if dx else F.at[0, pl.ds(0, X), pl.ds(0, 2)]

    def settle_pair(d, r, sent):
        back = opposite(d)
        ways = [t for t in (d, back) if needed(t, r)]
        here = [present(t if sent else opposite(t)) for t in ways]

        def one():
            c = copy(ways[0], r)
            c.wait_send() if sent else c.wait_recv()

        if len(ways) == 1:
            pl.when(here[0])(one)
        elif ways:
            sems = send_sem if sent else recv_sem

            @pl.when(jnp.logical_and(*here))
            def _():
                pltpu.make_async_copy(two(d), two(d), sems.at[r % 2, axes_of.index(d)]).wait()

            pl.when(jnp.logical_xor(*here))(one)

    def wait_sent(r):
        for d in axes_of:
            settle_pair(d, r, True)

    def wait(r):
        if r:
            wait_sent(r - 1)
        for d in axes_of:
            settle_pair(d, r, False)

    def spread(r):
        for side in range(2):
            if side == 0 and r == ROUNDS - 1:
                continue
            for t in range(KT // 4):
                tile = None
                for j, off in enumerate(offs):
                    part = PS[r, pl.ds(PAD + T8 * (4 * t + j), T8), :]
                    part = pltpu.roll(part, (off + 1 - side) % LANES, 1) if off + 1 - side else part
                    tile = part if tile is None else jnp.where(slots_of[j], part, tile)
                PZ[r, side, pl.ds(T8 * t, T8), :] = tile

    def build_halo(r):
        valid = jnp.logical_or(lane_8 <= 2 * (X - 1), lane_8 == LANES - 1)
        even = lane_8 % 2 == 0
        last = r == ROUNDS - 1

        def join(low, high):
            return jnp.where(valid, jnp.where(even, 0.0 if last else low, high), 0.0)

        for i, a in enumerate((0, TOP)):
            low = None if last else pltpu.roll(PR[r, 0, i], 1, 1)
            HB[pl.ds(a, T8), :] = join(low, pltpu.roll(PR[r, 1, i], LANES - 1, 1))
        for k in range(KT):
            t, off = pl.ds(T8 * (k // 4), T8), offs[k % 4]
            low = None if last else pltpu.roll(ZR[r, 0, t, :], (LANES - off) % LANES, 1)
            high = pltpu.roll(ZR[r, 1, t, :], LANES - 1 - off, 1)
            HB[pl.ds(PAD + T8 * k, T8), :] = join(low, high)
        got = [(1, jnp.where(lane_8 < span, ER[r, 3], ER[r, 1]))]
        if not last:
            got.append((0, jnp.where(lane_8 < span, ER[r, 2], ER[r, 0])))
        for k in range(KT):
            rows = pl.ds(PAD + T8 * k, T8)
            part = HB[rows, :]
            for i, tile in got:
                here = jnp.logical_or(lane_8 == 2 * X - i, lane_8 == LANES - 2 - i)
                part = jnp.where(here, pltpu.roll(tile, (2 * X - 2 * i - 2 * k) % LANES, 1), part)
            HB[rows, :] = part

    def zm(a):
        return pltpu.roll(a, 1, 1)

    def zp(a):
        return pltpu.roll(a, LANES - 1, 1)

    def unpack(part, x):
        return jnp.where(ends, pltpu.roll(part, lax.rem(LANES - 2 * x, LANES), 1), 0.0)

    def packed(plane, k, first, last):
        tile = None
        for x in range(first, last):
            part = pltpu.roll(plane(x, k), 2 * x, 1) if x else plane(x, k)
            tile = part if tile is None else jnp.where(jnp.logical_and(lane_8 >= 2 * x - 1, inner), part, tile)
        return tile

    def pack(r, plane):
        for k in range(KT):
            PS[r, pl.ds(PAD + T8 * k, T8), :] = packed(plane, k, 0, X)

    def label_tile(x, k):
        return (lab[x, pl.ds(T8 * k, T8), :] + 1).astype(f32)

    def field_tile(r):
        return lambda x, k: V[r][x + 1, pl.ds(PAD + T8 * k, T8), :]

    with scope("endwait"):
        for end_copy in end_copies:
            end_copy.wait()
    with scope("conv"):
        for x in (0, X - 1):
            for k in range(KT):
                V[0][x + 1, pl.ds(PAD + T8 * k, T8), :] = label_tile(x, k)
    with scope("barrier"):
        pl.semaphore_wait(barrier, greeted)
    with scope("start0"):
        start_x(0, label_tile)
    with scope("labwait"):
        lab_copy.wait()
        rhs_copy.start()
    with scope("pack0"):
        for x in range(1, X - 1):
            for k in (0, KT - 1):
                V[0][x + 1, pl.ds(PAD + T8 * k, T8), :] = label_tile(x, k)
        pack(0, label_tile)
        spread(0)
    with scope("start_0"):
        start_rest(0)

    cond_copy.wait()
    scale = (0.5, 0.5, 0.5, 0.25, 0.25, 0.25, 1.0)
    count = cond.shape[1]
    tables = []
    for c in range(7):
        table = jnp.zeros((T8, LANES), f32)
        for k in range(count):
            table = jnp.where(row_8 == k, cond[c, k] * scale[c], table)
        tables.append(table)


    def sigma_own(x, where):
        for a in where:
            index = lab[x, pl.ds(a - PAD, T8), :]
            for c in range(6):
                S[c, x + 1, pl.ds(a, T8), :] = look(c, index)

    with scope("sigma_own"):
        @pl.loop(0, X, unroll=4)
        def _(x):
            sigma_own(x, tiles[:2] + tiles[-2:])

        for x in (0, 1, X - 2, X - 1):
            sigma_own(x, tiles[2:-2])

    def coefficients(p, where, inside=True):
        for a in where:
            rows, up = pl.ds(a, T8), pl.ds(a + 1, T8)
            s3, s3u = S[3, p, rows, :], S[3, p, up, :]
            t3, t3u = S[3, p + 1, rows, :], S[3, p + 1, up, :]
            F[3, p, rows, :] = s3 + t3u
            F[4, p, rows, :] = t3 + s3u
            if inside:
                s5, s5u = S[5, p, rows, :], S[5, p, up, :]
                F[1, p, rows, :] = S[1, p, rows, :] + S[1, p, up, :]
                F[7, p, rows, :] = jnp.where(inner, s5 + zp(s5u), 0.0)
                F[8, p, rows, :] = jnp.where(inner, s5u + zp(s5), 0.0)
            if a:
                s4, t4 = S[4, p, rows, :], S[4, p + 1, rows, :]
                F[0, p, rows, :] = S[0, p, rows, :] + S[0, p + 1, rows, :]
                F[5, p, rows, :] = jnp.where(inner, s4 + zp(t4), 0.0)
                F[6, p, rows, :] = jnp.where(inner, t4 + zp(s4), 0.0)
                if inside:
                    s2 = S[2, p, rows, :]
                    F[2, p, rows, :] = jnp.where(inner, s2 + zp(s2), 0.0)

    def inside_of(x0, width, where):
        for a in where:
            rows = pl.ds(a, T8)
            own, up, down = (pl.ds(a - PAD + i, T8) for i in (0, 1, -1))
            here, above = lab[x0, own, :], lab[x0, up, :]
            s0, s3, s4, s3u = look(0, here), look(3, here), look(4, here), look(3, above)
            f0m = look(0, lab[x0 - 1, own, :]) + s0
            for i in range(width):
                x = x0 + i
                p = x + 1
                there, beyond = lab[x + 1, own, :], lab[x + 1, up, :]
                n0, n3, n4, n3u = look(0, there), look(3, there), look(4, there), look(3, beyond)
                s1, s2, s5 = look(1, here), look(2, here), look(5, here)
                s1u, s5u = look(1, above), look(5, above)
                f0, f1 = s0 + n0, s1 + s1u
                f2 = jnp.where(inner, s2 + zp(s2), 0.0)
                F[0, p, rows, :] = f0
                F[1, p, rows, :] = f1
                F[2, p, rows, :] = f2
                F[3, p, rows, :] = s3 + n3u
                F[4, p, rows, :] = n3 + s3u
                F[5, p, rows, :] = jnp.where(inner, s4 + zp(n4), 0.0)
                F[6, p, rows, :] = jnp.where(inner, n4 + zp(s4), 0.0)
                F[7, p, rows, :] = jnp.where(inner, s5 + zp(s5u), 0.0)
                F[8, p, rows, :] = jnp.where(inner, s5u + zp(s5), 0.0)
                diag = (look(6, here) + (f0m + f0)) + (f1 + (s1 + look(1, lab[x, down, :])))
                DI[x, own, :] = diag + ((f2 + zm(f2)) + jnp.where(ends, s2, 0.0))
                here, above, f0m = there, beyond, f0
                s0, s3, s4, s3u = n0, n3, n4, n3u

    with scope("coef_in"):
        width = group_size(X - 2, 5)
        for t in range(1, KT - 1, 3):
            @pl.loop(0, (X - 2) // width)
            def _(g, t=t):
                inside_of(1 + g * width, width, tiles[t : min(t + 3, KT - 1)])

        coefficients(1, tiles[1:-1])
    with scope("pack_d"):
        rhs_copy.wait()
        for k in range(1, KT - 1):
            rows = pl.ds(PAD + T8 * k, T8)
            DP[rows, :] = packed(lambda x, k: DI[x, pl.ds(T8 * k, T8), :], k, 1, X - 1)
            PS[1, rows, :] = packed(lambda x, k: rhs[x, pl.ds(T8 * k, T8), :], k, 1, X - 1)

    with scope("wait0"):
        wait(0)

    halo_tiles = [pl.ds(a, T8) for a in range(0, YE, T8)]

    def sigma_halo(x, rows, components):
        for c, s in zip(components, look_known(V[0][x, rows, :], components)):
            S[c, x, rows, :] = s

    with scope("sigma_halo"):
        build_halo(0)
        for rows in halo_tiles:
            (HS[0, rows, :],) = look_known(HB[rows, :], (2,))
        CP[...] = HS[0]
        for x in (0, X + 1):
            for a in tiles:
                sigma_halo(x, pl.ds(a, T8), (0,))
        for x in range(1, X + 1):
            for a in (0, TOP):
                sigma_halo(x, pl.ds(a, T8), (1,))

    def diagonal(x, total, where):
        p = x + 1
        for a in where:
            rows, up, down = pl.ds(a, T8), pl.ds(a + 1, T8), pl.ds(a - 1, T8)
            own = pl.ds(a - PAD, T8)
            s2 = S[2, p, rows, :]
            face = pltpu.roll(CP[rows, :], lax.rem(LANES - 2 * x, LANES), 1)
            diag = look(6, lab[x, own, :]) + 2.0 * ((S[0, p, rows, :] + S[1, p, rows, :]) + s2)
            diag = diag + (S[0, p - 1, rows, :] + S[0, p + 1, rows, :])
            diag = diag + (S[1, p, down, :] + S[1, p, up, :])
            diag = diag + (jnp.where(lane_8 == 0, face, zm(s2)) + jnp.where(inner, zp(s2), face))
            inverse = 1.0 / diag
            DI[x, own, :] = inverse
            r0 = rhs[x, own, :]
            w = r0 * inverse
            V[1][p, rows, :] = w
            total = total + r0 * w
        return total

    def zero():
        return jnp.zeros((T8, LANES), f32)

    with scope("diag_x"):
        MA[0] = diagonal(X - 1, diagonal(0, zero(), tiles), tiles)
    with scope("startx_1"):
        start_x(1, field_tile(1))
    with scope("diag_rim"):
        total = MA[0]
        for x in range(1, X - 1):
            total = diagonal(x, total, (PAD, TOP - T8))
        MA[0] = total

    def assemble(r, known):
        for k in range(KT):
            rows = pl.ds(PAD + T8 * k, T8)
            if k in (0, KT - 1):
                tile = packed(field_tile(r), k, 0, X)
            else:
                tile = jnp.where(lane_8 >= 2 * X - 3, pltpu.roll(V[r][X, rows, :], 2 * X - 2, 1), known(rows))
                tile = jnp.where(ends, V[r][1, rows, :], tile)
            PS[r, rows, :] = tile
        spread(r)

    def first(rows):
        inverse = 1.0 / (DP[rows, :] + CP[rows, :])
        DP[rows, :] = inverse
        return PS[1, rows, :] * inverse

    with scope("pack_1"):
        assemble(1, first)
    with scope("start_1"):
        start_rest(1)
    with scope("diag_in"):
        width = group_size(X - 2, 10)

        @pl.loop(0, (X - 2) // width)
        def _(g):
            total = zero()
            for a in tiles[1:-1]:
                own, halo = pl.ds(a - PAD, T8), CP[pl.ds(a, T8), :]
                for i in range(width):
                    x = 1 + g * width + i
                    inverse = 1.0 / (DI[x, own, :] + unpack(halo, x))
                    DI[x, own, :] = inverse
                    r0 = rhs[x, own, :]
                    w = r0 * inverse
                    V[1][x + 1, pl.ds(a, T8), :] = w
                    total = total + r0 * w
            MA[0] = MA[0] + total

    with scope("coef"):
        for rows in halo_tiles:
            for i, s in enumerate(look_known(HB[rows, :], (4, 5))):
                HS[i + 1, rows, :] = s
            for i, s in enumerate(look_known(PS[0, rows, :], (2, 4, 5))):
                PG[i, rows, :] = s
            for x in (0, X + 1):
                sigma_halo(x, rows, (3, 4))
        sign = jnp.where(lane_8 % 2 == 0, f32(-1.0), f32(1.0))
        for a in tiles:
            rows = pl.ds(a, T8)
            own, beside, above = PG[1, rows, :], HS[1, rows, :], PG[2, rows, :]
            K[0, rows, :] = PG[0, rows, :] + HS[0, rows, :]
            K[1, rows, :] = sign * (own + pltpu.roll(beside, LANES - 2, 1))
            K[2, rows, :] = -sign * (own + pltpu.roll(beside, 2, 1))
            K[3, rows, :] = sign * (above + HS[2, pl.ds(a + 1, T8), :])
            K[4, rows, :] = -sign * (above + HS[2, pl.ds(a - 1, T8), :])

        @pl.loop(1, X + 1, unroll=4)
        def _(x):
            for a in (0, TOP):
                sigma_halo(x, pl.ds(a, T8), (3, 5))

        coefficients(0, [0] + tiles, False)
        coefficients(X, [0] + tiles)
        coefficients(X - 1, (0, PAD, TOP - T8))
        width = group_size(X - 2, 10)

        @pl.loop(0, (X - 2) // width)
        def _(g):
            for i in range(width):
                coefficients(1 + g * width + i, (0, PAD, TOP - T8))

    def planes(r, x0, width, where, ready=True):
        odd, evn = zero(), zero()
        field, nxt = V[r], V[r + 1]
        for a in where:
            rows, up, down = pl.ds(a, T8), pl.ds(a + 1, T8), pl.ds(a - 1, T8)
            own = pl.ds(a - PAD, T8)
            halo = CP[rows, :] if ready else None
            m, mu, md = field[x0, rows, :], field[x0, up, :], field[x0, down, :]
            v, vu, vd = field[x0 + 1, rows, :], field[x0 + 1, up, :], field[x0 + 1, down, :]
            tv = zp(v)
            acc = F[0, x0, rows, :] * m + F[3, x0, down, :] * md
            acc = acc - F[4, x0, rows, :] * mu - F[6, x0, rows, :] * zp(m)
            accs = F[5, x0, rows, :] * m
            for i in range(width):
                x = x0 + i
                p = x + 1
                n, nu, nd = field[p + 1, rows, :], field[p + 1, up, :], field[p + 1, down, :]
                tn = zp(n)
                f0 = F[0, p, rows, :]
                f2 = F[2, p, rows, :]
                f3, f3d = F[3, p, rows, :], F[3, p, down, :]
                f4, f4d = F[4, p, rows, :], F[4, p, down, :]
                f5, f6 = F[5, p, rows, :], F[6, p, rows, :]
                f7, f7d = F[7, p, rows, :], F[7, p, down, :]
                f8, f8d = F[8, p, rows, :], F[8, p, down, :]
                s = (accs + f2 * v) + (f7d * vd - f8 * vu) - f6 * n
                q = (acc + f0 * n) + (F[1, p, rows, :] * vu + F[1, p, down, :] * vd)
                q = q + (f3 * nu - f4d * nd) + (f2 * tv + f5 * tn)
                q = q + (f7 * zp(vu) - f8d * zp(vd))
                q = q + zm(s)
                if ready:
                    q = q + unpack(halo, x)
                acc = (f0 * v + f3d * vd) - (f4 * vu + f6 * tv)
                accs = f5 * v
                odd = odd + v * q
                w = q * DI[x, own, :]
                evn = evn + w * q
                nxt[p, rows, :] = w
                v, vu, vd, tv = n, nu, nd, tn
        return odd, evn

    def settle(r, x0, width, where):
        odd, evn = zero(), zero()
        for a in where:
            rows, own = pl.ds(a, T8), pl.ds(a - PAD, T8)
            halo = CP[rows, :]
            for i in range(width):
                x = x0 + i
                c = unpack(halo, x)
                w = V[r + 1][x + 1, rows, :]
                full = w + c * DI[x, own, :]
                V[r + 1][x + 1, rows, :] = full
                odd = odd + c * V[r][x + 1, rows, :]
                evn = evn + c * (w + full)
        return odd, evn

    def pairs(r, x0, width, where):
        total = zero()
        field = V[r]
        for a in where:
            rows, up = pl.ds(a, T8), pl.ds(a + 1, T8)
            v, vu = field[x0 + 1, rows, :], field[x0 + 1, up, :]
            tv, tvu = zp(v), zp(vu)
            for i in range(width):
                p = x0 + i + 1
                n, nu = field[p + 1, rows, :], field[p + 1, up, :]
                tn, tnu = zp(n), zp(nu)
                a0 = (F[0, p, rows, :] * n + F[1, p, rows, :] * vu) + (F[3, p, rows, :] * nu + F[5, p, rows, :] * tn)
                a0 = a0 + F[7, p, rows, :] * tvu
                a1 = F[2, p, rows, :] * v - F[6, p, rows, :] * n - F[8, p, rows, :] * vu
                total = total + v * a0 + (tv * a1 - (F[4, p, rows, :] * n) * vu)
                v, vu, tv, tvu = n, nu, tn, tnu
        return total

    def sums(step, parts):
        for i, part in enumerate(parts):
            MA[2 * step + 1 + i] = MA[2 * step + 1 + i] + part

    for step in range(ITERS):
        r = step + 1
        last = step + 1 == ITERS
        if last:
            with scope("early_sums"):
                tile = zero()
                for k in range(MOMENTS - 1):
                    value = jnp.sum(jnp.sum(MA[k], axis=0, keepdims=True), axis=1, keepdims=True)
                    tile = jnp.where(lane_8 == k, value, tile)
                CP[pl.ds(0, T8), :] = tile
        with scope(f"inner_{r}"):
            if last:
                width = group_size(X - 2, 10)
                MA[MOMENTS - 1] = pairs(r, X - 2, 1, tiles[:-1])

                @pl.loop(0, (X - 2) // width)
                def _(g):
                    MA[MOMENTS - 1] = MA[MOMENTS - 1] + pairs(r, g * width, width, tiles[:-1])
            else:
                width = group_size(X - 2, 10)

                @pl.loop(0, (X - 2) // width)
                def _(g):
                    sums(step, planes(r, 1 + g * width, width, tiles[1:-1], False))

        if not last:
            with scope(f"pack_in_{r}"):
                for k in range(1, KT - 1):
                    PS[r + 1, pl.ds(PAD + T8 * k, T8), :] = packed(field_tile(r + 1), k, 1, X - 1)
        with scope(f"wait_{r}"):
            wait(r)
        with scope(f"halo_{r}"):
            build_halo(r)
            for a in tiles:
                rows = pl.ds(a, T8)
                h = HB[rows, :]
                total = K[0, rows, :] * h + K[1, rows, :] * pltpu.roll(h, LANES - 2, 1)
                total = total + K[2, rows, :] * pltpu.roll(h, 2, 1)
                total = total + K[3, rows, :] * HB[pl.ds(a + 1, T8), :]
                CP[rows, :] = total + K[4, rows, :] * HB[pl.ds(a - 1, T8), :]
        if last:
            break
        with scope(f"edge_{r}"):
            sums(step, planes(r, 0, 1, tiles))
            sums(step, planes(r, X - 1, 1, tiles))
        with scope(f"startx_{r + 1}"):
            start_x(r + 1, field_tile(r + 1))
        with scope(f"rim_{r}"):
            sums(step, planes(r, 1, X - 2, (PAD, TOP - T8)))

        with scope(f"pack_{r + 1}"):
            assemble(r + 1, lambda rows: PS[r + 1, rows, :] + CP[rows, :] * DP[rows, :])
        with scope(f"start_{r + 1}"):
            start_rest(r + 1)
        with scope(f"settle_{r}"):
            width = group_size(X - 2, 15)

            @pl.loop(0, (X - 2) // width)
            def _(g):
                sums(step, settle(r, 1 + g * width, width, tiles[1:-1]))

    with scope("pairs"):
        mine = jnp.logical_and(lane_8 % 2 == 1, jnp.logical_or(lane_8 < 2 * (X - 1), lane_8 == LANES - 1))
        total = pairs(ROUNDS - 1, X - 1, 1, tiles)
        for a in tiles:
            rows = pl.ds(a, T8)
            total = total + jnp.where(mine, PS[ROUNDS - 1, rows, :] * CP[rows, :], 0.0)
        MA[MOMENTS - 1] = MA[MOMENTS - 1] + (total + pairs(ROUNDS - 1, 0, X - 1, (TOP - T8,)))

    def leave():
        wait_sent(ROUNDS - 1)

        @pl.loop(0, X, unroll=4)
        def _(x):
            for i in range(ITERS):
                for k in range(KT):
                    W[i, x, pl.ds(T8 * k, T8), :] = V[i + 1][x + 1, pl.ds(PAD + T8 * k, T8), :]

    with scope("allreduce"):
        value = jnp.sum(jnp.sum(MA[MOMENTS - 1], axis=0, keepdims=True), axis=1, keepdims=True)
        tile = jnp.where(lane_8 == MOMENTS - 1, 2.0 * value, CP[pl.ds(0, T8), :])
        for order, group in enumerate(groups):
            slot = 0
            members = 1
            for i in group:
                slot = slot * sizes[i] + me[i]
                members *= sizes[i]
            RS[order] = tile[0:1]
            others = offsets(group)
            for t in others:
                pltpu.make_async_remote_copy(
                    src_ref=RS.at[order],
                    dst_ref=RR.at[order, slot],
                    send_sem=ar_send.at[order],
                    recv_sem=ar_recv.at[order],
                    device_id=partner(t),
                    device_id_type=pl.DeviceIdType.MESH,
                ).start()
            RR[order, slot] = tile[0:1]
            if order == 0:
                leave()
            sent = RR.at[order, pl.ds(0, len(others))]
            pltpu.make_async_copy(sent, sent, ar_send.at[order]).wait()
            pltpu.make_async_copy(sent, sent, ar_recv.at[order]).wait()
            parts = [RR[order, t] for t in range(members)]
            while len(parts) > 1:
                parts = [sum(parts[i + 1 : i + 2], parts[i]) for i in range(0, len(parts), 2)]
            tile = jnp.broadcast_to(parts[0], (T8, LANES))

    n0, n1, n2, n3, n4, n5 = (
        jnp.sum(jnp.where(lane_8 == k, tile, 0.0)[0:1], axis=1, keepdims=True) for k in range(MOMENTS)
    )

    def inverse_of(d):
        return jnp.where(d > 0.0, 1.0 / d, 0.0)

    g00, g01, g02, g12, g22 = n0 - n1, n1 - n2, n2 - n3, n3 - n4, n4 - n5
    i0 = 1.0 / g00
    l1, l2 = g01 * i0, g02 * i0
    i1 = inverse_of(g02 - l1 * g01)
    e = g12 - l2 * g01
    l21 = e * i1
    i2 = inverse_of(g22 - l2 * g02 - l21 * e)
    y1 = n1 - l1 * n0
    y2 = n2 - l2 * n0 - l21 * y1
    c2 = y2 * i2
    c1 = y1 * i1 - l21 * c2
    c0 = n0 * i0 - l1 * c1 - l2 * c2

    for i, c in enumerate((c0, c1, c2)):
        C[pl.ds(i, 1), :] = jnp.broadcast_to(c, (1, LANES))


def combine(W, C, out, part, sem):
    X, Y, Z = out.shape
    rows = C[...]
    c = [jnp.broadcast_to(rows[i : i + 1], (T8, Z)) for i in range(ITERS)]
    pieces = sem.shape[0]
    width = X // pieces
    copies = []
    for g in range(pieces):
        @pl.loop(g * width, (g + 1) * width, unroll=4)
        def _(x):
            for k in range(Y // T8):
                own = pl.ds(T8 * k, T8)
                part[x, own, :] = (c[0] * W[0, x, own, :] + c[1] * W[1, x, own, :]) + c[2] * W[2, x, own, :]

        block = pl.ds(g * width, width)
        copies.append(pltpu.make_async_copy(part.at[block], out.at[block], sem.at[g]))
        copies[-1].start()
    for piece in copies:
        piece.wait()


def solution(mesh):
    sizes = tuple(mesh.shape[a] for a in AXES)

    def local(labels, conductivity, right_side):
        X, Y, Z = right_side.shape
        YE = Y + 2 * PAD
        f32 = jnp.float32
        vmem = pltpu.VMEM
        orders = len(groups_of(sizes))
        fields, factors = pl.pallas_call(
            functools.partial(kernel, sizes),
            out_shape=(vmem((ITERS, X, Y, Z), f32), vmem((T8, Z), f32)),
            in_specs=[
                pl.BlockSpec(memory_space=pl.ANY),
                pl.BlockSpec(memory_space=pl.ANY),
                pl.BlockSpec(memory_space=pl.ANY),
            ],
            out_specs=[pl.BlockSpec(memory_space=vmem)] * 2,
            scratch_shapes=[
                vmem((X, Y, Z), jnp.int32),
                pltpu.SMEM(conductivity.shape, f32),
                vmem((X, Y, Z), f32),
                vmem((X + 2, YE, Z), f32),
                vmem((X + 2, YE, Z), f32),
                vmem((X + 2, YE, Z), f32),
                vmem((X + 2, YE, Z), f32),
                vmem((6, X + 2, YE, Z), f32),
                vmem((9, X + 1, YE, Z), f32),
                vmem((X, Y, Z), f32),
                vmem((ROUNDS, YE, Z), f32),
                vmem((ROUNDS, 2, Y // 4, Z), f32),
                vmem((ROUNDS, 2, 2, T8, Z), f32),
                vmem((ROUNDS, 2, Y // 4, Z), f32),
                vmem((ROUNDS, 8, Z), f32),
                vmem((ROUNDS, 4, 8, Z), f32),
                vmem((YE, Z), f32),
                vmem((3, YE, Z), f32),
                vmem((3, YE, Z), f32),
                vmem((YE, Z), f32),
                vmem((YE, Z), f32),
                vmem((5, YE, Z), f32),
                vmem((MOMENTS, 8, Z), f32),
                vmem((2, 1, Z), f32),
                vmem((2, 32, 1, Z), f32),
                pltpu.SemaphoreType.DMA((2, 9)),
                pltpu.SemaphoreType.DMA((2, 9)),
                pltpu.SemaphoreType.DMA((orders,)),
                pltpu.SemaphoreType.DMA((orders,)),
                pltpu.SemaphoreType.DMA((5,)),
            ],
            compiler_params=pltpu.CompilerParams(
                collective_id=0, has_side_effects=True, vmem_limit_bytes=60 * 1024 * 1024
            ),
        )(labels, conductivity, right_side)
        return pl.pallas_call(
            combine,
            out_shape=jax.ShapeDtypeStruct((X, Y, Z), f32),
            in_specs=[pl.BlockSpec(memory_space=vmem)] * 2,
            out_specs=pl.BlockSpec(memory_space=pl.ANY),
            scratch_shapes=[vmem((X, Y, Z), f32), pltpu.SemaphoreType.DMA((group_size(X, 4),))],
            compiler_params=pltpu.CompilerParams(vmem_limit_bytes=8 * 1024 * 1024),
        )(fields, factors)

    return jax.shard_map(
        local,
        mesh=mesh,
        in_specs=(P("gx", "gy", "gz"), P(), P("gx", "gy", "gz")),
        out_specs=P("gx", "gy", "gz"),
        check_vma=False,
    )
```

```python
import functools
import itertools
import math
import jax
import jax.numpy as jnp
from jax import lax
from jax.experimental import pallas as pl
from jax.experimental.pallas import tpu as pltpu
from jax.sharding import PartitionSpec as P

ITERS = 3
AXES = ("gx", "gy", "gz")
ROUNDS = ITERS + 1
MOMENTS = 2 * ITERS
LANES = 128
PAD = 8
T8 = 8


def group_size(n, most):
    return max(u for u in range(1, most + 1) if n % u == 0)


def groups_of(sizes):
    return [(0, 1, 2)] if math.prod(sizes) <= 32 else [(0, 1), (2,)]


def kernel(
    sizes, lab_hbm, cond_hbm, rhs_hbm, W, C, lab, cond, rhs, V0, V1, V2, V3, S, F, DI, PS, PZ, PR, ZR, ES, ER, HB, HS, PG, CP,
    DP, K, MA, RS, RR, send_sem, recv_sem, ar_send, ar_recv, in_sem,
):
    V = (V0, V1, V2, V3)
    X, Y, Z = rhs.shape
    end_copies = []
    for i, x in enumerate((0, X - 1)):
        end_copies.append(pltpu.make_async_copy(lab_hbm.at[x], lab.at[x], in_sem.at[3 + i]))
        end_copies[-1].start()
    inside = pl.ds(1, X - 2)
    lab_copy = pltpu.make_async_copy(lab_hbm.at[inside], lab.at[inside], in_sem.at[0])
    lab_copy.start()
    cond_copy = pltpu.make_async_copy(cond_hbm, cond, in_sem.at[2])
    cond_copy.start()
    rhs_copy = pltpu.make_async_copy(rhs_hbm, rhs, in_sem.at[1])
    YE = Y + 2 * PAD
    TOP = PAD + Y
    KT = Y // T8
    me = [lax.axis_index(a) for a in AXES]
    f32 = jnp.float32
    scope = jax.named_scope

    directions = []
    for dx in (-1, 0, 1):
        for dy in (-1, 0, 1):
            for dz in (-1, 0, 1):
                d = (dx, dy, dz)
                live = sum(1 for t in d if t)
                if live in (1, 2) and all(n > 1 for t, n in zip(d, sizes) if t):
                    directions.append(d)

    def opposite(d):
        return tuple(-t for t in d)

    axes_of = [d for d in directions if d > opposite(d)]

    def needed(d, r):
        if r < ROUNDS - 1:
            return True
        if d[2]:
            return d[2] < 0
        return d[0] <= 0 and d[1] <= 0

    def present(d):
        ok = None
        for t, m, n in zip(d, me, sizes):
            if t == 0:
                continue
            here = (m < n - 1) if t > 0 else (m > 0)
            ok = here if ok is None else jnp.logical_and(ok, here)
        return ok

    def places(d, r):
        dx, dy, dz = d
        rows_from = pl.ds(PAD, Y) if dy == 0 else (pl.ds(TOP - 1, 1) if dy > 0 else pl.ds(PAD, 1))
        rows_to = pl.ds(PAD, Y) if dy == 0 else (pl.ds(PAD - 1, 1) if dy > 0 else pl.ds(TOP, 1))
        if dz == 0:
            if dx == 0:
                return V[r].at[pl.ds(1, X), rows_from], V[r].at[pl.ds(1, X), rows_to]
            fx, tx = (X, 0) if dx > 0 else (1, X + 1)
            return V[r].at[fx, rows_from], V[r].at[tx, rows_to]
        side = 0 if dz > 0 else 1
        if dx == 0 and dy == 0:
            return PZ.at[r, side], ZR.at[r, side]
        if dx == 0:
            return PS.at[r, rows_from], PR.at[r, side, 0 if dy > 0 else 1, pl.ds(PAD - 1 if dy > 0 else 0, 1)]
        slot = (0 if dx > 0 else 2) + side
        return ES.at[r], ER.at[r, slot]

    def copy(d, r):
        src, dst = places(d, r)
        m = axes_of.index(max(d, opposite(d)))
        return pltpu.make_async_remote_copy(
            src_ref=src,
            dst_ref=dst,
            send_sem=send_sem.at[r % 2, m],
            recv_sem=recv_sem.at[r % 2, m],
            device_id=tuple(a + t for a, t in zip(me, d)),
            device_id_type=pl.DeviceIdType.MESH,
        )

    groups = groups_of(sizes)
    near = len(groups) == 1 and max(sizes) <= ROUNDS and sum(n - 1 for n in sizes) <= 2 * ROUNDS - 1

    def offsets(group):
        ranges = [range(n) if i in group else (0,) for i, n in enumerate(sizes)]
        return [t for t in itertools.product(*ranges) if any(t)]

    def partner(t):
        return tuple(lax.rem(m + k, n) for m, k, n in zip(me, t, sizes))

    barrier = pltpu.get_barrier_semaphore()
    greeted = 0
    if not near:
        for group in groups:
            for t in offsets(group):
                pl.semaphore_signal(
                    barrier, inc=1, device_id=partner(t), device_id_type=pl.DeviceIdType.MESH
                )
                greeted += 1
    if near or len(groups) > 1:
        for d in directions:
            pl.when(present(d))(
                lambda d=d: pl.semaphore_signal(
                    barrier,
                    inc=1,
                    device_id=tuple(a + t for a, t in zip(me, d)),
                    device_id_type=pl.DeviceIdType.MESH,
                )
            )
            greeted = greeted + jnp.where(present(d), 1, 0)

    for d in [
        (dx, dy, dz)
        for dx in (-1, 0, 1)
        for dy in (-1, 0, 1)
        for dz in (-1, 0, 1)
        if sum(1 for t in (dx, dy, dz) if t) in (1, 2)
    ]:
        def clear(d=d):
            for r in range(ROUNDS):
                if needed(d, r):
                    _, dst = places(d, r)
                    dst[...] = jnp.zeros(dst.shape, f32)

        if d in directions:
            back = tuple(-t for t in d)
            pl.when(jnp.logical_not(present(back)))(clear)
        else:
            clear()

    for r in range(ROUNDS):
        for a in (0, TOP):
            PS[r, pl.ds(a, PAD), :] = jnp.zeros((PAD, LANES), f32)
    for r in range(ROUNDS):
        for side in range(2):
            PR[r, side, 0, pl.ds(0, PAD - 1), :] = jnp.zeros((PAD - 1, LANES), f32)
            PR[r, side, 1, pl.ds(1, PAD - 1), :] = jnp.zeros((PAD - 1, LANES), f32)
    for x in range(X + 2):
        V[0][x, pl.ds(0, PAD - 1), :] = jnp.zeros((PAD - 1, LANES), f32)
        V[0][x, pl.ds(TOP + 1, PAD - 1), :] = jnp.zeros((PAD - 1, LANES), f32)
    MA[...] = jnp.zeros(MA.shape, f32)

    lane_8 = lax.broadcasted_iota(jnp.int32, (T8, LANES), 1)
    row_8 = lax.broadcasted_iota(jnp.int32, (T8, LANES), 0)
    ends = jnp.logical_or(lane_8 == 0, lane_8 == LANES - 1)
    inner = lane_8 < LANES - 1
    tiles = [PAD + T8 * k for k in range(KT)]

    by_row = lax.GatherDimensionNumbers(
        offset_dims=(),
        collapsed_slice_dims=(0,),
        start_index_map=(0,),
        operand_batching_dims=(1,),
        start_indices_batching_dims=(1,),
    )

    def look(c, index):
        return lax.gather(
            tables[c], index[..., None], by_row, (1, 1), mode=lax.GatherScatterMode.PROMISE_IN_BOUNDS
        )

    def look_known(values, components):
        index = jnp.maximum(values.astype(jnp.int32) - 1, 0)
        hit = values > 0.0
        return [jnp.where(hit, look(c, index), 0.0) for c in components]

    half = LANES // 2
    span = LANES - 2 - 2 * X
    offs = (0, 1, half, half + 1)
    slots_of = [jnp.logical_and(lane_8 % 2 == off % 2, (lane_8 < half) == (off < half)) for off in offs]

    def send(d, r):
        if d in directions and needed(d, r):
            pl.when(present(d))(lambda: copy(d, r).start())

    def start_x(r, plane):
        tile = jnp.zeros((T8, LANES), f32)
        for x, base in ((0, 0), (X - 1, span)):
            for k in range(KT):
                to = base + 2 * k
                here = jnp.logical_or(lane_8 == to, lane_8 == to + 1)
                tile = jnp.where(here, pltpu.roll(plane(x, k), to + 1, 1), tile)
        ES[r] = tile
        outer = sorted((d for d in directions if d[0]), key=lambda d: (-abs(d[2]), -abs(d[1])))

        def both(side):
            for t in (side, -side):
                for d in outer:
                    if d[0] == t:
                        send(d, r)

        far = lax.rem(me[0], 2) == 1
        pl.when(far)(lambda: both(1))
        pl.when(jnp.logical_not(far))(lambda: both(-1))

    def start_rest(r):
        for d in sorted(directions, key=lambda d: (-abs(d[2]), -abs(d[1]))):
            if not d[0]:
                send(d, r)

    def two(d):
        dx, dy, dz = map(abs, d)
        if dx + dy + dz == 2:
            return F.at[0, 0, pl.ds(0, 2 * T8 if dx and dz else 2)]
        if dz:
            return F.at[0, 0, pl.ds(0, Y // 2)]
        return F.at[0, pl.ds(0, 2), pl.ds(0, Y)] if dx else F.at[0, pl.ds(0, X), pl.ds(0, 2)]

    def settle_pair(d, r, sent):
        back = opposite(d)
        ways = [t for t in (d, back) if needed(t, r)]
        here = [present(t if sent else opposite(t)) for t in ways]

        def one():
            c = copy(ways[0], r)
            c.wait_send() if sent else c.wait_recv()

        if len(ways) == 1:
            pl.when(here[0])(one)
        elif ways:
            sems = send_sem if sent else recv_sem

            @pl.when(jnp.logical_and(*here))
            def _():
                pltpu.make_async_copy(two(d), two(d), sems.at[r % 2, axes_of.index(d)]).wait()

            pl.when(jnp.logical_xor(*here))(one)

    def wait_sent(r):
        for d in axes_of:
            settle_pair(d, r, True)

    def wait(r):
        if r:
            wait_sent(r - 1)
        for d in axes_of:
            settle_pair(d, r, False)

    def spread(r):
        for side in range(2):
            if side == 0 and r == ROUNDS - 1:
                continue
            for t in range(KT // 4):
                tile = None
                for j, off in enumerate(offs):
                    part = PS[r, pl.ds(PAD + T8 * (4 * t + j), T8), :]
                    part = pltpu.roll(part, (off + 1 - side) % LANES, 1) if off + 1 - side else part
                    tile = part if tile is None else jnp.where(slots_of[j], part, tile)
                PZ[r, side, pl.ds(T8 * t, T8), :] = tile

    def build_halo(r):
        valid = jnp.logical_or(lane_8 <= 2 * (X - 1), lane_8 == LANES - 1)
        even = lane_8 % 2 == 0
        last = r == ROUNDS - 1

        def join(low, high):
            return jnp.where(valid, jnp.where(even, 0.0 if last else low, high), 0.0)

        for i, a in enumerate((0, TOP)):
            low = None if last else pltpu.roll(PR[r, 0, i], 1, 1)
            HB[pl.ds(a, T8), :] = join(low, pltpu.roll(PR[r, 1, i], LANES - 1, 1))
        for k in range(KT):
            t, off = pl.ds(T8 * (k // 4), T8), offs[k % 4]
            low = None if last else pltpu.roll(ZR[r, 0, t, :], (LANES - off) % LANES, 1)
            high = pltpu.roll(ZR[r, 1, t, :], LANES - 1 - off, 1)
            HB[pl.ds(PAD + T8 * k, T8), :] = join(low, high)
        got = [(1, jnp.where(lane_8 < span, ER[r, 3], ER[r, 1]))]
        if not last:
            got.append((0, jnp.where(lane_8 < span, ER[r, 2], ER[r, 0])))
        for k in range(KT):
            rows = pl.ds(PAD + T8 * k, T8)
            part = HB[rows, :]
            for i, tile in got:
                here = jnp.logical_or(lane_8 == 2 * X - i, lane_8 == LANES - 2 - i)
                part = jnp.where(here, pltpu.roll(tile, (2 * X - 2 * i - 2 * k) % LANES, 1), part)
            HB[rows, :] = part

    def zm(a):
        return pltpu.roll(a, 1, 1)

    def zp(a):
        return pltpu.roll(a, LANES - 1, 1)

    def unpack(part, x):
        return jnp.where(ends, pltpu.roll(part, lax.rem(LANES - 2 * x, LANES), 1), 0.0)

    def packed(plane, k, first, last):
        tile = None
        for x in range(first, last):
            part = pltpu.roll(plane(x, k), 2 * x, 1) if x else plane(x, k)
            tile = part if tile is None else jnp.where(jnp.logical_and(lane_8 >= 2 * x - 1, inner), part, tile)
        return tile

    def pack(r, plane):
        for k in range(KT):
            PS[r, pl.ds(PAD + T8 * k, T8), :] = packed(plane, k, 0, X)

    def label_tile(x, k):
        return (lab[x, pl.ds(T8 * k, T8), :] + 1).astype(f32)

    def field_tile(r):
        return lambda x, k: V[r][x + 1, pl.ds(PAD + T8 * k, T8), :]

    with scope("endwait"):
        for end_copy in end_copies:
            end_copy.wait()
    with scope("conv"):
        for x in (0, X - 1):
            for k in range(KT):
                V[0][x + 1, pl.ds(PAD + T8 * k, T8), :] = label_tile(x, k)
    with scope("barrier"):
        pl.semaphore_wait(barrier, greeted)
    with scope("start0"):
        start_x(0, label_tile)
    with scope("labwait"):
        lab_copy.wait()
        rhs_copy.start()
    with scope("pack0"):
        for x in range(1, X - 1):
            for k in (0, KT - 1):
                V[0][x + 1, pl.ds(PAD + T8 * k, T8), :] = label_tile(x, k)
        pack(0, label_tile)
        spread(0)
    with scope("start_0"):
        start_rest(0)

    cond_copy.wait()
    scale = (0.5, 0.5, 0.5, 0.25, 0.25, 0.25, 1.0)
    count = cond.shape[1]
    tables = []
    for c in range(7):
        table = jnp.zeros((T8, LANES), f32)
        for k in range(count):
            table = jnp.where(row_8 == k, cond[c, k] * scale[c], table)
        tables.append(table)


    def sigma_own(x, where, components=range(6)):
        for a in where:
            index = lab[x, pl.ds(a - PAD, T8), :]
            for c in components:
                S[c, x + 1, pl.ds(a, T8), :] = look(c, index)

    with scope("sigma_own"):
        @pl.loop(0, X, unroll=4)
        def _(x):
            sigma_own(x, (tiles[0], tiles[-1]))
            sigma_own(x, (tiles[1],), (1, 3, 5))
            sigma_own(x, (tiles[-2],), (1,))

        for x in (0, 1, X - 2, X - 1):
            sigma_own(x, tiles[1:-1])

    def coefficients(p, where, inside=True):
        for a in where:
            rows, up = pl.ds(a, T8), pl.ds(a + 1, T8)
            s3, s3u = S[3, p, rows, :], S[3, p, up, :]
            t3, t3u = S[3, p + 1, rows, :], S[3, p + 1, up, :]
            F[3, p, rows, :] = s3 + t3u
            F[4, p, rows, :] = t3 + s3u
            if inside:
                s5, s5u = S[5, p, rows, :], S[5, p, up, :]
                F[1, p, rows, :] = S[1, p, rows, :] + S[1, p, up, :]
                F[7, p, rows, :] = jnp.where(inner, s5 + zp(s5u), 0.0)
                F[8, p, rows, :] = jnp.where(inner, s5u + zp(s5), 0.0)
            if a:
                s4, t4 = S[4, p, rows, :], S[4, p + 1, rows, :]
                F[0, p, rows, :] = S[0, p, rows, :] + S[0, p + 1, rows, :]
                F[5, p, rows, :] = jnp.where(inner, s4 + zp(t4), 0.0)
                F[6, p, rows, :] = jnp.where(inner, t4 + zp(s4), 0.0)
                if inside:
                    s2 = S[2, p, rows, :]
                    F[2, p, rows, :] = jnp.where(inner, s2 + zp(s2), 0.0)

    def inside_of(x0, width, where):
        for a in where:
            rows = pl.ds(a, T8)
            own, up, down = (pl.ds(a - PAD + i, T8) for i in (0, 1, -1))
            here, above = lab[x0, own, :], lab[x0, up, :]
            s0, s3, s4, s3u = look(0, here), look(3, here), look(4, here), look(3, above)
            f0m = look(0, lab[x0 - 1, own, :]) + s0
            for i in range(width):
                x = x0 + i
                p = x + 1
                there, beyond = lab[x + 1, own, :], lab[x + 1, up, :]
                n0, n3, n4, n3u = look(0, there), look(3, there), look(4, there), look(3, beyond)
                s1, s2, s5 = look(1, here), look(2, here), look(5, here)
                s1u, s5u = look(1, above), look(5, above)
                f0, f1 = s0 + n0, s1 + s1u
                f2 = jnp.where(inner, s2 + zp(s2), 0.0)
                F[0, p, rows, :] = f0
                F[1, p, rows, :] = f1
                F[2, p, rows, :] = f2
                F[3, p, rows, :] = s3 + n3u
                F[4, p, rows, :] = n3 + s3u
                F[5, p, rows, :] = jnp.where(inner, s4 + zp(n4), 0.0)
                F[6, p, rows, :] = jnp.where(inner, n4 + zp(s4), 0.0)
                F[7, p, rows, :] = jnp.where(inner, s5 + zp(s5u), 0.0)
                F[8, p, rows, :] = jnp.where(inner, s5u + zp(s5), 0.0)
                diag = (look(6, here) + (f0m + f0)) + (f1 + (s1 + look(1, lab[x, down, :])))
                DI[x, own, :] = diag + ((f2 + zm(f2)) + jnp.where(ends, s2, 0.0))
                here, above, f0m = there, beyond, f0
                s0, s3, s4, s3u = n0, n3, n4, n3u

    with scope("coef_in"):
        width = group_size(X - 2, 5)
        for t in range(1, KT - 1, 3):
            @pl.loop(0, (X - 2) // width)
            def _(g, t=t):
                inside_of(1 + g * width, width, tiles[t : min(t + 3, KT - 1)])

        coefficients(1, tiles[1:-1])
    with scope("pack_d"):
        rhs_copy.wait()
        for k in range(1, KT - 1):
            rows = pl.ds(PAD + T8 * k, T8)
            DP[rows, :] = packed(lambda x, k: DI[x, pl.ds(T8 * k, T8), :], k, 1, X - 1)
            PS[1, rows, :] = packed(lambda x, k: rhs[x, pl.ds(T8 * k, T8), :], k, 1, X - 1)

    with scope("wait0"):
        wait(0)

    halo_tiles = [pl.ds(a, T8) for a in range(0, YE, T8)]

    def sigma_halo(x, rows, components):
        for c, s in zip(components, look_known(V[0][x, rows, :], components)):
            S[c, x, rows, :] = s

    with scope("sigma_halo"):
        build_halo(0)
        for rows in halo_tiles:
            (HS[0, rows, :],) = look_known(HB[rows, :], (2,))
        CP[...] = HS[0]
        for x in (0, X + 1):
            for a in tiles:
                sigma_halo(x, pl.ds(a, T8), (0,))
        for x in range(1, X + 1):
            for a in (0, TOP):
                sigma_halo(x, pl.ds(a, T8), (1,))

    def diagonal(x, total, where):
        p = x + 1
        for a in where:
            rows, up, down = pl.ds(a, T8), pl.ds(a + 1, T8), pl.ds(a - 1, T8)
            own = pl.ds(a - PAD, T8)
            s2 = S[2, p, rows, :]
            face = pltpu.roll(CP[rows, :], lax.rem(LANES - 2 * x, LANES), 1)
            diag = look(6, lab[x, own, :]) + 2.0 * ((S[0, p, rows, :] + S[1, p, rows, :]) + s2)
            diag = diag + (S[0, p - 1, rows, :] + S[0, p + 1, rows, :])
            diag = diag + (S[1, p, down, :] + S[1, p, up, :])
            diag = diag + (jnp.where(lane_8 == 0, face, zm(s2)) + jnp.where(inner, zp(s2), face))
            inverse = 1.0 / diag
            DI[x, own, :] = inverse
            r0 = rhs[x, own, :]
            w = r0 * inverse
            V[1][p, rows, :] = w
            total = total + r0 * w
        return total

    def zero():
        return jnp.zeros((T8, LANES), f32)

    with scope("diag_x"):
        MA[0] = diagonal(X - 1, diagonal(0, zero(), tiles), tiles)
    with scope("startx_1"):
        start_x(1, field_tile(1))
    with scope("diag_rim"):
        total = MA[0]
        for x in range(1, X - 1):
            total = diagonal(x, total, (PAD, TOP - T8))
        MA[0] = total

    def assemble(r, known):
        for k in range(KT):
            rows = pl.ds(PAD + T8 * k, T8)
            if k in (0, KT - 1):
                tile = packed(field_tile(r), k, 0, X)
            else:
                tile = jnp.where(lane_8 >= 2 * X - 3, pltpu.roll(V[r][X, rows, :], 2 * X - 2, 1), known(rows))
                tile = jnp.where(ends, V[r][1, rows, :], tile)
            PS[r, rows, :] = tile
        spread(r)

    def first(rows):
        inverse = 1.0 / (DP[rows, :] + CP[rows, :])
        DP[rows, :] = inverse
        return PS[1, rows, :] * inverse

    with scope("pack_1"):
        assemble(1, first)
    with scope("start_1"):
        start_rest(1)
    with scope("diag_in"):
        width = group_size(X - 2, 10)

        @pl.loop(0, (X - 2) // width)
        def _(g):
            total = zero()
            for a in tiles[1:-1]:
                own, halo = pl.ds(a - PAD, T8), CP[pl.ds(a, T8), :]
                for i in range(width):
                    x = 1 + g * width + i
                    inverse = 1.0 / (DI[x, own, :] + unpack(halo, x))
                    DI[x, own, :] = inverse
                    r0 = rhs[x, own, :]
                    w = r0 * inverse
                    V[1][x + 1, pl.ds(a, T8), :] = w
                    total = total + r0 * w
            MA[0] = MA[0] + total

    with scope("coef"):
        for rows in halo_tiles:
            for i, s in enumerate(look_known(HB[rows, :], (4, 5))):
                HS[i + 1, rows, :] = s
            for i, s in enumerate(look_known(PS[0, rows, :], (2, 4, 5))):
                PG[i, rows, :] = s
            for x in (0, X + 1):
                sigma_halo(x, rows, (3, 4))
        sign = jnp.where(lane_8 % 2 == 0, f32(-1.0), f32(1.0))
        for a in tiles:
            rows = pl.ds(a, T8)
            own, beside, above = PG[1, rows, :], HS[1, rows, :], PG[2, rows, :]
            K[0, rows, :] = PG[0, rows, :] + HS[0, rows, :]
            K[1, rows, :] = sign * (own + pltpu.roll(beside, LANES - 2, 1))
            K[2, rows, :] = -sign * (own + pltpu.roll(beside, 2, 1))
            K[3, rows, :] = sign * (above + HS[2, pl.ds(a + 1, T8), :])
            K[4, rows, :] = -sign * (above + HS[2, pl.ds(a - 1, T8), :])

        @pl.loop(1, X + 1, unroll=4)
        def _(x):
            for a in (0, TOP):
                sigma_halo(x, pl.ds(a, T8), (3, 5))

        coefficients(0, [0] + tiles, False)
        coefficients(X, [0] + tiles)
        coefficients(X - 1, (0, PAD, TOP - T8))
        width = group_size(X - 2, 10)

        @pl.loop(0, (X - 2) // width)
        def _(g):
            for i in range(width):
                coefficients(1 + g * width + i, (0, PAD, TOP - T8))

    def planes(r, x0, width, where, ready=True):
        odd, evn = zero(), zero()
        field, nxt = V[r], V[r + 1]
        for a in where:
            rows, up, down = pl.ds(a, T8), pl.ds(a + 1, T8), pl.ds(a - 1, T8)
            own = pl.ds(a - PAD, T8)
            halo = CP[rows, :] if ready else None
            m, mu, md = field[x0, rows, :], field[x0, up, :], field[x0, down, :]
            v, vu, vd = field[x0 + 1, rows, :], field[x0 + 1, up, :], field[x0 + 1, down, :]
            tv = zp(v)
            acc = F[0, x0, rows, :] * m + F[3, x0, down, :] * md
            acc = acc - F[4, x0, rows, :] * mu - F[6, x0, rows, :] * zp(m)
            accs = F[5, x0, rows, :] * m
            for i in range(width):
                x = x0 + i
                p = x + 1
                n, nu, nd = field[p + 1, rows, :], field[p + 1, up, :], field[p + 1, down, :]
                tn = zp(n)
                f0 = F[0, p, rows, :]
                f2 = F[2, p, rows, :]
                f3, f3d = F[3, p, rows, :], F[3, p, down, :]
                f4, f4d = F[4, p, rows, :], F[4, p, down, :]
                f5, f6 = F[5, p, rows, :], F[6, p, rows, :]
                f7, f7d = F[7, p, rows, :], F[7, p, down, :]
                f8, f8d = F[8, p, rows, :], F[8, p, down, :]
                s = (accs + f2 * v) + (f7d * vd - f8 * vu) - f6 * n
                q = (acc + f0 * n) + (F[1, p, rows, :] * vu + F[1, p, down, :] * vd)
                q = q + (f3 * nu - f4d * nd) + (f2 * tv + f5 * tn)
                q = q + (f7 * zp(vu) - f8d * zp(vd))
                q = q + zm(s)
                if ready:
                    q = q + unpack(halo, x)
                acc = (f0 * v + f3d * vd) - (f4 * vu + f6 * tv)
                accs = f5 * v
                odd = odd + v * q
                w = q * DI[x, own, :]
                evn = evn + w * q
                nxt[p, rows, :] = w
                v, vu, vd, tv = n, nu, nd, tn
        return odd, evn

    def settle(r, x0, width, where):
        odd, evn = zero(), zero()
        for a in where:
            rows, own = pl.ds(a, T8), pl.ds(a - PAD, T8)
            halo = CP[rows, :]
            for i in range(width):
                x = x0 + i
                c = unpack(halo, x)
                w = V[r + 1][x + 1, rows, :]
                full = w + c * DI[x, own, :]
                V[r + 1][x + 1, rows, :] = full
                odd = odd + c * V[r][x + 1, rows, :]
                evn = evn + c * (w + full)
        return odd, evn

    def pairs(r, x0, width, where):
        total = zero()
        field = V[r]
        for a in where:
            rows, up = pl.ds(a, T8), pl.ds(a + 1, T8)
            v, vu = field[x0 + 1, rows, :], field[x0 + 1, up, :]
            tv, tvu = zp(v), zp(vu)
            for i in range(width):
                p = x0 + i + 1
                n, nu = field[p + 1, rows, :], field[p + 1, up, :]
                tn, tnu = zp(n), zp(nu)
                a0 = (F[0, p, rows, :] * n + F[1, p, rows, :] * vu) + (F[3, p, rows, :] * nu + F[5, p, rows, :] * tn)
                a0 = a0 + F[7, p, rows, :] * tvu
                a1 = F[2, p, rows, :] * v - F[6, p, rows, :] * n - F[8, p, rows, :] * vu
                total = total + v * a0 + (tv * a1 - (F[4, p, rows, :] * n) * vu)
                v, vu, tv, tvu = n, nu, tn, tnu
        return total

    def sums(step, parts):
        for i, part in enumerate(parts):
            MA[2 * step + 1 + i] = MA[2 * step + 1 + i] + part

    for step in range(ITERS):
        r = step + 1
        last = step + 1 == ITERS
        if last:
            with scope("early_sums"):
                tile = zero()
                for k in range(MOMENTS - 1):
                    value = jnp.sum(jnp.sum(MA[k], axis=0, keepdims=True), axis=1, keepdims=True)
                    tile = jnp.where(lane_8 == k, value, tile)
                CP[pl.ds(0, T8), :] = tile
        with scope(f"inner_{r}"):
            if last:
                width = group_size(X - 2, 10)
                MA[MOMENTS - 1] = pairs(r, X - 2, 1, tiles[:-1])

                @pl.loop(0, (X - 2) // width)
                def _(g):
                    MA[MOMENTS - 1] = MA[MOMENTS - 1] + pairs(r, g * width, width, tiles[:-1])
            else:
                width = group_size(X - 2, 10)

                @pl.loop(0, (X - 2) // width)
                def _(g):
                    sums(step, planes(r, 1 + g * width, width, tiles[1:-1], False))

        if not last:
            with scope(f"pack_in_{r}"):
                for k in range(1, KT - 1):
                    PS[r + 1, pl.ds(PAD + T8 * k, T8), :] = packed(field_tile(r + 1), k, 1, X - 1)
        with scope(f"wait_{r}"):
            wait(r)
        with scope(f"halo_{r}"):
            build_halo(r)
            for a in tiles:
                rows = pl.ds(a, T8)
                h = HB[rows, :]
                total = K[0, rows, :] * h + K[1, rows, :] * pltpu.roll(h, LANES - 2, 1)
                total = total + K[2, rows, :] * pltpu.roll(h, 2, 1)
                total = total + K[3, rows, :] * HB[pl.ds(a + 1, T8), :]
                CP[rows, :] = total + K[4, rows, :] * HB[pl.ds(a - 1, T8), :]
        if last:
            break
        with scope(f"edge_{r}"):
            sums(step, planes(r, 0, 1, tiles))
            sums(step, planes(r, X - 1, 1, tiles))
        with scope(f"startx_{r + 1}"):
            start_x(r + 1, field_tile(r + 1))
        with scope(f"rim_{r}"):
            sums(step, planes(r, 1, X - 2, (PAD, TOP - T8)))

        with scope(f"pack_{r + 1}"):
            assemble(r + 1, lambda rows: PS[r + 1, rows, :] + CP[rows, :] * DP[rows, :])
        with scope(f"start_{r + 1}"):
            start_rest(r + 1)
        with scope(f"settle_{r}"):
            width = group_size(X - 2, 15)

            @pl.loop(0, (X - 2) // width)
            def _(g):
                sums(step, settle(r, 1 + g * width, width, tiles[1:-1]))

    with scope("pairs"):
        mine = jnp.logical_and(lane_8 % 2 == 1, jnp.logical_or(lane_8 < 2 * (X - 1), lane_8 == LANES - 1))
        total = pairs(ROUNDS - 1, X - 1, 1, tiles)
        for a in tiles:
            rows = pl.ds(a, T8)
            total = total + jnp.where(mine, PS[ROUNDS - 1, rows, :] * CP[rows, :], 0.0)
        MA[MOMENTS - 1] = MA[MOMENTS - 1] + (total + pairs(ROUNDS - 1, 0, X - 1, (TOP - T8,)))

    def leave():
        wait_sent(ROUNDS - 1)

        @pl.loop(0, X, unroll=4)
        def _(x):
            for i in range(ITERS):
                for k in range(KT):
                    W[i, x, pl.ds(T8 * k, T8), :] = V[i + 1][x + 1, pl.ds(PAD + T8 * k, T8), :]

    with scope("allreduce"):
        value = jnp.sum(jnp.sum(MA[MOMENTS - 1], axis=0, keepdims=True), axis=1, keepdims=True)
        tile = jnp.where(lane_8 == MOMENTS - 1, 2.0 * value, CP[pl.ds(0, T8), :])
        for order, group in enumerate(groups):
            slot = 0
            members = 1
            for i in group:
                slot = slot * sizes[i] + me[i]
                members *= sizes[i]
            RS[order] = tile[0:1]
            others = offsets(group)
            for t in others:
                pltpu.make_async_remote_copy(
                    src_ref=RS.at[order],
                    dst_ref=RR.at[order, slot],
                    send_sem=ar_send.at[order],
                    recv_sem=ar_recv.at[order],
                    device_id=partner(t),
                    device_id_type=pl.DeviceIdType.MESH,
                ).start()
            RR[order, slot] = tile[0:1]
            if order == 0:
                leave()
            sent = RR.at[order, pl.ds(0, len(others))]
            pltpu.make_async_copy(sent, sent, ar_send.at[order]).wait()
            pltpu.make_async_copy(sent, sent, ar_recv.at[order]).wait()
            parts = [RR[order, t] for t in range(members)]
            while len(parts) > 1:
                parts = [sum(parts[i + 1 : i + 2], parts[i]) for i in range(0, len(parts), 2)]
            tile = jnp.broadcast_to(parts[0], (T8, LANES))

    n0, n1, n2, n3, n4, n5 = (
        jnp.sum(jnp.where(lane_8 == k, tile, 0.0)[0:1], axis=1, keepdims=True) for k in range(MOMENTS)
    )

    def inverse_of(d):
        return jnp.where(d > 0.0, 1.0 / d, 0.0)

    g00, g01, g02, g12, g22 = n0 - n1, n1 - n2, n2 - n3, n3 - n4, n4 - n5
    i0 = 1.0 / g00
    l1, l2 = g01 * i0, g02 * i0
    i1 = inverse_of(g02 - l1 * g01)
    e = g12 - l2 * g01
    l21 = e * i1
    i2 = inverse_of(g22 - l2 * g02 - l21 * e)
    y1 = n1 - l1 * n0
    y2 = n2 - l2 * n0 - l21 * y1
    c2 = y2 * i2
    c1 = y1 * i1 - l21 * c2
    c0 = n0 * i0 - l1 * c1 - l2 * c2

    for i, c in enumerate((c0, c1, c2)):
        C[pl.ds(i, 1), :] = jnp.broadcast_to(c, (1, LANES))


def combine(W, C, out, part, sem):
    X, Y, Z = out.shape
    rows = C[...]
    c = [jnp.broadcast_to(rows[i : i + 1], (T8, Z)) for i in range(ITERS)]
    pieces = sem.shape[0]
    width = X // pieces
    copies = []
    for g in range(pieces):
        @pl.loop(g * width, (g + 1) * width, unroll=4)
        def _(x):
            for k in range(Y // T8):
                own = pl.ds(T8 * k, T8)
                part[x, own, :] = (c[0] * W[0, x, own, :] + c[1] * W[1, x, own, :]) + c[2] * W[2, x, own, :]

        block = pl.ds(g * width, width)
        copies.append(pltpu.make_async_copy(part.at[block], out.at[block], sem.at[g]))
        copies[-1].start()
    for piece in copies:
        piece.wait()


def solution(mesh):
    sizes = tuple(mesh.shape[a] for a in AXES)

    def local(labels, conductivity, right_side):
        X, Y, Z = right_side.shape
        YE = Y + 2 * PAD
        f32 = jnp.float32
        vmem = pltpu.VMEM
        orders = len(groups_of(sizes))
        fields, factors = pl.pallas_call(
            functools.partial(kernel, sizes),
            out_shape=(vmem((ITERS, X, Y, Z), f32), vmem((T8, Z), f32)),
            in_specs=[
                pl.BlockSpec(memory_space=pl.ANY),
                pl.BlockSpec(memory_space=pl.ANY),
                pl.BlockSpec(memory_space=pl.ANY),
            ],
            out_specs=[pl.BlockSpec(memory_space=vmem)] * 2,
            scratch_shapes=[
                vmem((X, Y, Z), jnp.int32),
                pltpu.SMEM(conductivity.shape, f32),
                vmem((X, Y, Z), f32),
                vmem((X + 2, YE, Z), f32),
                vmem((X + 2, YE, Z), f32),
                vmem((X + 2, YE, Z), f32),
                vmem((X + 2, YE, Z), f32),
                vmem((6, X + 2, YE, Z), f32),
                vmem((9, X + 1, YE, Z), f32),
                vmem((X, Y, Z), f32),
                vmem((ROUNDS, YE, Z), f32),
                vmem((ROUNDS, 2, Y // 4, Z), f32),
                vmem((ROUNDS, 2, 2, T8, Z), f32),
                vmem((ROUNDS, 2, Y // 4, Z), f32),
                vmem((ROUNDS, 8, Z), f32),
                vmem((ROUNDS, 4, 8, Z), f32),
                vmem((YE, Z), f32),
                vmem((3, YE, Z), f32),
                vmem((3, YE, Z), f32),
                vmem((YE, Z), f32),
                vmem((YE, Z), f32),
                vmem((5, YE, Z), f32),
                vmem((MOMENTS, 8, Z), f32),
                vmem((2, 1, Z), f32),
                vmem((2, 32, 1, Z), f32),
                pltpu.SemaphoreType.DMA((2, 9)),
                pltpu.SemaphoreType.DMA((2, 9)),
                pltpu.SemaphoreType.DMA((orders,)),
                pltpu.SemaphoreType.DMA((orders,)),
                pltpu.SemaphoreType.DMA((5,)),
            ],
            compiler_params=pltpu.CompilerParams(
                collective_id=0, has_side_effects=True, vmem_limit_bytes=60 * 1024 * 1024
            ),
        )(labels, conductivity, right_side)
        return pl.pallas_call(
            combine,
            out_shape=jax.ShapeDtypeStruct((X, Y, Z), f32),
            in_specs=[pl.BlockSpec(memory_space=vmem)] * 2,
            out_specs=pl.BlockSpec(memory_space=pl.ANY),
            scratch_shapes=[vmem((X, Y, Z), f32), pltpu.SemaphoreType.DMA((group_size(X, 4),))],
            compiler_params=pltpu.CompilerParams(vmem_limit_bytes=8 * 1024 * 1024),
        )(fields, factors)

    return jax.shard_map(
        local,
        mesh=mesh,
        in_specs=(P("gx", "gy", "gz"), P(), P("gx", "gy", "gz")),
        out_specs=P("gx", "gy", "gz"),
        check_vma=False,
    )
```
